8 devices in a mesh: tp: 2 (over z, y), ep: 4 (over x, core).
Axes of the slice: x: 2, y: 2, z: 1, core: 2. Of those that a mesh axis runs over, the one named last changes fastest.
Arguments:
- x_norm: bfloat16 [4096, 1024], P(('ep', 'tp'))
- route_idx: int32 [4096, 8], P(('ep', 'tp'))
- route_slot: int32 [4096, 8], P(('ep', 'tp'))
- w_router: bfloat16 [1024, 32], replicated
- b_router: float32 [32], replicated
- w_gate_up: bfloat16 [32, 1024, 1024], P('ep', None, 'tp')
- b_gate_up: float32 [32, 1024], P('ep', 'tp')
- w_down: bfloat16 [32, 512, 1024], P('ep', 'tp')
- b_down: float32 [32, 1024], P('ep')
- d_out: bfloat16 [4096, 1024], P(('ep', 'tp'))
Outputs:
- output 1: bfloat16 [4096, 1024], P(('ep', 'tp'))
- output 2: bfloat16 [4096, 1024], P(('ep', 'tp'))
- output 3: bfloat16 [32, 1024, 1024], P('ep', None, 'tp')
- output 4: float32 [32, 1024], P('ep', 'tp')
- output 5: bfloat16 [32, 512, 1024], P('ep', 'tp')
- output 6: float32 [32, 1024], P('ep')
- output 7: float32 [1024, 32], replicated
- output 8: float32 [32], replicated
All inputs are finite; a program needn't handle non-finite values.
Results may differ from the reference program's by a relative error of at most 0.0122516.
Values are sent between devices in bfloat16 or wider.
A program may use at most 1 GiB of HBM per device.

```python
import functools
import jax
import jax.numpy as jnp
from jax import lax

HIDDEN = 1024
EXPERT_WIDTH = 512
EXPERTS = 32
TOP_K = 8
TOK_DEV = 512
DEVICES = 8
TP_SIZE = 2
TOKENS = TOK_DEV * DEVICES
CAPACITY = 2 * TOK_DEV * TOP_K // EXPERTS
SHARD_WIDTH = EXPERT_WIDTH // TP_SIZE
HOT_COUNT = max(1, EXPERTS // 8)
BUF_ROWS = EXPERTS * DEVICES * CAPACITY
CLAMP_LIMIT = 7.0
SWIGLU_ALPHA = 1.702


def draw_routing(route_key):
    perm_key, score_key = jax.random.split(route_key)
    hot_order = jax.random.permutation(perm_key, EXPERTS)
    hot_bonus = jnp.zeros((EXPERTS,), jnp.int32).at[hot_order[:HOT_COUNT]].set(32)
    scores = jax.random.randint(score_key, (TOKENS, EXPERTS), 0, 256, jnp.int32) + hot_bonus[None, :]
    local_pos = jnp.arange(TOKENS) % TOK_DEV
    forced = (local_pos < 2 * CAPACITY)[:, None] & (jnp.arange(EXPERTS) == hot_order[0])[None, :]
    scores = jnp.where(forced, 4096, scores)
    keyed_scores = scores * EXPERTS + jnp.arange(EXPERTS, dtype=jnp.int32)[None, :]
    route_idx = lax.top_k(keyed_scores, TOP_K)[1]
    expert_hits = (route_idx[:, :, None] == jnp.arange(EXPERTS)[None, None, :]).astype(jnp.int32)
    expert_hits = expert_hits.reshape(DEVICES, TOK_DEV * TOP_K, EXPERTS)
    slot_rank = jnp.sum((jnp.cumsum(expert_hits, axis=1) - 1) * expert_hits, axis=2)
    slot_rank = slot_rank.reshape(TOKENS, TOP_K)
    route_slot = jnp.where(slot_rank < CAPACITY, slot_rank, -1)
    return route_idx.astype(jnp.int32), route_slot.astype(jnp.int32)


def setup_inputs(seed: int = 0) -> dict:
    base_key = jax.random.key(seed)
    sub_keys = jax.random.split(base_key, 9)
    x_norm = jax.random.normal(sub_keys[0], (TOKENS, HIDDEN), jnp.float32)
    w_router = jax.random.normal(sub_keys[1], (HIDDEN, EXPERTS), jnp.float32) * HIDDEN ** -0.5
    b_router = jax.random.normal(sub_keys[2], (EXPERTS,), jnp.float32)
    w_gate_up = jax.random.normal(sub_keys[3], (EXPERTS, HIDDEN, 2 * EXPERT_WIDTH), jnp.float32) * (3.0 * HIDDEN ** -0.5)
    b_gate_up = jax.random.normal(sub_keys[4], (EXPERTS, 2 * EXPERT_WIDTH), jnp.float32)
    w_down = jax.random.normal(sub_keys[5], (EXPERTS, EXPERT_WIDTH, HIDDEN), jnp.float32) * (0.25 * EXPERT_WIDTH ** -0.5)
    b_down = jax.random.normal(sub_keys[6], (EXPERTS, HIDDEN), jnp.float32)
    d_out = jax.random.normal(sub_keys[7], (TOKENS, HIDDEN), jnp.float32)
    route_idx, route_slot = draw_routing(sub_keys[8])
    return {'x_norm': x_norm.astype(jnp.bfloat16), 'route_idx': route_idx, 'route_slot': route_slot, 'w_router': w_router.astype(jnp.bfloat16), 'b_router': b_router, 'w_gate_up': w_gate_up.astype(jnp.bfloat16), 'b_gate_up': b_gate_up, 'w_down': w_down.astype(jnp.bfloat16), 'b_down': b_down, 'd_out': d_out.astype(jnp.bfloat16)}


def bf16_snap(value):
    return value + lax.stop_gradient(value.astype(jnp.bfloat16).astype(jnp.float32) - value)


def clamped_swiglu(h_pair):
    gate_val = jnp.minimum(h_pair[..., 0], CLAMP_LIMIT)
    up_val = jnp.clip(h_pair[..., 1], -CLAMP_LIMIT, CLAMP_LIMIT)
    return gate_val * jax.nn.sigmoid(SWIGLU_ALPHA * gate_val) * (up_val + 1.0)


def expert_rows(operands):
    rows_in, w_gu_one, b_gu_one, w_dn_one, b_dn_one = operands
    hidden_pre = jnp.dot(rows_in, w_gu_one) + b_gu_one[None, :]
    act_val = bf16_snap(clamped_swiglu(hidden_pre.reshape(-1, EXPERT_WIDTH, 2)))
    part_out = jnp.einsum('rsf,sfd->rsd', act_val.reshape(-1, TP_SIZE, SHARD_WIDTH), w_dn_one.reshape(TP_SIZE, SHARD_WIDTH, HIDDEN))
    first_mask = (jnp.arange(TP_SIZE) == 0).astype(part_out.dtype)
    part_out = bf16_snap(part_out + first_mask[None, :, None] * b_dn_one[None, None, :])
    return bf16_snap(jnp.sum(part_out, axis=1))


def block_forward(x_wide, w_router, b_router, w_gate_up, b_gate_up, w_down, b_down, route_idx, route_slot):
    logits = jnp.dot(x_wide, w_router) + b_router[None, :]
    gate_w = jax.nn.softmax(jnp.take_along_axis(logits, route_idx, axis=1), axis=1)
    is_kept = route_slot >= 0
    source_dev = (jnp.arange(TOKENS) // TOK_DEV)[:, None]
    flat_pos = jnp.where(is_kept, (route_idx * DEVICES + source_dev) * CAPACITY + route_slot, BUF_ROWS)
    token_ids = jnp.broadcast_to(jnp.arange(TOKENS, dtype=jnp.int32)[:, None], (TOKENS, TOP_K))
    row_token = jnp.full((BUF_ROWS,), TOKENS, jnp.int32).at[flat_pos.reshape(-1)].set(token_ids.reshape(-1), mode='drop')
    x_pad = jnp.concatenate([x_wide, jnp.zeros((1, HIDDEN), x_wide.dtype)], axis=0)
    routed_rows = x_pad[row_token].reshape(EXPERTS, DEVICES * CAPACITY, HIDDEN)
    expert_out = lax.map(jax.checkpoint(expert_rows), (routed_rows, w_gate_up, b_gate_up, w_down, b_down))
    y_flat = expert_out.reshape(BUF_ROWS, HIDDEN)
    safe_pos = jnp.where(is_kept, flat_pos, 0)
    kept_w = gate_w * is_kept.astype(gate_w.dtype)
    moe_acc = jnp.zeros((TOKENS, HIDDEN), gate_w.dtype)
    for choice in range(TOP_K):
        moe_acc = moe_acc + kept_w[:, choice:choice + 1] * y_flat[safe_pos[:, choice]]
    return bf16_snap(moe_acc)


def reference(x_norm, route_idx, route_slot, w_router, b_router, w_gate_up, b_gate_up, w_down, b_down, d_out):
    forward_fn = functools.partial(block_forward, route_idx=route_idx, route_slot=route_slot)
    moe_out, pullback = jax.vjp(forward_fn, x_norm.astype(jnp.float32), w_router.astype(jnp.float32), b_router, w_gate_up.astype(jnp.float32), b_gate_up, w_down.astype(jnp.float32), b_down)
    grad_all = pullback(d_out.astype(jnp.float32))
    return (moe_out.astype(jnp.bfloat16), grad_all[0].astype(jnp.bfloat16), grad_all[3].astype(jnp.bfloat16), grad_all[4], grad_all[5].astype(jnp.bfloat16), grad_all[6], grad_all[1], grad_all[2])
```

```python
import functools
import jax
import jax.numpy as jnp
from jax import lax
from jax.experimental import pallas as pl
from jax.experimental.pallas import tpu as pltpu
from jax.sharding import PartitionSpec as P

LIMIT = 7.0
ALPHA = 1.702
BF = jnp.bfloat16
F32 = jnp.float32
SIZES = (64, 128, 192, 256)
SEG = 256
KT = 256


def dot(a, b, dims=((1,), (0,))):
    return lax.dot_general(a, b, (dims, ((), ())), preferred_element_type=F32)


def chunk_kernel(cnt_ref, x_ref, d_ref, rk_ref, wv_ref, w1_ref, w1t_ref, w2_ref, w2t_ref, b1_ref, b2_ref,
                 out_ref, dx_ref, dg_ref, gb1_ref, xs_ref, ds_ref, dh_ref, wa_ref,
                 sel, ybuf, dxbuf, acc, off):
    e = pl.program_id(0)
    i = pl.program_id(1)
    n_e = pl.num_programs(0)
    toks = x_ref.shape[1]
    half = w2_ref.shape[1]

    @pl.when(e == 0)
    def _():
        off[i] = 0

    @pl.when(i == 0)
    def _():
        gb1_ref[...] = jnp.zeros_like(gb1_ref)

    count = cnt_ref[e * 2 + i]
    start = pl.multiple_of(off[i], 64)

    def rows(m):
        rk = rk_ref[0, pl.ds(i, 1), :]
        wv = wv_ref[0, pl.ds(i, 1), :]
        pos = lax.broadcasted_iota(jnp.int32, (m, toks), 0).astype(F32)
        hot = jnp.broadcast_to(rk, (m, toks)) == pos
        hot_b = jnp.where(hot, 1.0, 0.0).astype(BF)
        w_row = jnp.sum(jnp.where(hot, jnp.broadcast_to(wv, (m, toks)), 0.0), axis=1, keepdims=True)
        x_rows = dot(hot_b, x_ref[i]).astype(BF)
        d_rows = dot(hot_b, d_ref[i]).astype(BF)
        hid = dot(x_rows, w1_ref[0]) + b1_ref[0]
        gate, up = hid[:, :half], hid[:, half:]
        g = jnp.minimum(gate, LIMIT)
        u1 = jnp.clip(up, -LIMIT, LIMIT) + 1.0
        sg = jax.nn.sigmoid(ALPHA * g)
        gs = g * sg
        act = (gs * u1).astype(BF)
        part = (dot(act, w2_ref[0]) + b2_ref[0]).astype(BF).astype(F32)
        dg_row = jnp.sum(part * d_rows.astype(F32), axis=1, keepdims=True)
        dg_ref[0, pl.ds(i, 1), :] = jnp.sum(jnp.where(hot, dg_row, 0.0), axis=0, keepdims=True)
        ybuf[i, pl.ds(start, m), :] = (w_row * part).astype(BF)
        sel[i, pl.ds(start, m), :] = hot_b
        d_act = w_row * dot(d_rows, w2t_ref[0])
        gate_on = jnp.where(gate < LIMIT, 1.0, jnp.where(gate == LIMIT, 0.5, 0.0))
        up_abs = jnp.abs(up)
        up_on = jnp.where(up_abs < LIMIT, 1.0, jnp.where(up_abs == LIMIT, 0.5, 0.0))
        d_gate = d_act * u1 * (sg * (1.0 + ALPHA * g * (1.0 - sg))) * gate_on
        d_up = d_act * gs * up_on
        d_hid = jnp.concatenate([d_gate, d_up], axis=1)
        gb1_ref[0] += jnp.sum(d_hid, axis=0, keepdims=True)
        d_hid_b = d_hid.astype(BF)
        dxbuf[i, pl.ds(start, m), :] = dot(d_hid_b, w1t_ref[0]).astype(BF)
        xs_ref[0, 0, :m, :] = x_rows
        ds_ref[0, 0, :m, :] = d_rows
        dh_ref[0, 0, :m, :] = d_hid_b
        wa_ref[0, 0, :m, :] = (w_row * act.astype(F32)).astype(BF)
        if m < SEG:
            for ref in (xs_ref, ds_ref, dh_ref, wa_ref):
                ref[0, 0, m:, :] = jnp.zeros((SEG - m, ref.shape[3]), BF)
        off[i] = start + m

    low = 0
    for m in SIZES:
        pl.when((count > low) & (count <= m))(functools.partial(rows, m))
        low = m

    @pl.when(count == 0)
    def _():
        dg_ref[0, pl.ds(i, 1), :] = jnp.zeros((1, toks), F32)
        for ref in (xs_ref, ds_ref, dh_ref, wa_ref):
            ref[...] = jnp.zeros_like(ref)

    @pl.when(e == n_e - 1)
    def _():
        total = off[i]
        fill = pl.multiple_of(total, 64)
        for buf in (sel, ybuf, dxbuf):
            buf[i, pl.ds(fill, KT), :] = jnp.zeros((KT, buf.shape[2]), BF)
        tiles = (total + KT - 1) // KT
        for buf, dst in ((ybuf, out_ref), (dxbuf, dx_ref)):
            acc[...] = jnp.zeros_like(acc)

            def step(k, _):
                at = pl.ds(pl.multiple_of(k * KT, KT), KT)
                acc[...] += dot(sel[i, at, :], buf[i, at, :], ((0,), (0,)))
                return 0

            lax.fori_loop(0, tiles, step, 0)
            dst[i] = acc[...].astype(BF)


def run_chunk(cnt, x2, d2, rk, wv, w1, w1t, w2, w2t, b1, b2):
    n_e, dim, wide = w1.shape
    half = w2.shape[1]
    toks = x2.shape[1]
    whole3 = lambda e, i, c: (0, 0, 0)
    per_e = lambda e, i, c: (e, 0, 0)
    seg = lambda e, i, c: (e, i, 0, 0)
    room = n_e * SEG + KT
    return pl.pallas_call(
        chunk_kernel,
        grid_spec=pltpu.PrefetchScalarGridSpec(
            num_scalar_prefetch=1,
            grid=(n_e, 2),
            in_specs=[
                pl.BlockSpec((2, toks, dim), whole3, pipeline_mode=pl.Buffered(1)),
                pl.BlockSpec((2, toks, dim), whole3, pipeline_mode=pl.Buffered(1)),
                pl.BlockSpec((1, 2, toks), per_e),
                pl.BlockSpec((1, 2, toks), per_e),
                pl.BlockSpec((1, dim, wide), per_e),
                pl.BlockSpec((1, wide, dim), per_e),
                pl.BlockSpec((1, half, dim), per_e),
                pl.BlockSpec((1, dim, half), per_e),
                pl.BlockSpec((1, 1, wide), per_e),
                pl.BlockSpec((1, 1, dim), per_e),
            ],
            out_specs=[
                pl.BlockSpec((2, toks, dim), whole3, pipeline_mode=pl.Buffered(1)),
                pl.BlockSpec((2, toks, dim), whole3, pipeline_mode=pl.Buffered(1)),
                pl.BlockSpec((1, 2, toks), per_e),
                pl.BlockSpec((1, 1, wide), per_e),
                pl.BlockSpec((1, 1, SEG, dim), seg),
                pl.BlockSpec((1, 1, SEG, dim), seg),
                pl.BlockSpec((1, 1, SEG, wide), seg),
                pl.BlockSpec((1, 1, SEG, half), seg),
            ],
            scratch_shapes=[
                pltpu.VMEM((2, room, toks), BF),
                pltpu.VMEM((2, room, dim), BF),
                pltpu.VMEM((2, room, dim), BF),
                pltpu.VMEM((toks, dim), F32),
                pltpu.SMEM((2,), jnp.int32),
            ],
        ),
        out_shape=[
            jax.ShapeDtypeStruct((2, toks, dim), BF),
            jax.ShapeDtypeStruct((2, toks, dim), BF),
            jax.ShapeDtypeStruct((n_e, 2, toks), F32),
            jax.ShapeDtypeStruct((n_e, 1, wide), F32),
            jax.ShapeDtypeStruct((n_e, 2, SEG, dim), BF),
            jax.ShapeDtypeStruct((n_e, 2, SEG, dim), BF),
            jax.ShapeDtypeStruct((n_e, 2, SEG, wide), BF),
            jax.ShapeDtypeStruct((n_e, 2, SEG, half), BF),
        ],
        compiler_params=pltpu.CompilerParams(dimension_semantics=('arbitrary', 'arbitrary'), vmem_limit_bytes=64000 * 1024),
        cost_estimate=pl.CostEstimate(flops=28_000_000_000, bytes_accessed=64_000_000, transcendentals=0),
        name='experts',
    )(cnt, x2, d2, rk, wv, w1, w1t, w2, w2t, b1, b2)


def wgrad_kernel(n_c, *refs):
    xs, ds, dh, wa = (refs[k * n_c:(k + 1) * n_c] for k in range(4))
    mix_ref, gw1_ref, gw2_ref, acc1, acc2 = refs[4 * n_c:]
    lhs = ((0,), (0,))
    for k in range(n_c):
        for i in range(2):
            one = dot(xs[k][0, i], dh[k][0, i], lhs)
            two = dot(wa[k][0, i], ds[k][0, i], lhs)
            if k + i == 0:
                acc1[...] = one
                acc2[...] = two
            else:
                acc1[...] += one
                acc2[...] += two
    gw2_ref[0] = acc2[...].astype(BF)
    gw1_ref[0] = dot(acc1[...].astype(BF), mix_ref[...]).astype(BF)


def run_wgrad(xs, ds, dh, wa, unmix):
    n_c = len(xs)
    n_e, _, _, dim = xs[0].shape
    wide, half = dh[0].shape[3], wa[0].shape[3]
    spec = lambda w: [pl.BlockSpec((1, 2, SEG, w), lambda e: (e, 0, 0, 0)) for _ in range(n_c)]
    return pl.pallas_call(
        functools.partial(wgrad_kernel, n_c),
        grid=(n_e,),
        in_specs=spec(dim) + spec(dim) + spec(wide) + spec(half) + [pl.BlockSpec((wide, wide), lambda e: (0, 0))],
        out_specs=[pl.BlockSpec((1, dim, wide), lambda e: (e, 0, 0)), pl.BlockSpec((1, half, dim), lambda e: (e, 0, 0))],
        out_shape=[jax.ShapeDtypeStruct((n_e, dim, wide), BF), jax.ShapeDtypeStruct((n_e, half, dim), BF)],
        scratch_shapes=[pltpu.VMEM((dim, wide), F32), pltpu.VMEM((half, dim), F32)],
        compiler_params=pltpu.CompilerParams(dimension_semantics=('arbitrary',), vmem_limit_bytes=64000 * 1024),
        cost_estimate=pl.CostEstimate(flops=26_000_000_000, bytes_accessed=100_000_000, transcendentals=0),
        name='weight_grads',
    )(*xs, *ds, *dh, *wa, unmix)


def solution(mesh):
    tp_count = mesh.shape['tp']
    ep_count = mesh.shape['ep']
    n_dev = tp_count * ep_count
    tok_spec = P(('ep', 'tp'), None)

    CORE, XF, YF = 2, 4, 1

    def flip(arr, bits):
        turned = (bits & 1) * ep_count + (bits >> 1)
        return lax.ppermute(arr, ('tp', 'ep'), [(s, s ^ turned) for s in range(n_dev)])

    def device_fn(x_loc, idx_loc, slot_loc, w_router, b_router, w_gate_up, b_gate_up, w_down, b_down, dy_loc):
        toks, dim = x_loc.shape
        n_experts = w_router.shape[1]
        n_e = w_gate_up.shape[0]
        wide = w_gate_up.shape[2]
        half = wide // 2
        tp_index = lax.axis_index('tp')
        ep_index = lax.axis_index('ep')
        me = ep_index * tp_count + tp_index

        logits = jnp.dot(x_loc, w_router, preferred_element_type=F32) + b_router[None, :]
        expert_hot = idx_loc[:, :, None] == jnp.arange(n_experts)[None, None, :]
        picked = jnp.sum(jnp.where(expert_hot, logits[:, None, :], 0.0), axis=2)
        gate_w = jax.nn.softmax(picked, axis=1)
        w_full = jnp.sum(jnp.where(expert_hot, gate_w[:, :, None], 0.0), axis=1)
        kept = jnp.any(expert_hot & (slot_loc >= 0)[:, :, None], axis=1)
        below = (jnp.arange(toks)[None, :] < jnp.arange(toks)[:, None]).astype(BF)
        rank = jnp.where(kept, jnp.dot(below, kept.astype(BF), preferred_element_type=F32), -1.0)
        aux = jnp.concatenate([w_full.T, rank.T], axis=0)

        xd = jnp.stack([x_loc, dy_loc])
        pairs = []
        for bits in (0, XF, YF, XF | YF):
            got, got_aux = (xd, aux) if bits == 0 else (flip(xd, bits), flip(aux, bits))
            pairs.append((bits, got, got_aux, flip(got, CORE), flip(got_aux, CORE)))

        col = jnp.arange(wide)
        split_mat = (jnp.where(col < half, 2 * col, 2 * (col - half) + 1)[None, :] == col[:, None]).astype(BF)
        w1 = jnp.einsum('edf,fg->edg', w_gate_up, split_mat, preferred_element_type=BF)
        w1t = jnp.einsum('edf,fg->egd', w_gate_up, split_mat, preferred_element_type=BF)
        w2t = jnp.swapaxes(w_down, 1, 2)
        b1 = jnp.concatenate([b_gate_up[:, 0::2], b_gate_up[:, 1::2]], axis=1)[:, None, :]
        b2 = (b_down * (tp_index == 0).astype(F32))[:, None, :]

        outs, dxs, dgs, gb1s, saved, w_all, kept_all = [], [], [], [], [], [], []
        for bits, xd_a, aux_a, xd_b, aux_b in pairs:
            x2 = jnp.stack([xd_a[0], xd_b[0]])
            d2 = jnp.stack([xd_a[1], xd_b[1]])
            both = jnp.stack([aux_a, aux_b], axis=1)
            wv = lax.dynamic_slice_in_dim(both, ep_index * n_e, n_e, axis=0)
            rk = lax.dynamic_slice_in_dim(both, n_experts + ep_index * n_e, n_e, axis=0)
            cnt = (jnp.max(rk, axis=2) + 1.0).astype(jnp.int32).reshape(-1)
            out2, dx2, dg2, gb1, xs, ds, dh, wa = run_chunk(cnt, x2, d2, rk, wv, w1, w1t, w_down, w2t, b1, b2)
            theirs = flip(jnp.stack([out2[1], dx2[1]]), CORE)
            mine = jnp.stack([out2[0], dx2[0]]).astype(F32) + theirs.astype(F32)
            if bits:
                mine = flip(mine.astype(BF), bits).astype(F32)
            outs.append(mine)
            dgs.append(dg2)
            gb1s.append(gb1)
            saved.append((xs, ds, dh, wa))
            wk = jnp.where(rk >= 0, wv, 0.0)
            w_all.append(wk)

        gw1, gw2 = run_wgrad(*[list(t) for t in zip(*saved)], split_mat.T)
        gb1 = functools.reduce(jnp.add, gb1s)[:, 0, :]
        gb1 = jnp.stack([gb1[:, :half], gb1[:, half:]], axis=2).reshape(n_e, wide)
        gb2 = 0.0
        for (bits, xd_a, _, xd_b, _), wk in zip(pairs, w_all):
            for k, xd_k in enumerate((xd_a, xd_b)):
                gb2 = gb2 + jnp.dot(wk[:, k, :], xd_k[1].astype(F32), precision=lax.Precision.HIGHEST)

        rel = [b | c for b in (0, XF, YF, XF | YF) for c in (0, CORE)]
        dg_rel = jnp.stack([dg[:, k, :] for dg in dgs for k in range(2)])
        slot_of = jnp.array([rel.index(m) for m in range(n_dev)], jnp.int32)
        dg_abs = dg_rel[slot_of[jnp.arange(n_dev) ^ me]]
        dg_back = lax.all_to_all(dg_abs, ('ep', 'tp'), 0, 0, tiled=True)
        d_gate = jnp.sum(dg_back.reshape(ep_count, tp_count, n_e, toks), axis=1).reshape(n_experts, toks).T
        d_logits = w_full * (d_gate - jnp.sum(w_full * d_gate, axis=1, keepdims=True))
        d_logits_b = d_logits.astype(BF)
        gwr = lax.psum(jnp.einsum('td,te->de', x_loc, d_logits_b, preferred_element_type=F32), ('tp', 'ep'))
        gbr = lax.psum(jnp.sum(d_logits, axis=0), ('tp', 'ep'))
        total = functools.reduce(jnp.add, outs)
        d_x = total[1] + jnp.einsum('te,de->td', d_logits_b, w_router, preferred_element_type=F32)
        return (total[0].astype(BF), d_x.astype(BF), gw1, gb1, gw2, gb2, gwr, gbr)

    in_specs = (tok_spec, tok_spec, tok_spec, P(None, None), P(None), P('ep', None, 'tp'), P('ep', 'tp'), P('ep', 'tp', None), P('ep', None), tok_spec)
    out_specs = (tok_spec, tok_spec, P('ep', None, 'tp'), P('ep', 'tp'), P('ep', 'tp', None), P('ep', None), P(None, None), P(None))
    return jax.shard_map(device_fn, mesh=mesh, in_specs=in_specs, out_specs=out_specs, check_vma=False)
```

```python
import functools
import jax
import jax.numpy as jnp
from jax import lax
from jax.experimental import pallas as pl
from jax.experimental.pallas import tpu as pltpu
from jax.sharding import PartitionSpec as P

LIMIT = 7.0
ALPHA = 1.702
BF = jnp.bfloat16
F32 = jnp.float32
TILE = 256
SIZES = (128, 256)
BACK = ((1,), (1,))
LHS = ((0,), (0,))


def dot(a, b, dims=((1,), (0,))):
    return lax.dot_general(a, b, (dims, ((), ())), preferred_element_type=F32)


def chunk_kernel(first, toks, ep_ref, xa_ref, xb_ref, w1_in, w2_ref, b1_ref, b2_ref, *refs):
    if first:
        split_ref, *refs = refs
    oa_ref, ob_ref, dg_ref, gb1_ref, gb2_ref, nt_ref, *refs = refs
    if first:
        w1_ref, *refs = refs
    else:
        w1_ref = w1_in
    xs_hbm, ds_hbm, dh_hbm, wa_hbm, *refs = refs
    aux, xbuf, dbuf, dhst, wast, wrow, dgrow, yst, dxst, sel, ybuf, dxbuf, acc, off, sems = refs
    e = pl.program_id(0)
    n_e = pl.num_programs(0)
    half = w2_ref.shape[1]
    tok_refs = (xa_ref, xb_ref)
    par = lax.rem(e, 2)

    def saves(expert, t, p):
        at = pl.ds(t * TILE, TILE)
        pairs = ((xbuf, xs_hbm), (dbuf, ds_hbm), (dhst, dh_hbm), (wast, wa_hbm))
        return [pltpu.make_async_copy(src.at[p, at], dst.at[expert, t], sems.at[p, t, k])
                for k, (src, dst) in enumerate(pairs)]

    def drain(expert, p):
        for t in range(2):
            @pl.when(nt_ref[expert] > t)
            def _():
                for copy in saves(expert, t, p):
                    copy.wait()

    @pl.when(e == 0)
    def _():
        for i in range(2):
            off[i] = 0
            aux[i] = tok_refs[i][2 * toks:, :].astype(F32)
            xbuf[i] = jnp.zeros(xbuf.shape[1:], BF)
            dbuf[i] = jnp.zeros(dbuf.shape[1:], BF)
        yst[...] = jnp.zeros_like(yst)
        dxst[...] = jnp.zeros_like(dxst)

    for p in range(2):
        @pl.when((e >= 2) & (par == p))
        def _():
            drain(e - 2, p)

    if first:
        w1_ref[0] = dot(w1_in[0], split_ref[...]).astype(BF)

    row = ep_ref[0] * n_e + e
    wrow[...] = jnp.zeros_like(wrow)
    ranks, counts = [], []
    for i in range(2):
        rk = aux[i, pl.ds(row + 4 * n_e, 1), :][:, toks:]
        ranks.append(rk)
        counts.append((jnp.max(rk) + 1.0).astype(jnp.int32))
    starts = (0, pl.multiple_of((counts[0] + 15) // 16 * 16, 16))
    n_tiles = (starts[1] + counts[1] + TILE - 1) // TILE
    nt_ref[e] = n_tiles

    def place(i, m):
        pair = aux[i, pl.ds(row, 1), :]
        low = aux[i, pl.ds(row + 4 * n_e, 1), :]
        wv = pair[:, :toks] + pair[:, toks:] + low[:, :toks]
        pos = lax.broadcasted_iota(jnp.int32, (m, toks), 0).astype(F32)
        hot = jnp.broadcast_to(ranks[i], (m, toks)) == pos
        hot_b = jnp.where(hot, 1.0, 0.0).astype(BF)
        at = pl.ds(starts[i], m)
        wrow[at, :] = jnp.sum(jnp.where(hot, jnp.broadcast_to(wv, (m, toks)), 0.0), axis=1, keepdims=True)
        xbuf[par, at, :] = dot(hot_b, tok_refs[i][:toks, :]).astype(BF)
        dbuf[par, at, :] = dot(hot_b, tok_refs[i][toks:2 * toks, :]).astype(BF)
        sel[i, pl.ds(pl.multiple_of(off[i], 128), m), :] = hot_b

    for i in range(2):
        low = 0
        for m in SIZES:
            pl.when((counts[i] > low) & (counts[i] <= m))(functools.partial(place, i, m))
            low = m

    gb1_ref[...] = jnp.zeros_like(gb1_ref)
    gb2_ref[...] = jnp.zeros_like(gb2_ref)

    def tile(t, _):
        at = pl.ds(pl.multiple_of(t * TILE, TILE), TILE)
        x_rows = xbuf[par, at, :]
        d_rows = dbuf[par, at, :]
        w_row = wrow[at, :]
        hid = dot(x_rows, w1_ref[0]) + b1_ref[0]
        gate, up = hid[:, :half], hid[:, half:]
        g = jnp.minimum(gate, LIMIT)
        u1 = jnp.clip(up, -LIMIT, LIMIT) + 1.0
        sg = jax.nn.sigmoid(ALPHA * g)
        gs = g * sg
        act = (gs * u1).astype(BF)
        part = (dot(act, w2_ref[0]) + b2_ref[0]).astype(BF).astype(F32)
        d_wide = d_rows.astype(F32)
        dgrow[at, :] = jnp.sum(part * d_wide, axis=1, keepdims=True)
        gb2_ref[0] += jnp.sum(w_row * d_wide, axis=0, keepdims=True)
        yst[at, :] = (w_row * part).astype(BF)
        d_act = w_row * dot(d_rows, w2_ref[0], BACK)
        gate_on = jnp.where(gate < LIMIT, 1.0, jnp.where(gate == LIMIT, 0.5, 0.0))
        up_abs = jnp.abs(up)
        up_on = jnp.where(up_abs < LIMIT, 1.0, jnp.where(up_abs == LIMIT, 0.5, 0.0))
        d_gate = d_act * u1 * (sg * (1.0 + ALPHA * g * (1.0 - sg))) * gate_on
        d_up = d_act * gs * up_on
        d_hid = jnp.concatenate([d_gate, d_up], axis=1)
        gb1_ref[0] += jnp.sum(d_hid, axis=0, keepdims=True)
        d_hid_b = d_hid.astype(BF)
        dhst[par, at, :] = d_hid_b
        wast[par, at, :] = (w_row * act.astype(F32)).astype(BF)
        dxst[at, :] = dot(d_hid_b, w1_ref[0], BACK).astype(BF)
        for copy in saves(e, t, par):
            copy.start()
        return 0

    lax.fori_loop(0, n_tiles, tile, 0)

    def collect(i, m):
        src = pl.ds(starts[i], m)
        dst = pl.ds(pl.multiple_of(off[i], 128), m)
        ybuf[i, dst, :] = yst[src, :]
        dxbuf[i, dst, :] = dxst[src, :]
        pos = lax.broadcasted_iota(jnp.int32, (m, toks), 0).astype(F32)
        hot = jnp.broadcast_to(ranks[i], (m, toks)) == pos
        dg_ref[0, i:i + 1, :] = jnp.sum(jnp.where(hot, dgrow[src, :], 0.0), axis=0, keepdims=True)
        off[i] = off[i] + m

    low = 0
    for m in SIZES:
        for i in range(2):
            pl.when((counts[i] > low) & (counts[i] <= m))(functools.partial(collect, i, m))
        low = m
    for i in range(2):
        @pl.when(counts[i] == 0)
        def _():
            dg_ref[0, i:i + 1, :] = jnp.zeros((1, toks), F32)

    @pl.when(e == n_e - 1)
    def _():
        for i, o_ref in enumerate((oa_ref, ob_ref)):
            total = pl.multiple_of(off[i], 128)
            for buf in (sel, ybuf, dxbuf):
                buf[i, pl.ds(total, TILE), :] = jnp.zeros((TILE, buf.shape[2]), BF)
            tiles = (total + TILE - 1) // TILE
            for k, buf in enumerate((ybuf, dxbuf)):
                acc[...] = jnp.zeros_like(acc)

                def step(j, _):
                    at = pl.ds(pl.multiple_of(j * TILE, TILE), TILE)
                    acc[...] += dot(sel[i, at, :], buf[i, at, :], LHS)
                    return 0

                lax.fori_loop(0, tiles, step, 0)
                o_ref[k * toks:(k + 1) * toks, :] = acc[...].astype(BF)
        for back in (1, 0):
            p = lax.rem(e - back, 2)
            drain(e - back, p)


def run_chunk(ep, xa, xb, w1, w2, b1, b2, toks, split=None):
    first = split is not None
    n_e, dim, wide = w1.shape
    half = w2.shape[1]
    whole = lambda e, ep: (0, 0)
    per_e = lambda e, ep: (e, 0, 0)
    once = dict(pipeline_mode=pl.Buffered(1))
    room = n_e * TILE + TILE
    hbm = pl.BlockSpec(memory_space=pl.ANY)
    in_specs = [
        pl.BlockSpec(xa.shape, whole, **once),
        pl.BlockSpec(xb.shape, whole, **once),
        pl.BlockSpec((1, dim, wide), per_e),
        pl.BlockSpec((1, half, dim), per_e),
        pl.BlockSpec((1, 1, wide), per_e),
        pl.BlockSpec((1, 1, dim), per_e),
    ]
    out_specs = [
        pl.BlockSpec((2 * toks, dim), whole, **once),
        pl.BlockSpec((2 * toks, dim), whole, **once),
        pl.BlockSpec((1, 2, toks), per_e),
        pl.BlockSpec((1, 1, wide), per_e),
        pl.BlockSpec((1, 1, dim), per_e),
        pl.BlockSpec(memory_space=pltpu.SMEM),
    ]
    shape = jax.ShapeDtypeStruct
    out_shape = [
        shape((2 * toks, dim), BF), shape((2 * toks, dim), BF), shape((n_e, 2, toks), F32),
        shape((n_e, 1, wide), F32), shape((n_e, 1, dim), F32), shape((n_e,), jnp.int32),
    ]
    if first:
        in_specs.append(pl.BlockSpec((wide, wide), whole))
        out_specs.append(pl.BlockSpec((1, dim, wide), per_e))
        out_shape.append(shape((n_e, dim, wide), BF))
    out_specs += [hbm] * 4
    out_shape += [shape((n_e, 2, TILE, w), BF) for w in (dim, dim, wide, half)]
    got = pl.pallas_call(
        functools.partial(chunk_kernel, first, toks),
        grid_spec=pltpu.PrefetchScalarGridSpec(
            num_scalar_prefetch=1,
            grid=(n_e,),
            in_specs=in_specs,
            out_specs=out_specs,
            scratch_shapes=[
                pltpu.VMEM((2, xa.shape[0] - 2 * toks, dim), F32),
                pltpu.VMEM((2, 2 * TILE, dim), BF),
                pltpu.VMEM((2, 2 * TILE, dim), BF),
                pltpu.VMEM((2, 2 * TILE, wide), BF),
                pltpu.VMEM((2, 2 * TILE, half), BF),
                pltpu.VMEM((2 * TILE, 1), F32),
                pltpu.VMEM((2 * TILE, 1), F32),
                pltpu.VMEM((2 * TILE, dim), BF),
                pltpu.VMEM((2 * TILE, dim), BF),
                pltpu.VMEM((2, room, toks), BF),
                pltpu.VMEM((2, room, dim), BF),
                pltpu.VMEM((2, room, dim), BF),
                pltpu.VMEM((toks, dim), F32),
                pltpu.SMEM((2,), jnp.int32),
                pltpu.SemaphoreType.DMA((2, 2, 4)),
            ],
        ),
        out_shape=out_shape,
        compiler_params=pltpu.CompilerParams(dimension_semantics=('arbitrary',), vmem_limit_bytes=65000 * 1024),
        cost_estimate=pl.CostEstimate(flops=28_000_000_000, bytes_accessed=40_000_000, transcendentals=0),
        name='experts',
    )(ep, xa, xb, w1, w2, b1, b2, *((split,) if first else ()))
    oa, ob, dg, gb1, gb2, nt = got[:6]
    return oa, ob, dg, gb1, gb2, nt, got[-4:], (got[6] if first else w1)


def wgrad_kernel(n_c, first_e, nt_ref, *refs):
    hbm = [refs[k * n_c:(k + 1) * n_c] for k in range(4)]
    mix_ref, gw1_ref, gw2_ref, acc1, acc2, *bufs, sems = refs[4 * n_c:]
    e = pl.program_id(0)
    n_e = pl.num_programs(0)
    par = lax.rem(e, 2)

    def fetches(step, c, t, p):
        return [pltpu.make_async_copy(hbm[k][c].at[first_e + step, t], bufs[k].at[p, 2 * c + t], sems.at[p, 2 * c + t, k])
                for k in range(4)]

    def each(step, act):
        for c in range(n_c):
            for t in range(2):
                pl.when(nt_ref[c, first_e + step] > t)(functools.partial(act, c, t))

    def start(step, p):
        def go(c, t):
            for copy in fetches(step, c, t, p):
                copy.start()
        each(step, go)

    @pl.when(e == 0)
    def _():
        start(e, par)

    @pl.when(e + 1 < n_e)
    def _():
        start(e + 1, 1 - par)

    acc1[...] = jnp.zeros_like(acc1)
    acc2[...] = jnp.zeros_like(acc2)

    def add(c, t):
        for copy in fetches(e, c, t, par):
            copy.wait()
        x_rows, d_rows, d_hid, act_w = (buf[par, 2 * c + t] for buf in bufs)
        acc1[...] += dot(x_rows, d_hid, LHS)
        acc2[...] += dot(act_w, d_rows, LHS)

    each(e, add)
    gw2_ref[0] = acc2[...].astype(BF)
    gw1_ref[0] = dot(acc1[...].astype(BF), mix_ref[...]).astype(BF)


def run_wgrad(nt, saved, unmix, first_e, n_e):
    n_c = len(saved)
    xs, ds, dh, wa = (list(t) for t in zip(*saved))
    dim, wide, half = xs[0].shape[3], dh[0].shape[3], wa[0].shape[3]
    return pl.pallas_call(
        functools.partial(wgrad_kernel, n_c, first_e),
        grid_spec=pltpu.PrefetchScalarGridSpec(
            num_scalar_prefetch=1,
            grid=(n_e,),
            in_specs=[pl.BlockSpec(memory_space=pl.ANY)] * (4 * n_c) + [pl.BlockSpec((wide, wide), lambda e, nt: (0, 0))],
            out_specs=[pl.BlockSpec((1, dim, wide), lambda e, nt: (e, 0, 0)), pl.BlockSpec((1, half, dim), lambda e, nt: (e, 0, 0))],
            scratch_shapes=[pltpu.VMEM((dim, wide), F32), pltpu.VMEM((half, dim), F32)]
            + [pltpu.VMEM((2, 2 * n_c, TILE, w), BF) for w in (dim, dim, wide, half)]
            + [pltpu.SemaphoreType.DMA((2, 2 * n_c, 4))],
        ),
        out_shape=[jax.ShapeDtypeStruct((n_e, dim, wide), BF), jax.ShapeDtypeStruct((n_e, half, dim), BF)],
        compiler_params=pltpu.CompilerParams(dimension_semantics=('arbitrary',), vmem_limit_bytes=64000 * 1024),
        cost_estimate=pl.CostEstimate(flops=26_000_000_000, bytes_accessed=60_000_000, transcendentals=0),
        name='weight_grads',
    )(nt, *xs, *ds, *dh, *wa, unmix)


def solution(mesh):
    tp_count = mesh.shape['tp']
    ep_count = mesh.shape['ep']
    n_dev = tp_count * ep_count
    tok_spec = P(('ep', 'tp'), None)

    CORE, XF, YF = 2, 4, 1
    CHIPS = (0, XF, YF | CORE, XF | YF)

    def flip(arr, bits):
        turned = (bits & 1) * ep_count + (bits >> 1)
        return lax.ppermute(arr, ('tp', 'ep'), [(s, s ^ turned) for s in range(n_dev)])

    def device_fn(x_loc, idx_loc, slot_loc, w_router, b_router, w_gate_up, b_gate_up, w_down, b_down, dy_loc):
        toks, dim = x_loc.shape
        n_experts = w_router.shape[1]
        n_e = w_gate_up.shape[0]
        wide = w_gate_up.shape[2]
        half = wide // 2
        tp_index = lax.axis_index('tp')
        ep_index = lax.axis_index('ep')
        me = ep_index * tp_count + tp_index

        logits = jnp.dot(x_loc, w_router, preferred_element_type=F32) + b_router[None, :]
        expert_hot = idx_loc[:, :, None] == jnp.arange(n_experts)[None, None, :]
        picked = jnp.sum(jnp.where(expert_hot, logits[:, None, :], 0.0), axis=2)
        gate_w = jax.nn.softmax(picked, axis=1)
        w_full = jnp.sum(jnp.where(expert_hot, gate_w[:, :, None], 0.0), axis=1)
        kept = jnp.any(expert_hot & (slot_loc >= 0)[:, :, None], axis=1)
        below = (jnp.arange(toks)[None, :] < jnp.arange(toks)[:, None]).astype(BF)
        rank = jnp.where(kept, jnp.dot(below, kept.astype(BF), preferred_element_type=F32), -1.0)
        w_top = lax.reduce_precision(w_full, 8, 7)
        w_mid = lax.reduce_precision(w_full - w_top, 8, 7)
        w_low = w_full - w_top - w_mid
        aux = jnp.concatenate([
            jnp.concatenate([w_top.T, w_mid.T], axis=1),
            jnp.concatenate([w_low.T, rank.T], axis=1)], axis=0).astype(BF)
        load = jnp.concatenate([x_loc, dy_loc, aux], axis=0)

        pairs = []
        for bits in CHIPS:
            got = load if bits == 0 else flip(load, bits)
            pairs.append((bits, got, flip(got, CORE)))

        col = jnp.arange(wide)
        split_mat = (jnp.where(col < half, 2 * col, 2 * (col - half) + 1)[None, :] == col[:, None]).astype(BF)
        b1 = jnp.concatenate([b_gate_up[:, 0::2], b_gate_up[:, 1::2]], axis=1)[:, None, :]
        b2 = (b_down * (tp_index == 0).astype(F32))[:, None, :]
        ep = ep_index.astype(jnp.int32)[None]

        w1 = w_gate_up
        outs, dgs, gb1s, gb2s, nts, saved = [], [], [], [], [], []
        pending = []

        def second_hop(bits, oa, theirs):
            mine = oa.astype(F32) + theirs.astype(F32)
            return mine.astype(BF) if bits else mine

        for step, (bits, xa, xb) in enumerate(pairs):
            if len(pending) == 2:
                b, oa_p, th_p = pending.pop(0)
                mine = second_hop(b, oa_p, th_p)
                mine, xa = lax.optimization_barrier((mine, xa))
                outs.append(flip(mine, b) if b else mine)
            oa, ob, dg, gb1, gb2, nt, keep, w1 = run_chunk(
                ep, xa, xb, w1, w_down, b1, b2, toks, split_mat if step == 0 else None)
            pending.append((bits, oa, flip(ob, CORE)))
            dgs.append(dg)
            gb1s.append(gb1)
            gb2s.append(gb2)
            nts.append(nt)
            saved.append(keep)

        unmix = split_mat.T
        nt_all = jnp.stack(nts)
        b, oa_p, th_p = pending.pop(0)
        mine = second_hop(b, oa_p, th_p)
        mine, nt_a = lax.optimization_barrier((mine, nt_all))
        outs.append(flip(mine, b))

        rel = [CHIPS[k // 2] ^ (CORE * (k % 2)) for k in range(n_dev)]
        dg_rel = jnp.stack([dg[:, k, :] for dg in dgs for k in range(2)])
        slot_of = jnp.array([rel.index(m) for m in range(n_dev)], jnp.int32)
        dg_abs = dg_rel[slot_of[jnp.arange(n_dev) ^ me]]
        dg_back = lax.all_to_all(dg_abs, ('ep', 'tp'), 0, 0, tiled=True)

        part_e = n_e // 2
        gw1_a, gw2_a = run_wgrad(nt_a, saved, unmix, 0, part_e)
        b, oa_p, th_p = pending.pop(0)
        mine = second_hop(b, oa_p, th_p)
        d_gate = jnp.sum(dg_back.reshape(ep_count, tp_count, n_e, toks), axis=1).reshape(n_experts, toks).T
        d_logits = w_full * (d_gate - jnp.sum(w_full * d_gate, axis=1, keepdims=True))
        mine, d_logits, nt_b, _ = lax.optimization_barrier((mine, d_logits, nt_all, gw2_a[0, 0, 0]))
        outs.append(flip(mine, b))
        gw1_b, gw2_b = run_wgrad(nt_b, saved, unmix, part_e, n_e - part_e)
        gw1 = jnp.concatenate([gw1_a, gw1_b])
        gw2 = jnp.concatenate([gw2_a, gw2_b])
        gb1 = functools.reduce(jnp.add, gb1s)[:, 0, :]
        gb1 = jnp.stack([gb1[:, :half], gb1[:, half:]], axis=2).reshape(n_e, wide)
        gb2 = functools.reduce(jnp.add, gb2s)[:, 0, :]

        d_all = lax.all_gather(d_logits, ('ep', 'tp'))
        d_all_b = d_all.astype(BF)
        gwr = 0.0
        for k, (_, xa, xb) in enumerate(pairs):
            for i, rows in enumerate((xa, xb)):
                gwr = gwr + jnp.einsum('td,te->de', rows[:toks], d_all_b[me ^ rel[2 * k + i]], preferred_element_type=F32)
        gbr = jnp.sum(d_all, axis=(0, 1))
        total = functools.reduce(jnp.add, [o.astype(F32) for o in outs])
        d_x = total[toks:] + jnp.einsum('te,de->td', d_logits.astype(BF), w_router, preferred_element_type=F32)
        return (total[:toks].astype(BF), d_x.astype(BF), gw1, gb1, gw2, gb2, gwr, gbr)

    in_specs = (tok_spec, tok_spec, tok_spec, P(None, None), P(None), P('ep', None, 'tp'), P('ep', 'tp'), P('ep', 'tp', None), P('ep', None), tok_spec)
    out_specs = (tok_spec, tok_spec, P('ep', None, 'tp'), P('ep', 'tp'), P('ep', 'tp', None), P('ep', None), P(None, None), P(None))
    return jax.shard_map(device_fn, mesh=mesh, in_specs=in_specs, out_specs=out_specs, check_vma=False)
```

```python
import functools
import jax
import jax.numpy as jnp
from jax import lax
from jax.experimental import pallas as pl
from jax.experimental.pallas import tpu as pltpu
from jax.sharding import PartitionSpec as P

LIMIT = 7.0
ALPHA = 1.702
BF = jnp.bfloat16
F32 = jnp.float32
TILE = 256
SIZES = (128, 256)
BACK = ((1,), (1,))
LHS = ((0,), (0,))


def dot(a, b, dims=((1,), (0,))):
    return lax.dot_general(a, b, (dims, ((), ())), preferred_element_type=F32)


def chunk_kernel(first, toks, ep_ref, xa_ref, xb_ref, w1_in, w2_ref, b1_ref, b2_ref, *refs):
    if first:
        split_ref, *refs = refs
    oa_ref, ob_ref, dg_ref, gb1_ref, gb2_ref, nt_ref, *refs = refs
    if first:
        w1_ref, *refs = refs
    else:
        w1_ref = w1_in
    xs_hbm, ds_hbm, dh_hbm, wa_hbm, *refs = refs
    aux, xbuf, dbuf, dhst, wast, wrow, dgrow, yst, dxst, sel, ybuf, dxbuf, acc, off, sems = refs
    e = pl.program_id(0)
    n_e = pl.num_programs(0)
    half = w2_ref.shape[1]
    tok_refs = (xa_ref, xb_ref)
    par = lax.rem(e, 2)

    def saves(expert, t, p):
        at = pl.ds(t * TILE, TILE)
        pairs = ((xbuf, xs_hbm), (dbuf, ds_hbm), (dhst, dh_hbm), (wast, wa_hbm))
        return [pltpu.make_async_copy(src.at[p, at], dst.at[expert, t], sems.at[p, t, k])
                for k, (src, dst) in enumerate(pairs)]

    def drain(expert, p):
        for t in range(2):
            @pl.when(nt_ref[expert] > t)
            def _():
                for copy in saves(expert, t, p):
                    copy.wait()

    @pl.when(e == 0)
    def _():
        for i in range(2):
            off[i] = 0
            aux[i] = tok_refs[i][2 * toks:, :].astype(F32)
            xbuf[i] = jnp.zeros(xbuf.shape[1:], BF)
            dbuf[i] = jnp.zeros(dbuf.shape[1:], BF)
        yst[...] = jnp.zeros_like(yst)
        dxst[...] = jnp.zeros_like(dxst)

    for p in range(2):
        @pl.when((e >= 2) & (par == p))
        def _():
            drain(e - 2, p)

    if first:
        w1_ref[0] = dot(w1_in[0], split_ref[...]).astype(BF)

    row = ep_ref[0] * n_e + e
    wrow[...] = jnp.zeros_like(wrow)
    ranks, counts = [], []
    for i in range(2):
        rk = aux[i, pl.ds(row + 4 * n_e, 1), :][:, toks:]
        ranks.append(rk)
        counts.append((jnp.max(rk) + 1.0).astype(jnp.int32))
    starts = (0, pl.multiple_of((counts[0] + 15) // 16 * 16, 16))
    n_tiles = (starts[1] + counts[1] + TILE - 1) // TILE
    nt_ref[e] = n_tiles

    def place(i, m):
        pair = aux[i, pl.ds(row, 1), :]
        low = aux[i, pl.ds(row + 4 * n_e, 1), :]
        wv = pair[:, :toks] + pair[:, toks:] + low[:, :toks]
        pos = lax.broadcasted_iota(jnp.int32, (m, toks), 0).astype(F32)
        hot = jnp.broadcast_to(ranks[i], (m, toks)) == pos
        hot_b = jnp.where(hot, 1.0, 0.0).astype(BF)
        at = pl.ds(starts[i], m)
        wrow[at, :] = jnp.sum(jnp.where(hot, jnp.broadcast_to(wv, (m, toks)), 0.0), axis=1, keepdims=True)
        xbuf[par, at, :] = dot(hot_b, tok_refs[i][:toks, :]).astype(BF)
        dbuf[par, at, :] = dot(hot_b, tok_refs[i][toks:2 * toks, :]).astype(BF)
        sel[i, pl.ds(pl.multiple_of(off[i], 128), m), :] = hot_b

    for i in range(2):
        low = 0
        for m in SIZES:
            pl.when((counts[i] > low) & (counts[i] <= m))(functools.partial(place, i, m))
            low = m

    gb1_ref[...] = jnp.zeros_like(gb1_ref)
    gb2_ref[...] = jnp.zeros_like(gb2_ref)

    def tile(t, _):
        at = pl.ds(pl.multiple_of(t * TILE, TILE), TILE)
        x_rows = xbuf[par, at, :]
        d_rows = dbuf[par, at, :]
        w_row = wrow[at, :]
        hid = dot(x_rows, w1_ref[0]) + b1_ref[0]
        d_act = w_row * dot(d_rows, w2_ref[0], BACK)
        gate, up = hid[:, :half], hid[:, half:]
        g = jnp.minimum(gate, LIMIT)
        u1 = jnp.clip(up, -LIMIT, LIMIT) + 1.0
        sg = jax.nn.sigmoid(ALPHA * g)
        gs = g * sg
        act = (gs * u1).astype(BF)
        part = (dot(act, w2_ref[0]) + b2_ref[0]).astype(BF).astype(F32)
        gate_on = jnp.where(gate < LIMIT, 1.0, jnp.where(gate == LIMIT, 0.5, 0.0))
        up_abs = jnp.abs(up)
        up_on = jnp.where(up_abs < LIMIT, 1.0, jnp.where(up_abs == LIMIT, 0.5, 0.0))
        d_gate = d_act * u1 * (sg * (1.0 + ALPHA * g * (1.0 - sg))) * gate_on
        d_up = d_act * gs * up_on
        d_hid = jnp.concatenate([d_gate, d_up], axis=1)
        gb1_ref[0] += jnp.sum(d_hid, axis=0, keepdims=True)
        d_hid_b = d_hid.astype(BF)
        dhst[par, at, :] = d_hid_b
        wast[par, at, :] = (w_row * act.astype(F32)).astype(BF)
        dxst[at, :] = dot(d_hid_b, w1_ref[0], BACK).astype(BF)
        d_wide = d_rows.astype(F32)
        dgrow[at, :] = jnp.sum(part * d_wide, axis=1, keepdims=True)
        gb2_ref[0] += jnp.sum(w_row * d_wide, axis=0, keepdims=True)
        yst[at, :] = (w_row * part).astype(BF)
        for copy in saves(e, t, par):
            copy.start()
        return 0

    lax.fori_loop(0, n_tiles, tile, 0)

    def collect(i, m):
        src = pl.ds(starts[i], m)
        dst = pl.ds(pl.multiple_of(off[i], 128), m)
        ybuf[i, dst, :] = yst[src, :]
        dxbuf[i, dst, :] = dxst[src, :]
        pos = lax.broadcasted_iota(jnp.int32, (m, toks), 0).astype(F32)
        hot = jnp.broadcast_to(ranks[i], (m, toks)) == pos
        dg_ref[0, i:i + 1, :] = jnp.sum(jnp.where(hot, dgrow[src, :], 0.0), axis=0, keepdims=True)
        off[i] = off[i] + m

    low = 0
    for m in SIZES:
        for i in range(2):
            pl.when((counts[i] > low) & (counts[i] <= m))(functools.partial(collect, i, m))
        low = m
    for i in range(2):
        @pl.when(counts[i] == 0)
        def _():
            dg_ref[0, i:i + 1, :] = jnp.zeros((1, toks), F32)

    @pl.when(e == n_e - 1)
    def _():
        for i, o_ref in enumerate((oa_ref, ob_ref)):
            total = pl.multiple_of(off[i], 128)
            for buf in (sel, ybuf, dxbuf):
                buf[i, pl.ds(total, TILE), :] = jnp.zeros((TILE, buf.shape[2]), BF)
            tiles = (total + TILE - 1) // TILE
            for k, buf in enumerate((ybuf, dxbuf)):
                acc[...] = jnp.zeros_like(acc)

                def step(j, _):
                    at = pl.ds(pl.multiple_of(j * TILE, TILE), TILE)
                    acc[...] += dot(sel[i, at, :], buf[i, at, :], LHS)
                    return 0

                lax.fori_loop(0, tiles, step, 0)
                o_ref[k * toks:(k + 1) * toks, :] = acc[...].astype(BF)
        for back in (1, 0):
            p = lax.rem(e - back, 2)
            drain(e - back, p)


def run_chunk(ep, xa, xb, w1, w2, b1, b2, toks, split=None):
    first = split is not None
    n_e, dim, wide = w1.shape
    half = w2.shape[1]
    whole = lambda e, ep: (0, 0)
    per_e = lambda e, ep: (e, 0, 0)
    once = dict(pipeline_mode=pl.Buffered(1))
    room = n_e * TILE + TILE
    hbm = pl.BlockSpec(memory_space=pl.ANY)
    in_specs = [
        pl.BlockSpec(xa.shape, whole, **once),
        pl.BlockSpec(xb.shape, whole, **once),
        pl.BlockSpec((1, dim, wide), per_e),
        pl.BlockSpec((1, half, dim), per_e),
        pl.BlockSpec((1, 1, wide), per_e),
        pl.BlockSpec((1, 1, dim), per_e),
    ]
    out_specs = [
        pl.BlockSpec((2 * toks, dim), whole, **once),
        pl.BlockSpec((2 * toks, dim), whole, **once),
        pl.BlockSpec((1, 2, toks), per_e),
        pl.BlockSpec((1, 1, wide), per_e),
        pl.BlockSpec((1, 1, dim), per_e),
        pl.BlockSpec(memory_space=pltpu.SMEM),
    ]
    shape = jax.ShapeDtypeStruct
    out_shape = [
        shape((2 * toks, dim), BF), shape((2 * toks, dim), BF), shape((n_e, 2, toks), F32),
        shape((n_e, 1, wide), F32), shape((n_e, 1, dim), F32), shape((n_e,), jnp.int32),
    ]
    if first:
        in_specs.append(pl.BlockSpec((wide, wide), whole))
        out_specs.append(pl.BlockSpec((1, dim, wide), per_e))
        out_shape.append(shape((n_e, dim, wide), BF))
    out_specs += [hbm] * 4
    out_shape += [shape((n_e, 2, TILE, w), BF) for w in (dim, dim, wide, half)]
    got = pl.pallas_call(
        functools.partial(chunk_kernel, first, toks),
        grid_spec=pltpu.PrefetchScalarGridSpec(
            num_scalar_prefetch=1,
            grid=(n_e,),
            in_specs=in_specs,
            out_specs=out_specs,
            scratch_shapes=[
                pltpu.VMEM((2, xa.shape[0] - 2 * toks, dim), F32),
                pltpu.VMEM((2, 2 * TILE, dim), BF),
                pltpu.VMEM((2, 2 * TILE, dim), BF),
                pltpu.VMEM((2, 2 * TILE, wide), BF),
                pltpu.VMEM((2, 2 * TILE, half), BF),
                pltpu.VMEM((2 * TILE, 1), F32),
                pltpu.VMEM((2 * TILE, 1), F32),
                pltpu.VMEM((2 * TILE, dim), BF),
                pltpu.VMEM((2 * TILE, dim), BF),
                pltpu.VMEM((2, room, toks), BF),
                pltpu.VMEM((2, room, dim), BF),
                pltpu.VMEM((2, room, dim), BF),
                pltpu.VMEM((toks, dim), F32),
                pltpu.SMEM((2,), jnp.int32),
                pltpu.SemaphoreType.DMA((2, 2, 4)),
            ],
        ),
        out_shape=out_shape,
        compiler_params=pltpu.CompilerParams(dimension_semantics=('arbitrary',), vmem_limit_bytes=65000 * 1024),
        cost_estimate=pl.CostEstimate(flops=28_000_000_000, bytes_accessed=40_000_000, transcendentals=0),
        name='experts',
    )(ep, xa, xb, w1, w2, b1, b2, *((split,) if first else ()))
    oa, ob, dg, gb1, gb2, nt = got[:6]
    return oa, ob, dg, gb1, gb2, nt, got[-4:], (got[6] if first else w1)


def wgrad_kernel(n_c, first_e, n_prev, nt_ref, *refs):
    hbm = [refs[k * n_c:(k + 1) * n_c] for k in range(4)]
    mix_ref = refs[4 * n_c]
    gw1_ref, gw2_ref, acc1, acc2, *bufs, sems = refs[4 * n_c + 1 + n_prev:]
    e = pl.program_id(0)
    n_e = pl.num_programs(0)
    par = lax.rem(e, 2)

    def fetches(step, c, t, p):
        return [pltpu.make_async_copy(hbm[k][c].at[first_e + step, t], bufs[k].at[p, 2 * c + t], sems.at[p, 2 * c + t, k])
                for k in range(4)]

    def each(step, act):
        for c in range(n_c):
            for t in range(2):
                pl.when(nt_ref[c, first_e + step] > t)(functools.partial(act, c, t))

    def start(step, p):
        def go(c, t):
            for copy in fetches(step, c, t, p):
                copy.start()
        each(step, go)

    @pl.when(e == 0)
    def _():
        start(e, par)

    @pl.when(e + 1 < n_e)
    def _():
        start(e + 1, 1 - par)

    acc1[...] = jnp.zeros_like(acc1)
    acc2[...] = jnp.zeros_like(acc2)

    def add(c, t):
        for copy in fetches(e, c, t, par):
            copy.wait()
        x_rows, d_rows, d_hid, act_w = (buf[par, 2 * c + t] for buf in bufs)
        acc1[...] += dot(x_rows, d_hid, LHS)
        acc2[...] += dot(act_w, d_rows, LHS)

    each(e, add)
    gw2_ref[0] = acc2[...].astype(BF)
    gw1_ref[0] = dot(acc1[...].astype(BF), mix_ref[...]).astype(BF)


def run_wgrad(nt, saved, unmix, first_e, n_e, all_e, prev=()):
    n_c = len(saved)
    xs, ds, dh, wa = (list(t) for t in zip(*saved))
    dim, wide, half = xs[0].shape[3], dh[0].shape[3], wa[0].shape[3]
    return pl.pallas_call(
        functools.partial(wgrad_kernel, n_c, first_e, len(prev)),
        grid_spec=pltpu.PrefetchScalarGridSpec(
            num_scalar_prefetch=1,
            grid=(n_e,),
            in_specs=[pl.BlockSpec(memory_space=pl.ANY)] * (4 * n_c) + [pl.BlockSpec((wide, wide), lambda e, nt: (0, 0))]
            + [pl.BlockSpec(memory_space=pl.ANY)] * len(prev),
            out_specs=[pl.BlockSpec((1, dim, wide), lambda e, nt: (first_e + e, 0, 0)), pl.BlockSpec((1, half, dim), lambda e, nt: (first_e + e, 0, 0))],
            scratch_shapes=[pltpu.VMEM((dim, wide), F32), pltpu.VMEM((half, dim), F32)]
            + [pltpu.VMEM((2, 2 * n_c, TILE, w), BF) for w in (dim, dim, wide, half)]
            + [pltpu.SemaphoreType.DMA((2, 2 * n_c, 4))],
        ),
        out_shape=[jax.ShapeDtypeStruct((all_e, dim, wide), BF), jax.ShapeDtypeStruct((all_e, half, dim), BF)],
        input_output_aliases={4 * n_c + 2 + k: k for k in range(len(prev))},
        compiler_params=pltpu.CompilerParams(dimension_semantics=('arbitrary',), vmem_limit_bytes=64000 * 1024),
        cost_estimate=pl.CostEstimate(flops=26_000_000_000, bytes_accessed=60_000_000, transcendentals=0),
        name='weight_grads',
    )(nt, *xs, *ds, *dh, *wa, unmix, *prev)


def pack_kernel(x_ref, d_ref, idx_ref, slot_ref, wr_ref, br_ref, load_ref, w_ref):
    toks = x_ref.shape[0]
    top_k, n = idx_ref.shape[0], wr_ref.shape[1]
    logits = lax.dot_general(wr_ref[...], x_ref[...], (((0,), (1,)), ((), ())), preferred_element_type=F32) + br_ref[...]
    expert = lax.broadcasted_iota(jnp.int32, (n, toks), 0)
    hots = [jnp.broadcast_to(idx_ref[k:k + 1, :], (n, toks)) == expert for k in range(top_k)]
    picked = [jnp.sum(jnp.where(h, logits, 0.0), axis=0, keepdims=True) for h in hots]
    top = functools.reduce(jnp.maximum, picked)
    exps = [jnp.exp(v - top) for v in picked]
    norm = functools.reduce(jnp.add, exps)
    w_full = jnp.zeros((n, toks), F32)
    kept = jnp.zeros((n, toks), F32)
    for k in range(top_k):
        w_full += jnp.where(hots[k], exps[k] / norm, 0.0)
        kept += jnp.where(hots[k], jnp.where(slot_ref[k:k + 1, :] >= 0, 1.0, 0.0), 0.0)
    w_ref[...] = w_full
    ahead = lax.broadcasted_iota(jnp.int32, (toks, toks), 0) < lax.broadcasted_iota(jnp.int32, (toks, toks), 1)
    rank = dot(kept.astype(BF), jnp.where(ahead, 1.0, 0.0).astype(BF))
    rank = jnp.where(kept > 0.0, rank, -1.0)
    w_top = w_full.astype(BF)
    rest = w_full - w_top.astype(F32)
    w_mid = rest.astype(BF)
    w_low = (rest - w_mid.astype(F32)).astype(BF)
    load_ref[:toks, :] = x_ref[...]
    load_ref[toks:2 * toks, :] = d_ref[...]
    load_ref[2 * toks:2 * toks + n, :toks] = w_top
    load_ref[2 * toks:2 * toks + n, toks:] = w_mid
    load_ref[2 * toks + n:, :toks] = w_low
    load_ref[2 * toks + n:, toks:] = rank.astype(BF)


def run_pack(x_loc, dy_loc, idx_t, slot_t, w_router, b_router):
    toks, dim = x_loc.shape
    n = w_router.shape[1]
    return pl.pallas_call(
        pack_kernel,
        out_shape=[jax.ShapeDtypeStruct((2 * toks + 2 * n, dim), BF), jax.ShapeDtypeStruct((n, toks), F32)],
        compiler_params=pltpu.CompilerParams(vmem_limit_bytes=32000 * 1024),
        name='pack',
    )(x_loc, dy_loc, idx_t, slot_t, w_router, b_router)


def solution(mesh):
    tp_count = mesh.shape['tp']
    ep_count = mesh.shape['ep']
    n_dev = tp_count * ep_count
    tok_spec = P(('ep', 'tp'), None)

    CORE, XF, YF = 2, 4, 1
    CHIPS = (0, XF, YF, XF | YF)

    def flip(arr, bits):
        turned = (bits & 1) * ep_count + (bits >> 1)
        return lax.ppermute(arr, ('tp', 'ep'), [(s, s ^ turned) for s in range(n_dev)])

    def device_fn(x_loc, idx_loc, slot_loc, w_router, b_router, w_gate_up, b_gate_up, w_down, b_down, dy_loc):
        toks, dim = x_loc.shape
        n_experts = w_router.shape[1]
        n_e = w_gate_up.shape[0]
        wide = w_gate_up.shape[2]
        half = wide // 2
        tp_index = lax.axis_index('tp')
        ep_index = lax.axis_index('ep')
        me = ep_index * tp_count + tp_index

        load, w_full = run_pack(x_loc, dy_loc, idx_loc.T, slot_loc.T, w_router, b_router[:, None])

        from_x, from_y = flip(load, XF), flip(load, YF)
        from_far = flip(from_x, YF)
        pairs = [(bits, got, flip(got, CORE)) for bits, got in zip(CHIPS, (load, from_x, from_y, from_far))]

        col = jnp.arange(wide)
        split_mat = (jnp.where(col < half, 2 * col, 2 * (col - half) + 1)[None, :] == col[:, None]).astype(BF)
        b1 = jnp.concatenate([b_gate_up[:, 0::2], b_gate_up[:, 1::2]], axis=1)[:, None, :]
        b2 = (b_down * (tp_index == 0).astype(F32))[:, None, :]
        ep = ep_index.astype(jnp.int32)[None]

        w1 = w_gate_up
        outs, dgs, gb1s, gb2s, nts, saved = [], [], [], [], [], []
        pending = []

        def hop():
            bits, oa_p, theirs = pending.pop(0)
            return bits, (oa_p.astype(F32) + theirs.astype(F32)).astype(BF)

        for step, (bits, xa, xb) in enumerate(pairs):
            if len(pending) == 2:
                b, mine = hop()
                mine, xa = lax.optimization_barrier((mine, xa))
                outs.append(flip(mine, b))
            oa, ob, dg, gb1, gb2, nt, keep, w1 = run_chunk(
                ep, xa, xb, w1, w_down, b1, b2, toks, split_mat if step == 0 else None)
            if bits:
                pending.append((bits, oa, flip(ob, CORE)))
            else:
                own = (oa, flip(ob, CORE))
            dgs.append(dg)
            gb1s.append(gb1)
            gb2s.append(gb2)
            nts.append(nt)
            saved.append(keep)

        rel = [CHIPS[k // 2] ^ (CORE * (k % 2)) for k in range(n_dev)]
        dg_rel = jnp.stack([dg[:, k, :] for dg in dgs for k in range(2)])
        slot_of = jnp.array([rel.index(m) for m in range(n_dev)], jnp.int32)
        dg_abs = dg_rel[slot_of[jnp.arange(n_dev) ^ me]]
        dg_back = lax.all_to_all(dg_abs, ('ep', 'tp'), 0, 0, tiled=True)
        b, mine_y = hop()
        d_gate = jnp.sum(dg_back.reshape(ep_count, tp_count, n_e, toks), axis=1).reshape(n_experts, toks)
        d_logits = w_full * (d_gate - jnp.sum(w_full * d_gate, axis=0, keepdims=True))
        d_all = lax.all_gather(d_logits, ('ep', 'tp'))
        mine_y, d_all = lax.optimization_barrier((mine_y, d_all))
        outs.append(flip(mine_y, b))
        b, mine_f = hop()
        mine_f, d_all, nt_all = lax.optimization_barrier((mine_f, d_all, jnp.stack(nts)))
        outs.append(flip(mine_f, b))

        unmix = split_mat.T
        part_e = n_e // 2
        grads = run_wgrad(nt_all, saved, unmix, 0, part_e, n_e)
        gw1, gw2 = run_wgrad(nt_all, saved, unmix, part_e, n_e - part_e, n_e, grads)
        gb1 = functools.reduce(jnp.add, gb1s)[:, 0, :]
        gb1 = jnp.stack([gb1[:, :half], gb1[:, half:]], axis=2).reshape(n_e, wide)
        gb2 = functools.reduce(jnp.add, gb2s)[:, 0, :]

        d_all_b = d_all.astype(BF)
        gwr = 0.0
        for k, (_, xa, xb) in enumerate(pairs):
            for i, rows in enumerate((xa, xb)):
                gwr = gwr + jnp.einsum('td,et->de', rows[:toks], d_all_b[me ^ rel[2 * k + i]], preferred_element_type=F32)
        gbr = jnp.sum(d_all, axis=(0, 2))
        total = functools.reduce(jnp.add, [o.astype(F32) for o in (*own, *outs)])
        d_x = total[toks:] + jnp.einsum('et,de->td', d_logits.astype(BF), w_router, preferred_element_type=F32)
        return (total[:toks].astype(BF), d_x.astype(BF), gw1, gb1, gw2, gb2, gwr, gbr)

    in_specs = (tok_spec, tok_spec, tok_spec, P(None, None), P(None), P('ep', None, 'tp'), P('ep', 'tp'), P('ep', 'tp', None), P('ep', None), tok_spec)
    out_specs = (tok_spec, tok_spec, P('ep', None, 'tp'), P('ep', 'tp'), P('ep', 'tp', None), P('ep', None), P(None, None), P(None))
    return jax.shard_map(device_fn, mesh=mesh, in_specs=in_specs, out_specs=out_specs, check_vma=False)
```

```python
import functools
import jax
import jax.numpy as jnp
from jax import lax
from jax.experimental import pallas as pl
from jax.experimental.pallas import tpu as pltpu
from jax.sharding import PartitionSpec as P

LIMIT = 7.0
ALPHA = 1.702
BF = jnp.bfloat16
F32 = jnp.float32
TILE = 256
SIZES = (128, 256)
BACK = ((1,), (1,))
LHS = ((0,), (0,))


def dot(a, b, dims=((1,), (0,))):
    return lax.dot_general(a, b, (dims, ((), ())), preferred_element_type=F32)


def chunk_kernel(first, toks, ep_ref, xa_hbm, da_hbm, xb_hbm, db_hbm, w1_in, w2_ref, b1_ref, b2_ref, *refs):
    if first:
        split_ref, *refs = refs
    ya_hbm, dxa_hbm, yb_hbm, dxb_hbm, dg_ref, gb1_ref, gb2_ref, nt_ref, *refs = refs
    if first:
        w1_ref, *refs = refs
    else:
        w1_ref = w1_in
    xs_hbm, ds_hbm, dh_hbm, wa_hbm, *refs = refs
    xin, din, ost, aux, xbuf, dbuf, dhst, wast, wrow, dgrow, yst, dxst, sel, ybuf, dxbuf, acc, off, sems, io_sems = refs
    e = pl.program_id(0)
    n_e = pl.num_programs(0)
    half = w2_ref.shape[1]
    par = lax.rem(e, 2)
    loads = [[pltpu.make_async_copy(x_h, xin.at[i], io_sems.at[i, 0]), pltpu.make_async_copy(d_h, din.at[i], io_sems.at[i, 1])]
             for i, (x_h, d_h) in enumerate(((xa_hbm, da_hbm), (xb_hbm, db_hbm)))]
    stores = [[pltpu.make_async_copy(ost.at[i, k], o_h, io_sems.at[i, k]) for k, o_h in enumerate(pair)]
              for i, pair in enumerate(((ya_hbm, dxa_hbm), (yb_hbm, dxb_hbm)))]

    def saves(expert, t, p):
        at = pl.ds(t * TILE, TILE)
        pairs = ((xbuf, xs_hbm), (dbuf, ds_hbm), (dhst, dh_hbm), (wast, wa_hbm))
        return [pltpu.make_async_copy(src.at[p, at], dst.at[expert, t], sems.at[p, t, k])
                for k, (src, dst) in enumerate(pairs)]

    def drain(expert, p):
        for t in range(2):
            @pl.when(nt_ref[expert] > t)
            def _():
                for copy in saves(expert, t, p):
                    copy.wait()

    @pl.when(e == 0)
    def _():
        for i in range(2):
            for copy in reversed(loads[i]):
                copy.start()
        for i in range(2):
            off[i] = 0
            xbuf[i] = jnp.zeros(xbuf.shape[1:], BF)
            dbuf[i] = jnp.zeros(dbuf.shape[1:], BF)
        yst[...] = jnp.zeros_like(yst)
        dxst[...] = jnp.zeros_like(dxst)

    for p in range(2):
        @pl.when((e >= 2) & (par == p))
        def _():
            drain(e - 2, p)

    if first:
        w1_ref[0] = dot(w1_in[0], split_ref[...]).astype(BF)

    @pl.when(e == 0)
    def _():
        for i in range(2):
            for copy in reversed(loads[i]):
                copy.wait()
            aux[i] = din[i, toks:, :].astype(F32)

    row = ep_ref[0] * n_e + e
    wrow[...] = jnp.zeros_like(wrow)
    ranks, counts = [], []
    for i in range(2):
        rk = aux[i, pl.ds(row + 4 * n_e, 1), :][:, toks:]
        ranks.append(rk)
        counts.append((jnp.max(rk) + 1.0).astype(jnp.int32))
    starts = (0, pl.multiple_of((counts[0] + 15) // 16 * 16, 16))
    n_tiles = (starts[1] + counts[1] + TILE - 1) // TILE
    nt_ref[e] = n_tiles

    def place(i, m):
        pair = aux[i, pl.ds(row, 1), :]
        low = aux[i, pl.ds(row + 4 * n_e, 1), :]
        wv = pair[:, :toks] + pair[:, toks:] + low[:, :toks]
        pos = lax.broadcasted_iota(jnp.int32, (m, toks), 0).astype(F32)
        hot = jnp.broadcast_to(ranks[i], (m, toks)) == pos
        hot_b = jnp.where(hot, 1.0, 0.0).astype(BF)
        at = pl.ds(starts[i], m)
        wrow[at, :] = jnp.sum(jnp.where(hot, jnp.broadcast_to(wv, (m, toks)), 0.0), axis=1, keepdims=True)
        xbuf[par, at, :] = dot(hot_b, xin[i]).astype(BF)
        dbuf[par, at, :] = dot(hot_b, din[i, :toks, :]).astype(BF)
        sel[i, pl.ds(pl.multiple_of(off[i], 128), m), :] = hot_b

    for i in range(2):
        low = 0
        for m in SIZES:
            pl.when((counts[i] > low) & (counts[i] <= m))(functools.partial(place, i, m))
            low = m

    gb1_ref[...] = jnp.zeros_like(gb1_ref)
    gb2_ref[...] = jnp.zeros_like(gb2_ref)

    def tile(t, _):
        at = pl.ds(pl.multiple_of(t * TILE, TILE), TILE)
        x_rows = xbuf[par, at, :]
        d_rows = dbuf[par, at, :]
        w_row = wrow[at, :]
        hid = dot(x_rows, w1_ref[0]) + b1_ref[0]
        d_act = w_row * dot(d_rows, w2_ref[0], BACK)
        gate, up = hid[:, :half], hid[:, half:]
        g = jnp.minimum(gate, LIMIT)
        u1 = jnp.clip(up, -LIMIT, LIMIT) + 1.0
        sg = jax.nn.sigmoid(ALPHA * g)
        gs = g * sg
        act = (gs * u1).astype(BF)
        part = (dot(act, w2_ref[0]) + b2_ref[0]).astype(BF).astype(F32)
        gate_on = jnp.where(gate < LIMIT, 1.0, jnp.where(gate == LIMIT, 0.5, 0.0))
        up_abs = jnp.abs(up)
        up_on = jnp.where(up_abs < LIMIT, 1.0, jnp.where(up_abs == LIMIT, 0.5, 0.0))
        d_gate = d_act * u1 * (sg * (1.0 + ALPHA * g * (1.0 - sg))) * gate_on
        d_up = d_act * gs * up_on
        d_hid = jnp.concatenate([d_gate, d_up], axis=1)
        gb1_ref[0] += jnp.sum(d_hid, axis=0, keepdims=True)
        d_hid_b = d_hid.astype(BF)
        dhst[par, at, :] = d_hid_b
        wast[par, at, :] = (w_row * act.astype(F32)).astype(BF)
        dxst[at, :] = dot(d_hid_b, w1_ref[0], BACK).astype(BF)
        d_wide = d_rows.astype(F32)
        dgrow[at, :] = jnp.sum(part * d_wide, axis=1, keepdims=True)
        gb2_ref[0] += jnp.sum(w_row * d_wide, axis=0, keepdims=True)
        yst[at, :] = (w_row * part).astype(BF)
        for copy in saves(e, t, par):
            copy.start()
        return 0

    lax.fori_loop(0, n_tiles, tile, 0)

    def collect(i, m):
        src = pl.ds(starts[i], m)
        dst = pl.ds(pl.multiple_of(off[i], 128), m)
        ybuf[i, dst, :] = yst[src, :]
        dxbuf[i, dst, :] = dxst[src, :]
        pos = lax.broadcasted_iota(jnp.int32, (m, toks), 0).astype(F32)
        hot = jnp.broadcast_to(ranks[i], (m, toks)) == pos
        dg_ref[0, i:i + 1, :] = jnp.sum(jnp.where(hot, dgrow[src, :], 0.0), axis=0, keepdims=True)
        off[i] = off[i] + m

    low = 0
    for m in SIZES:
        for i in range(2):
            pl.when((counts[i] > low) & (counts[i] <= m))(functools.partial(collect, i, m))
        low = m
    for i in range(2):
        @pl.when(counts[i] == 0)
        def _():
            dg_ref[0, i:i + 1, :] = jnp.zeros((1, toks), F32)

    @pl.when(e == n_e - 1)
    def _():
        for i in range(2):
            total = pl.multiple_of(off[i], 128)
            for buf in (sel, ybuf, dxbuf):
                buf[i, pl.ds(total, TILE), :] = jnp.zeros((TILE, buf.shape[2]), BF)
            long = 4 * TILE
            done = jnp.where(total >= long, 4, 0)
            tiles = (total + TILE - 1) // TILE
            for k, buf in enumerate((ybuf, dxbuf)):
                @pl.when(total >= long)
                def _():
                    acc[...] = dot(sel[i, :long, :], buf[i, :long, :], LHS)

                @pl.when(total < long)
                def _():
                    acc[...] = jnp.zeros_like(acc)

                def step(j, _):
                    at = pl.ds(pl.multiple_of(j * TILE, TILE), TILE)
                    acc[...] += dot(sel[i, at, :], buf[i, at, :], LHS)
                    return 0

                lax.fori_loop(done, tiles, step, 0)
                ost[i, k] = acc[...].astype(BF)
                stores[i][k].start()
        for back in (1, 0):
            p = lax.rem(e - back, 2)
            drain(e - back, p)
        for i in range(2):
            for copy in stores[i]:
                copy.wait()


def run_chunk(ep, blocks, w1, w2, b1, b2, split=None):
    first = split is not None
    n_e, dim, wide = w1.shape
    half = w2.shape[1]
    toks, tall = blocks[0].shape[0], blocks[1].shape[0]
    whole = lambda e, ep: (0, 0)
    per_e = lambda e, ep: (e, 0, 0)
    room = n_e * TILE + TILE
    hbm = pl.BlockSpec(memory_space=pl.ANY)
    in_specs = [
        hbm, hbm, hbm, hbm,
        pl.BlockSpec((1, dim, wide), per_e),
        pl.BlockSpec((1, half, dim), per_e),
        pl.BlockSpec((1, 1, wide), per_e),
        pl.BlockSpec((1, 1, dim), per_e),
    ]
    out_specs = [
        hbm, hbm, hbm, hbm,
        pl.BlockSpec((1, 2, toks), per_e),
        pl.BlockSpec((1, 1, wide), per_e),
        pl.BlockSpec((1, 1, dim), per_e),
        pl.BlockSpec(memory_space=pltpu.SMEM),
    ]
    shape = jax.ShapeDtypeStruct
    out_shape = [
        *[shape((toks, dim), BF)] * 4, shape((n_e, 2, toks), F32),
        shape((n_e, 1, wide), F32), shape((n_e, 1, dim), F32), shape((n_e,), jnp.int32),
    ]
    if first:
        in_specs.append(pl.BlockSpec((wide, wide), whole))
        out_specs.append(pl.BlockSpec((1, dim, wide), per_e))
        out_shape.append(shape((n_e, dim, wide), BF))
    out_specs += [hbm] * 4
    out_shape += [shape((n_e, 2, TILE, w), BF) for w in (dim, dim, wide, half)]
    got = pl.pallas_call(
        functools.partial(chunk_kernel, first, toks),
        grid_spec=pltpu.PrefetchScalarGridSpec(
            num_scalar_prefetch=1,
            grid=(n_e,),
            in_specs=in_specs,
            out_specs=out_specs,
            scratch_shapes=[
                pltpu.VMEM((2, toks, dim), BF),
                pltpu.VMEM((2, tall, dim), BF),
                pltpu.VMEM((2, 2, toks, dim), BF),
                pltpu.VMEM((2, tall - toks, dim), F32),
                pltpu.VMEM((2, 2 * TILE, dim), BF),
                pltpu.VMEM((2, 2 * TILE, dim), BF),
                pltpu.VMEM((2, 2 * TILE, wide), BF),
                pltpu.VMEM((2, 2 * TILE, half), BF),
                pltpu.VMEM((2 * TILE, 1), F32),
                pltpu.VMEM((2 * TILE, 1), F32),
                pltpu.VMEM((2 * TILE, dim), BF),
                pltpu.VMEM((2 * TILE, dim), BF),
                pltpu.VMEM((2, room, toks), BF),
                pltpu.VMEM((2, room, dim), BF),
                pltpu.VMEM((2, room, dim), BF),
                pltpu.VMEM((toks, dim), F32),
                pltpu.SMEM((2,), jnp.int32),
                pltpu.SemaphoreType.DMA((2, 2, 4)),
                pltpu.SemaphoreType.DMA((2, 2)),
            ],
        ),
        out_shape=out_shape,
        compiler_params=pltpu.CompilerParams(dimension_semantics=('arbitrary',), vmem_limit_bytes=65000 * 1024),
        cost_estimate=pl.CostEstimate(flops=28_000_000_000, bytes_accessed=40_000_000, transcendentals=0),
        name='experts',
    )(ep, *blocks, w1, w2, b1, b2, *((split,) if first else ()))
    return got[:4], got[4:8], got[-4:], (got[8] if first else w1)


def wgrad_kernel(n_c, first_e, n_prev, nt_ref, *refs):
    hbm = [refs[k * n_c:(k + 1) * n_c] for k in range(4)]
    mix_ref = refs[4 * n_c]
    gw1_ref, gw2_ref, acc1, acc2, *bufs, sems = refs[4 * n_c + 1 + n_prev:]
    e = pl.program_id(0)
    n_e = pl.num_programs(0)
    par = lax.rem(e, 2)

    def fetches(step, c, t, p):
        return [pltpu.make_async_copy(hbm[k][c].at[first_e + step, t], bufs[k].at[p, 2 * c + t], sems.at[p, 2 * c + t, k])
                for k in range(4)]

    def each(step, act):
        for c in range(n_c):
            for t in range(2):
                pl.when(nt_ref[c, first_e + step] > t)(functools.partial(act, c, t))

    def start(step, p):
        def go(c, t):
            for copy in fetches(step, c, t, p):
                copy.start()

        each(step, go)

    @pl.when(e == 0)
    def _():
        start(e, par)

    @pl.when(e + 1 < n_e)
    def _():
        start(e + 1, 1 - par)

    acc1[...] = jnp.zeros_like(acc1)
    acc2[...] = jnp.zeros_like(acc2)

    def add(c, t):
        for copy in fetches(e, c, t, par):
            copy.wait()
        x_rows, d_rows, d_hid, act_w = (buf[par, 2 * c + t] for buf in bufs)
        acc1[...] += dot(x_rows, d_hid, LHS)
        acc2[...] += dot(act_w, d_rows, LHS)

    each(e, add)
    gw2_ref[0] = acc2[...].astype(BF)
    gw1_ref[0] = dot(acc1[...].astype(BF), mix_ref[...]).astype(BF)


def run_wgrad(nt, saved, unmix, first_e, n_e, all_e, prev=()):
    n_c = len(saved)
    xs, ds, dh, wa = (list(t) for t in zip(*saved))
    dim, wide, half = xs[0].shape[3], dh[0].shape[3], wa[0].shape[3]
    return pl.pallas_call(
        functools.partial(wgrad_kernel, n_c, first_e, len(prev)),
        grid_spec=pltpu.PrefetchScalarGridSpec(
            num_scalar_prefetch=1,
            grid=(n_e,),
            in_specs=[pl.BlockSpec(memory_space=pl.ANY)] * (4 * n_c) + [pl.BlockSpec((wide, wide), lambda e, nt: (0, 0))]
            + [pl.BlockSpec(memory_space=pl.ANY)] * len(prev),
            out_specs=[pl.BlockSpec((1, dim, wide), lambda e, nt: (first_e + e, 0, 0)), pl.BlockSpec((1, half, dim), lambda e, nt: (first_e + e, 0, 0))],
            scratch_shapes=[pltpu.VMEM((dim, wide), F32), pltpu.VMEM((half, dim), F32)]
            + [pltpu.VMEM((2, 2 * n_c, TILE, w), BF) for w in (dim, dim, wide, half)]
            + [pltpu.SemaphoreType.DMA((2, 2 * n_c, 4))],
        ),
        out_shape=[jax.ShapeDtypeStruct((all_e, dim, wide), BF), jax.ShapeDtypeStruct((all_e, half, dim), BF)],
        input_output_aliases={4 * n_c + 2 + k: k for k in range(len(prev))},
        compiler_params=pltpu.CompilerParams(dimension_semantics=('arbitrary',), vmem_limit_bytes=64000 * 1024),
        cost_estimate=pl.CostEstimate(flops=26_000_000_000, bytes_accessed=60_000_000, transcendentals=0),
        name='weight_grads',
    )(nt, *xs, *ds, *dh, *wa, unmix, *prev)


def pack_kernel(x_ref, d_ref, idx_ref, slot_ref, wr_ref, br_ref, tall_ref, w_ref):
    toks = x_ref.shape[0]
    top_k, n = idx_ref.shape[0], wr_ref.shape[1]
    logits = lax.dot_general(wr_ref[...], x_ref[...], (((0,), (1,)), ((), ())), preferred_element_type=F32) + br_ref[...]
    expert = lax.broadcasted_iota(jnp.int32, (n, toks), 0)
    hots = [jnp.broadcast_to(idx_ref[k:k + 1, :], (n, toks)) == expert for k in range(top_k)]
    picked = [jnp.sum(jnp.where(h, logits, 0.0), axis=0, keepdims=True) for h in hots]
    top = functools.reduce(jnp.maximum, picked)
    exps = [jnp.exp(v - top) for v in picked]
    norm = functools.reduce(jnp.add, exps)
    w_full = jnp.zeros((n, toks), F32)
    kept = jnp.zeros((n, toks), F32)
    for k in range(top_k):
        w_full += jnp.where(hots[k], exps[k] / norm, 0.0)
        kept += jnp.where(hots[k], jnp.where(slot_ref[k:k + 1, :] >= 0, 1.0, 0.0), 0.0)
    w_ref[...] = w_full
    ahead = lax.broadcasted_iota(jnp.int32, (toks, toks), 0) < lax.broadcasted_iota(jnp.int32, (toks, toks), 1)
    rank = dot(kept.astype(BF), jnp.where(ahead, 1.0, 0.0).astype(BF))
    rank = jnp.where(kept > 0.0, rank, -1.0)
    w_top = w_full.astype(BF)
    rest = w_full - w_top.astype(F32)
    w_mid = rest.astype(BF)
    w_low = (rest - w_mid.astype(F32)).astype(BF)
    tall_ref[:toks, :] = d_ref[...]
    tall_ref[toks:toks + n, :toks] = w_top
    tall_ref[toks:toks + n, toks:] = w_mid
    tall_ref[toks + n:, :toks] = w_low
    tall_ref[toks + n:, toks:] = rank.astype(BF)


def run_pack(x_loc, dy_loc, idx_t, slot_t, w_router, b_router):
    toks, dim = x_loc.shape
    n = w_router.shape[1]
    return pl.pallas_call(
        pack_kernel,
        out_shape=[jax.ShapeDtypeStruct((toks + 2 * n, dim), BF), jax.ShapeDtypeStruct((n, toks), F32)],
        compiler_params=pltpu.CompilerParams(vmem_limit_bytes=32000 * 1024),
        name='pack',
    )(x_loc, dy_loc, idx_t, slot_t, w_router, b_router)


def router_kernel(rel, me_ref, *refs):
    n = len(rel)
    d_ref, out_ref = refs[n:]
    total = jnp.zeros(out_ref.shape, F32)
    for k in range(n):
        d_one = d_ref[me_ref[0] ^ rel[k]].astype(BF)
        total += lax.dot_general(refs[k][...], d_one, (((0,), (1,)), ((), ())), preferred_element_type=F32)
    out_ref[...] = total


def run_router_grad(me, rel, x_blocks, d_rel):
    n = len(x_blocks)
    toks, dim = x_blocks[0].shape
    experts = d_rel.shape[1]
    cut = dim // 4
    return pl.pallas_call(
        functools.partial(router_kernel, rel),
        grid_spec=pltpu.PrefetchScalarGridSpec(
            num_scalar_prefetch=1,
            grid=(4,),
            in_specs=[pl.BlockSpec((toks, cut), lambda j, me: (0, j))] * n + [pl.BlockSpec(d_rel.shape, lambda j, me: (0, 0, 0))],
            out_specs=pl.BlockSpec((cut, experts), lambda j, me: (j, 0)),
        ),
        out_shape=jax.ShapeDtypeStruct((dim, experts), F32),
        compiler_params=pltpu.CompilerParams(vmem_limit_bytes=32000 * 1024),
        name='router_grad',
    )(me, *x_blocks, d_rel)


def solution(mesh):
    tp_count = mesh.shape['tp']
    ep_count = mesh.shape['ep']
    n_dev = tp_count * ep_count
    tok_spec = P(('ep', 'tp'), None)

    CORE, XF, YF = 2, 4, 1
    FAR = XF | YF
    CHIPS = (0, YF, FAR, XF)

    def flip(arr, bits):
        turned = (bits & 1) * ep_count + (bits >> 1)
        return lax.ppermute(arr, ('tp', 'ep'), [(s, s ^ turned) for s in range(n_dev)])

    def device_fn(x_loc, idx_loc, slot_loc, w_router, b_router, w_gate_up, b_gate_up, w_down, b_down, dy_loc):
        toks, _ = x_loc.shape
        n_experts = w_router.shape[1]
        n_e = w_gate_up.shape[0]
        wide = w_gate_up.shape[2]
        half = wide // 2
        tp_index = lax.axis_index('tp')
        ep_index = lax.axis_index('ep')
        me = ep_index * tp_count + tp_index

        tall, w_full = run_pack(x_loc, dy_loc, idx_loc.T, slot_loc.T, w_router, b_router[:, None])

        x_of = {XF: flip(x_loc, XF), YF: flip(x_loc, YF)}
        d_of = {XF: flip(tall, XF | CORE), YF: flip(tall, YF | CORE)}
        x_of[FAR] = flip(x_of[XF], YF)
        d_of[FAR] = flip(d_of[YF], XF)
        pairs = [(x_loc, tall, flip(x_loc, CORE), flip(tall, CORE))]
        for bits in CHIPS[1:]:
            pairs.append((x_of[bits], flip(d_of[bits], CORE), flip(x_of[bits], CORE), d_of[bits]))

        col = jnp.arange(wide)
        split_mat = (jnp.where(col < half, 2 * col, 2 * (col - half) + 1)[None, :] == col[:, None]).astype(BF)
        b1 = jnp.concatenate([b_gate_up[:, 0::2], b_gate_up[:, 1::2]], axis=1)[:, None, :]
        b2 = (b_down * (tp_index == 0).astype(F32))[:, None, :]
        ep = ep_index.astype(jnp.int32)[None]

        w1 = w_gate_up
        dgs, gb1s, gb2s, nts, saved, part = [], [], [], [], [], []

        def chunk(step, blocks, w1):
            o, small, keep, w1 = run_chunk(ep, blocks, w1, w_down, b1, b2, split_mat if step == 0 else None)
            for lst, v in zip((dgs, gb1s, gb2s, nts), small):
                lst.append(v)
            saved.append(keep)
            ya, dxa, yb, dxb = o
            if step == 0:
                part.append((ya, flip(yb, CORE), dxa, flip(dxb, CORE)))
            else:
                part.append((ya, flip(yb, CORE), dxb, flip(dxa, CORE)))
            return w1

        def both(step):
            ya, yb, dxa, dxb = part[step]
            add = lambda a, b: (a.astype(F32) + b.astype(F32)).astype(BF)
            return add(ya, yb), add(dxa, dxb)

        def hop(step, y, dx):
            bits = CHIPS[step]
            return flip(y, bits), flip(dx, bits | CORE)

        w1 = chunk(0, pairs[0], w_gate_up)
        w1 = chunk(1, pairs[1], w1)
        w1 = chunk(2, pairs[2], w1)
        sum_1, sum_2 = both(1), both(2)
        sum_1, sum_2, last = lax.optimization_barrier((sum_1, sum_2, pairs[3]))
        got_1, got_2 = hop(1, *sum_1), hop(2, *sum_2)
        chunk(3, last, w1)

        rel = [CHIPS[k // 2] ^ (CORE * (k % 2)) for k in range(n_dev)]
        dg_rel = jnp.stack([dg[:, k, :] for dg in dgs for k in range(2)])
        slot_of = jnp.array([rel.index(m) for m in range(n_dev)], jnp.int32)
        dg_abs = dg_rel[slot_of[jnp.arange(n_dev) ^ me]]
        dg_back = lax.all_to_all(dg_abs, ('ep', 'tp'), 0, 0, tiled=True)
        sum_3, nt_all = lax.optimization_barrier((both(3), jnp.stack(nts)))
        got_3 = hop(3, *sum_3)

        unmix = split_mat.T
        part_e = n_e // 2
        grads = run_wgrad(nt_all, saved, unmix, 0, part_e, n_e)
        dg_back, nt_all, grads = lax.optimization_barrier((dg_back, nt_all, grads))
        d_gate = jnp.sum(dg_back.reshape(ep_count, tp_count, n_e, toks), axis=1).reshape(n_experts, toks)
        d_logits = w_full * (d_gate - jnp.sum(w_full * d_gate, axis=0, keepdims=True))
        gw1, gw2 = run_wgrad(nt_all, saved, unmix, part_e, n_e - part_e, n_e, grads)
        gb1 = functools.reduce(jnp.add, gb1s)[:, 0, :]
        gb1 = jnp.stack([gb1[:, :half], gb1[:, half:]], axis=2).reshape(n_e, wide)
        gb2 = functools.reduce(jnp.add, gb2s)[:, 0, :]

        wide_sum = lambda *terms: functools.reduce(jnp.add, [t.astype(F32) for t in terms])
        y_most = wide_sum(part[0][0], part[0][1], got_1[0], got_2[0])
        dx_most = wide_sum(part[0][2], part[0][3], got_1[1], got_2[1])
        dx_most = dx_most + jnp.einsum('et,de->td', d_logits.astype(BF), w_router, preferred_element_type=F32)
        d_logits, gw1, y_most, dx_most = lax.optimization_barrier((d_logits, gw1, y_most, dx_most))
        d_all = lax.all_gather(d_logits, ('ep', 'tp'))
        gwr = run_router_grad(me.astype(jnp.int32)[None], rel, [p[k] for p in pairs for k in (0, 2)], d_all)
        gbr = jnp.sum(d_all, axis=(0, 2))
        return (wide_sum(y_most, got_3[0]).astype(BF), wide_sum(dx_most, got_3[1]).astype(BF), gw1, gb1, gw2, gb2, gwr, gbr)

    in_specs = (tok_spec, tok_spec, tok_spec, P(None, None), P(None), P('ep', None, 'tp'), P('ep', 'tp'), P('ep', 'tp', None), P('ep', None), tok_spec)
    out_specs = (tok_spec, tok_spec, P('ep', None, 'tp'), P('ep', 'tp'), P('ep', 'tp', None), P('ep', None), P(None, None), P(None))

    return jax.shard_map(device_fn, mesh=mesh, in_specs=in_specs, out_specs=out_specs, check_vma=False)
```

```python
import functools
import jax
import jax.numpy as jnp
from jax import lax
from jax.experimental import pallas as pl
from jax.experimental.pallas import tpu as pltpu
from jax.sharding import PartitionSpec as P

LIMIT = 7.0
ALPHA = 1.702
BF = jnp.bfloat16
F32 = jnp.float32
TILE = 256
BACK = ((1,), (1,))
LHS = ((0,), (0,))


def dot(a, b, dims=((1,), (0,))):
    return lax.dot_general(a, b, (dims, ((), ())), preferred_element_type=F32)


def split3(v):
    top = v.astype(BF)
    rest = v - top.astype(F32)
    mid = rest.astype(BF)
    return top, mid, (rest - mid.astype(F32)).astype(BF)


def chunk_kernel(first, toks, ep_ref, xa_hbm, da_hbm, xb_hbm, db_hbm, w1_in, w2_ref, b1_ref, b2_ref, *refs):
    if first:
        split_ref, *refs = refs
    ya_hbm, dxa_hbm, yb_hbm, dxb_hbm, dg_ref, gb1_ref, gb2_ref, nt_ref, *refs = refs
    if first:
        w1_ref, *refs = refs
    else:
        w1_ref = w1_in
    xs_hbm, ds_hbm, dh_hbm, wa_hbm, *refs = refs
    xin, din, ost, wst, rst, bst, xbuf, dbuf, dhst, wast, sel, zbuf, acc, off, sems, io_sems = refs
    e = pl.program_id(0)
    n_e = pl.num_programs(0)
    half, dim = w2_ref.shape[1:]
    par = lax.rem(e, 2)
    cuts = [slice(j, j + TILE) for j in range(0, dim, TILE)]
    loads = [[pltpu.make_async_copy(x_h, xin.at[i], io_sems.at[i, 0]), pltpu.make_async_copy(d_h, din.at[i], io_sems.at[i, 1])]
             for i, (x_h, d_h) in enumerate(((xa_hbm, da_hbm), (xb_hbm, db_hbm)))]
    stores = [[pltpu.make_async_copy(ost.at[i, k], o_h, io_sems.at[i, k]) for k, o_h in enumerate(pair)]
              for i, pair in enumerate(((ya_hbm, dxa_hbm), (yb_hbm, dxb_hbm)))]

    def saves(expert, t, p):
        at = pl.ds(t * TILE, TILE)
        pairs = ((xbuf, xs_hbm), (dbuf, ds_hbm), (dhst, dh_hbm), (wast, wa_hbm))
        return [pltpu.make_async_copy(src.at[p, at], dst.at[expert, t], sems.at[p, t, k])
                for k, (src, dst) in enumerate(pairs)]

    def drain(expert, p):
        for t in range(2):
            @pl.when(nt_ref[expert] > t)
            def _():
                for copy in saves(expert, t, p):
                    copy.wait()

    @pl.when(e == 0)
    def _():
        for i in range(2):
            for copy in reversed(loads[i]):
                copy.start()
            off[i] = 0

    if first:
        w1_ref[0] = dot(w1_in[0], split_ref[...]).astype(BF)

    @pl.when(e == 0)
    def _():
        base = pl.multiple_of(ep_ref[0] * 8, 8)
        b_parts = jnp.concatenate(split3(b2_ref[...]), axis=0)
        for i in range(2):
            for copy in reversed(loads[i]):
                copy.wait()
            aux = din[i, toks:, :].astype(F32)
            n = aux.shape[0] // 2
            wst[i] = aux[:n, :toks] + aux[:n, toks:] + aux[n:, :toks]
            rst[i] = aux[n:, toks:]
            local_w = wst[i, pl.ds(base, 8), :]
            local_r = rst[i, pl.ds(base, 8), :]
            w_parts = jnp.concatenate(split3(jnp.where(local_r >= 0.0, local_w, 0.0)), axis=0)
            d_all = din[i, :toks, :]
            got = dot(w_parts, d_all)
            got = got[:8] + got[8:16] + got[16:]
            if i == 0:
                gb2_ref[...] = got
            else:
                gb2_ref[...] += got
            got = dot(b_parts, d_all, BACK)
            bst[i] = got[:8] + got[8:16] + got[16:]

    for p in range(2):
        @pl.when((e >= 2) & (par == p))
        def _():
            drain(e - 2, p)

    row = ep_ref[0] * n_e + e
    counts = [(jnp.max(rst[i, pl.ds(row, 1), :]) + 1.0).astype(jnp.int32) for i in range(2)]
    gb1_ref[...] = jnp.zeros_like(gb1_ref)
    b_row = b2_ref[pl.ds(e, 1), :]

    def tile(t, parts):
        rows = pl.ds(pl.multiple_of(t * TILE, TILE), TILE)
        hots, w_rows, at = [], [], 0
        for i, m in parts:
            pos = lax.broadcasted_iota(jnp.int32, (m, toks), 0).astype(F32)
            hot = jnp.broadcast_to(rst[i, pl.ds(row, 1), :], (m, toks)) == pos
            hot_b = jnp.where(hot, 1.0, 0.0).astype(BF)
            sel[i, pl.ds(pl.multiple_of(off[i], 128), m), :] = hot_b
            w_rows.append(jnp.sum(jnp.where(hot, jnp.broadcast_to(wst[i, pl.ds(row, 1), :], (m, toks)), 0.0), axis=1, keepdims=True))
            hots.append(hot)
            dst = pl.ds(pl.multiple_of(t * TILE + at, 128), m)
            for c in cuts:
                xbuf[par, dst, c] = dot(hot_b, xin[i, :, c]).astype(BF)
            for c in cuts:
                dbuf[par, dst, c] = dot(hot_b, din[i, :toks, c]).astype(BF)
            at += m
        w_row = jnp.concatenate(w_rows, axis=0)
        x_rows = xbuf[par, rows, :]
        gate = dot(x_rows, w1_ref[0, :, :half]) + b1_ref[0, :, :half]
        up = dot(x_rows, w1_ref[0, :, half:]) + b1_ref[0, :, half:]
        d_raw = dot(dbuf[par, rows, :], w2_ref[0], BACK)
        g = jnp.minimum(gate, LIMIT)
        u1 = jnp.clip(up, -LIMIT, LIMIT) + 1.0
        sg = jax.nn.sigmoid(ALPHA * g)
        gs = g * sg
        act = (gs * u1).astype(BF)
        act_w = act.astype(F32)
        wast[par, rows, :] = (w_row * act_w).astype(BF)
        dg_row = jnp.sum(act_w * d_raw, axis=1, keepdims=True)
        d_act = w_row * d_raw
        gate_on = jnp.where(gate < LIMIT, 1.0, jnp.where(gate == LIMIT, 0.5, 0.0))
        up_abs = jnp.abs(up)
        up_on = jnp.where(up_abs < LIMIT, 1.0, jnp.where(up_abs == LIMIT, 0.5, 0.0))
        d_gate = d_act * u1 * (sg * (1.0 + ALPHA * g * (1.0 - sg))) * gate_on
        d_up = d_act * gs * up_on
        gb1_ref[0, :, :half] += jnp.sum(d_gate, axis=0, keepdims=True)
        gb1_ref[0, :, half:] += jnp.sum(d_up, axis=0, keepdims=True)
        dhst[par, rows, :half] = d_gate.astype(BF)
        dhst[par, rows, half:] = d_up.astype(BF)
        d_hid = dhst[par, rows, :]

        def put(k, c, value):
            at = 0
            for i, m in parts:
                zbuf[k, i, pl.ds(pl.multiple_of(off[i], 128), m), c] = value[at:at + m]
                at += m

        for c in cuts:
            part = (dot(act, w2_ref[0, :, c]) + b_row[:, c]).astype(BF).astype(F32)
            put(0, c, (w_row * part).astype(BF))
        for c in cuts:
            put(1, c, dot(d_hid, w1_ref[0, c, :], BACK).astype(BF))
        for copy in saves(e, t, par):
            copy.start()
        at = 0
        for (i, m), hot in zip(parts, hots):
            dg = jnp.sum(jnp.where(hot, dg_row[at:at + m], 0.0), axis=0, keepdims=True)
            bias = jnp.where(rst[i, pl.ds(row, 1), :] >= 0.0, bst[i, pl.ds(e, 1), :], 0.0)
            dg_ref[0, pl.ds(i, 1), :] = dg + bias
            off[i] = off[i] + m
            at += m

    short = (counts[0] <= TILE // 2) & (counts[1] <= TILE // 2)
    nt_ref[e] = jnp.where(short, 1, 2)

    @pl.when(short)
    def _():
        tile(0, ((0, TILE // 2), (1, TILE // 2)))

    @pl.when(jnp.logical_not(short))
    def _():
        def one(i, _):
            tile(i, ((i, TILE),))
            return 0

        lax.fori_loop(0, 2, one, 0)

    @pl.when(e == n_e - 1)
    def _():
        long = 4 * TILE

        def combine(j):
            i, k = j // 2, lax.rem(j, 2)
            total = pl.multiple_of(off[i], 128)
            acc[...] = dot(sel[i, :long, :], zbuf[k, i, :long, :], LHS)

            def step(q, _):
                at = pl.ds(pl.multiple_of(q * TILE, TILE), TILE)
                acc[...] += dot(sel[i, at, :], zbuf[k, i, at, :], LHS)
                return 0

            lax.fori_loop(4, (total + TILE - 1) // TILE, step, 0)
            ost[i, k] = acc[...].astype(BF)
            return 0

        for i in range(2):
            total = pl.multiple_of(off[i], 128)
            sel[i, pl.ds(total, TILE), :] = jnp.zeros((TILE, toks), BF)
            for k in range(2):
                zbuf[k, i, pl.ds(total, TILE), :] = jnp.zeros((TILE, dim), BF)

        def go(j, _):
            combine(j)
            for q in range(4):
                @pl.when(j == q)
                def _():
                    stores[q // 2][q % 2].start()
            return 0

        lax.fori_loop(0, 4, go, 0)
        for back in (1, 0):
            p = lax.rem(e - back, 2)
            drain(e - back, p)
        for i in range(2):
            for copy in stores[i]:
                copy.wait()


def run_chunk(ep, blocks, w1, w2, b1, b2, split=None):
    first = split is not None
    n_e, dim, wide = w1.shape
    half = w2.shape[1]
    toks, tall = blocks[0].shape[0], blocks[1].shape[0]
    whole = lambda e, ep: (0, 0)
    per_e = lambda e, ep: (e, 0, 0)
    room = n_e * TILE + TILE
    hbm = pl.BlockSpec(memory_space=pl.ANY)
    in_specs = [
        hbm, hbm, hbm, hbm,
        pl.BlockSpec((1, dim, wide), per_e),
        pl.BlockSpec((1, half, dim), per_e),
        pl.BlockSpec((1, 1, wide), per_e),
        pl.BlockSpec((n_e, dim), whole),
    ]
    out_specs = [
        hbm, hbm, hbm, hbm,
        pl.BlockSpec((1, 2, toks), per_e),
        pl.BlockSpec((1, 1, wide), per_e),
        pl.BlockSpec((n_e, dim), whole),
        pl.BlockSpec(memory_space=pltpu.SMEM),
    ]
    shape = jax.ShapeDtypeStruct
    out_shape = [
        *[shape((toks, dim), BF)] * 4, shape((n_e, 2, toks), F32),
        shape((n_e, 1, wide), F32), shape((n_e, dim), F32), shape((n_e,), jnp.int32),
    ]
    if first:
        in_specs.append(pl.BlockSpec((wide, wide), whole))
        out_specs.append(pl.BlockSpec((1, dim, wide), per_e))
        out_shape.append(shape((n_e, dim, wide), BF))
    out_specs += [hbm] * 4
    out_shape += [shape((n_e, 2, TILE, w), BF) for w in (dim, dim, wide, half)]
    got = pl.pallas_call(
        functools.partial(chunk_kernel, first, toks),
        grid_spec=pltpu.PrefetchScalarGridSpec(
            num_scalar_prefetch=1,
            grid=(n_e,),
            in_specs=in_specs,
            out_specs=out_specs,
            scratch_shapes=[
                pltpu.VMEM((2, toks, dim), BF),
                pltpu.VMEM((2, tall, dim), BF),
                pltpu.VMEM((2, 2, toks, dim), BF),
                pltpu.VMEM((2, (tall - toks) // 2, toks), F32),
                pltpu.VMEM((2, (tall - toks) // 2, toks), F32),
                pltpu.VMEM((2, n_e, toks), F32),
                pltpu.VMEM((2, 2 * TILE, dim), BF),
                pltpu.VMEM((2, 2 * TILE, dim), BF),
                pltpu.VMEM((2, 2 * TILE, wide), BF),
                pltpu.VMEM((2, 2 * TILE, half), BF),
                pltpu.VMEM((2, room, toks), BF),
                pltpu.VMEM((2, 2, room, dim), BF),
                pltpu.VMEM((toks, dim), F32),
                pltpu.SMEM((2,), jnp.int32),
                pltpu.SemaphoreType.DMA((2, 2, 4)),
                pltpu.SemaphoreType.DMA((2, 2)),
            ],
        ),
        out_shape=out_shape,
        compiler_params=pltpu.CompilerParams(dimension_semantics=('arbitrary',), vmem_limit_bytes=65000 * 1024),
        cost_estimate=pl.CostEstimate(flops=28_000_000_000, bytes_accessed=40_000_000, transcendentals=0),
        name='experts',
    )(ep, *blocks, w1, w2, b1, b2, *((split,) if first else ()))
    return got[:4], got[4:8], got[-4:], (got[8] if first else w1)


def wgrad_kernel(n_c, first_e, n_prev, nt_ref, *refs):
    hbm = [refs[k * n_c:(k + 1) * n_c] for k in range(4)]
    mix_ref = refs[4 * n_c]
    gw1_ref, gw2_ref, acc1, acc2, *bufs, sems = refs[4 * n_c + 1 + n_prev:]
    e = pl.program_id(0)
    n_e = pl.num_programs(0)
    par = lax.rem(e, 2)

    def fetches(step, c, t, p):
        return [pltpu.make_async_copy(hbm[k][c].at[first_e + step, t], bufs[k].at[p, 2 * c + t], sems.at[p, 2 * c + t, k])
                for k in range(4)]

    def each(step, act):
        for c in range(n_c):
            for t in range(2):
                pl.when(nt_ref[c, first_e + step] > t)(functools.partial(act, c, t))

    def start(step, p):
        def go(c, t):
            for copy in fetches(step, c, t, p):
                copy.start()

        each(step, go)

    @pl.when(e == 0)
    def _():
        start(e, par)

    @pl.when(e + 1 < n_e)
    def _():
        start(e + 1, 1 - par)

    acc1[...] = jnp.zeros_like(acc1)
    acc2[...] = jnp.zeros_like(acc2)

    def add(c, t):
        for copy in fetches(e, c, t, par):
            copy.wait()
        x_rows, d_rows, d_hid, act_w = (buf[par, 2 * c + t] for buf in bufs)
        acc1[...] += dot(x_rows, d_hid, LHS)
        acc2[...] += dot(act_w, d_rows, LHS)

    each(e, add)
    gw2_ref[0] = acc2[...].astype(BF)
    gw1_ref[0] = dot(acc1[...].astype(BF), mix_ref[...]).astype(BF)


def run_wgrad(nt, saved, unmix, first_e, n_e, all_e, prev=()):
    n_c = len(saved)
    xs, ds, dh, wa = (list(t) for t in zip(*saved))
    dim, wide, half = xs[0].shape[3], dh[0].shape[3], wa[0].shape[3]
    return pl.pallas_call(
        functools.partial(wgrad_kernel, n_c, first_e, len(prev)),
        grid_spec=pltpu.PrefetchScalarGridSpec(
            num_scalar_prefetch=1,
            grid=(n_e,),
            in_specs=[pl.BlockSpec(memory_space=pl.ANY)] * (4 * n_c) + [pl.BlockSpec((wide, wide), lambda e, nt: (0, 0))]
            + [pl.BlockSpec(memory_space=pl.ANY)] * len(prev),
            out_specs=[pl.BlockSpec((1, dim, wide), lambda e, nt: (first_e + e, 0, 0)), pl.BlockSpec((1, half, dim), lambda e, nt: (first_e + e, 0, 0))],
            scratch_shapes=[pltpu.VMEM((dim, wide), F32), pltpu.VMEM((half, dim), F32)]
            + [pltpu.VMEM((2, 2 * n_c, TILE, w), BF) for w in (dim, dim, wide, half)]
            + [pltpu.SemaphoreType.DMA((2, 2 * n_c, 4))],
        ),
        out_shape=[jax.ShapeDtypeStruct((all_e, dim, wide), BF), jax.ShapeDtypeStruct((all_e, half, dim), BF)],
        input_output_aliases={4 * n_c + 2 + k: k for k in range(len(prev))},
        compiler_params=pltpu.CompilerParams(dimension_semantics=('arbitrary',), vmem_limit_bytes=64000 * 1024),
        cost_estimate=pl.CostEstimate(flops=26_000_000_000, bytes_accessed=60_000_000, transcendentals=0),
        name='weight_grads',
    )(nt, *xs, *ds, *dh, *wa, unmix, *prev)


def pack_kernel(x_ref, d_ref, idx_ref, slot_ref, wr_ref, br_ref, tall_ref, w_ref):
    toks = x_ref.shape[0]
    top_k, n = idx_ref.shape[0], wr_ref.shape[1]
    logits = lax.dot_general(wr_ref[...], x_ref[...], (((0,), (1,)), ((), ())), preferred_element_type=F32) + br_ref[...]
    expert = lax.broadcasted_iota(jnp.int32, (n, toks), 0)
    hots = [jnp.broadcast_to(idx_ref[k:k + 1, :], (n, toks)) == expert for k in range(top_k)]
    picked = [jnp.sum(jnp.where(h, logits, 0.0), axis=0, keepdims=True) for h in hots]
    top = functools.reduce(jnp.maximum, picked)
    exps = [jnp.exp(v - top) for v in picked]
    norm = functools.reduce(jnp.add, exps)
    w_full = jnp.zeros((n, toks), F32)
    kept = jnp.zeros((n, toks), F32)
    for k in range(top_k):
        w_full += jnp.where(hots[k], exps[k] / norm, 0.0)
        kept += jnp.where(hots[k], jnp.where(slot_ref[k:k + 1, :] >= 0, 1.0, 0.0), 0.0)
    w_ref[...] = w_full
    ahead = lax.broadcasted_iota(jnp.int32, (toks, toks), 0) < lax.broadcasted_iota(jnp.int32, (toks, toks), 1)
    rank = dot(kept.astype(BF), jnp.where(ahead, 1.0, 0.0).astype(BF))
    rank = jnp.where(kept > 0.0, rank, -1.0)
    w_top = w_full.astype(BF)
    rest = w_full - w_top.astype(F32)
    w_mid = rest.astype(BF)
    w_low = (rest - w_mid.astype(F32)).astype(BF)
    tall_ref[:toks, :] = d_ref[...]
    tall_ref[toks:toks + n, :toks] = w_top
    tall_ref[toks:toks + n, toks:] = w_mid
    tall_ref[toks + n:, :toks] = w_low
    tall_ref[toks + n:, toks:] = rank.astype(BF)


def run_pack(x_loc, dy_loc, idx_t, slot_t, w_router, b_router):
    toks, dim = x_loc.shape
    n = w_router.shape[1]
    return pl.pallas_call(
        pack_kernel,
        out_shape=[jax.ShapeDtypeStruct((toks + 2 * n, dim), BF), jax.ShapeDtypeStruct((n, toks), F32)],
        compiler_params=pltpu.CompilerParams(vmem_limit_bytes=32000 * 1024),
        name='pack',
    )(x_loc, dy_loc, idx_t, slot_t, w_router, b_router)


def router_kernel(rel, me_ref, *refs):
    n = len(rel)
    d_ref, out_ref = refs[n:]
    total = jnp.zeros(out_ref.shape, F32)
    for k in range(n):
        d_one = d_ref[me_ref[0] ^ rel[k]].astype(BF)
        total += lax.dot_general(refs[k][...], d_one, (((0,), (1,)), ((), ())), preferred_element_type=F32)
    out_ref[...] = total


def run_router_grad(me, rel, x_blocks, d_rel):
    n = len(x_blocks)
    toks, dim = x_blocks[0].shape
    experts = d_rel.shape[1]
    cut = dim // 4
    return pl.pallas_call(
        functools.partial(router_kernel, rel),
        grid_spec=pltpu.PrefetchScalarGridSpec(
            num_scalar_prefetch=1,
            grid=(4,),
            in_specs=[pl.BlockSpec((toks, cut), lambda j, me: (0, j))] * n + [pl.BlockSpec(d_rel.shape, lambda j, me: (0, 0, 0))],
            out_specs=pl.BlockSpec((cut, experts), lambda j, me: (j, 0)),
        ),
        out_shape=jax.ShapeDtypeStruct((dim, experts), F32),
        compiler_params=pltpu.CompilerParams(vmem_limit_bytes=32000 * 1024),
        name='router_grad',
    )(me, *x_blocks, d_rel)


def solution(mesh):
    tp_count = mesh.shape['tp']
    ep_count = mesh.shape['ep']
    n_dev = tp_count * ep_count
    tok_spec = P(('ep', 'tp'), None)

    CORE, XF, YF = 2, 4, 1
    FAR = XF | YF
    CHIPS = (0, YF, FAR, XF)

    def flip(arr, bits):
        turned = (bits & 1) * ep_count + (bits >> 1)
        return lax.ppermute(arr, ('tp', 'ep'), [(s, s ^ turned) for s in range(n_dev)])

    def device_fn(x_loc, idx_loc, slot_loc, w_router, b_router, w_gate_up, b_gate_up, w_down, b_down, dy_loc):
        toks, _ = x_loc.shape
        n_experts = w_router.shape[1]
        n_e = w_gate_up.shape[0]
        wide = w_gate_up.shape[2]
        half = wide // 2
        tp_index = lax.axis_index('tp')
        ep_index = lax.axis_index('ep')
        me = ep_index * tp_count + tp_index

        tall, w_full = run_pack(x_loc, dy_loc, idx_loc.T, slot_loc.T, w_router, b_router[:, None])

        x_of = {XF: flip(x_loc, XF), YF: flip(x_loc, YF)}
        d_of = {XF: flip(tall, XF | CORE), YF: flip(tall, YF | CORE)}
        x_of[FAR] = flip(x_of[XF], YF)
        d_of[FAR] = flip(d_of[YF], XF)
        pairs = [(x_loc, tall, flip(x_loc, CORE), flip(tall, CORE))]
        for bits in CHIPS[1:]:
            pairs.append((x_of[bits], flip(d_of[bits], CORE), flip(x_of[bits], CORE), d_of[bits]))

        col = jnp.arange(wide)
        split_mat = (jnp.where(col < half, 2 * col, 2 * (col - half) + 1)[None, :] == col[:, None]).astype(BF)
        b1 = jnp.concatenate([b_gate_up[:, 0::2], b_gate_up[:, 1::2]], axis=1)[:, None, :]
        b2 = b_down * (tp_index == 0).astype(F32)
        ep = ep_index.astype(jnp.int32)[None]

        w1 = w_gate_up
        dgs, gb1s, gb2s, nts, saved, part = [], [], [], [], [], []

        def chunk(step, blocks, w1):
            o, small, keep, w1 = run_chunk(ep, blocks, w1, w_down, b1, b2, split_mat if step == 0 else None)
            for lst, v in zip((dgs, gb1s, gb2s, nts), small):
                lst.append(v)
            saved.append(keep)
            ya, dxa, yb, dxb = o
            if step == 0:
                part.append((ya, flip(yb, CORE), dxa, flip(dxb, CORE)))
            else:
                part.append((ya, flip(yb, CORE), dxb, flip(dxa, CORE)))
            return w1

        def both(step):
            ya, yb, dxa, dxb = part[step]
            add = lambda a, b: (a.astype(F32) + b.astype(F32)).astype(BF)
            return add(ya, yb), add(dxa, dxb)

        def hop(step, y, dx):
            bits = CHIPS[step]
            return flip(y, bits), flip(dx, bits | CORE)

        w1 = chunk(0, pairs[0], w_gate_up)
        w1 = chunk(1, pairs[1], w1)
        sum_1, blocks = lax.optimization_barrier((both(1), pairs[2]))
        got_1 = hop(1, *sum_1)
        w1 = chunk(2, blocks, w1)
        sum_2, blocks = lax.optimization_barrier((both(2), pairs[3]))
        got_2 = hop(2, *sum_2)
        chunk(3, blocks, w1)

        rel = [CHIPS[k // 2] ^ (CORE * (k % 2)) for k in range(n_dev)]
        dg_rel = jnp.stack([dg[:, k, :] for dg in dgs for k in range(2)])
        slot_of = jnp.array([rel.index(m) for m in range(n_dev)], jnp.int32)
        dg_abs = dg_rel[slot_of[jnp.arange(n_dev) ^ me]]
        dg_back = lax.all_to_all(dg_abs, ('ep', 'tp'), 0, 0, tiled=True)
        sum_3, nt_all = lax.optimization_barrier((both(3), jnp.stack(nts)))
        got_3 = hop(3, *sum_3)

        unmix = split_mat.T
        part_e = n_e // 2
        grads = run_wgrad(nt_all, saved, unmix, 0, part_e, n_e)
        dg_back, nt_all, grads = lax.optimization_barrier((dg_back, nt_all, grads))
        d_gate = jnp.sum(dg_back.reshape(ep_count, tp_count, n_e, toks), axis=1).reshape(n_experts, toks)
        d_logits = w_full * (d_gate - jnp.sum(w_full * d_gate, axis=0, keepdims=True))
        d_all = lax.all_to_all(jnp.broadcast_to(d_logits[None], (n_dev, *d_logits.shape)), ('ep', 'tp'), 0, 0, tiled=True)
        gw1, gw2 = run_wgrad(nt_all, saved, unmix, part_e, n_e - part_e, n_e, grads)
        gb1 = functools.reduce(jnp.add, gb1s)[:, 0, :]
        gb1 = jnp.stack([gb1[:, :half], gb1[:, half:]], axis=2).reshape(n_e, wide)
        gb2 = functools.reduce(jnp.add, gb2s)

        wide_sum = lambda *terms: functools.reduce(jnp.add, [t.astype(F32) for t in terms])
        y_most = wide_sum(part[0][0], part[0][1], got_1[0], got_2[0])
        dx_most = wide_sum(part[0][2], part[0][3], got_1[1], got_2[1])
        dx_most = dx_most + jnp.einsum('et,de->td', d_logits.astype(BF), w_router, preferred_element_type=F32)
        d_all, gw1, y_most, dx_most = lax.optimization_barrier((d_all, gw1, y_most, dx_most))
        gwr = run_router_grad(me.astype(jnp.int32)[None], rel, [p[k] for p in pairs for k in (0, 2)], d_all)
        gbr = jnp.sum(d_all, axis=(0, 2))
        return (wide_sum(y_most, got_3[0]).astype(BF), wide_sum(dx_most, got_3[1]).astype(BF), gw1, gb1, gw2, gb2, gwr, gbr)

    in_specs = (tok_spec, tok_spec, tok_spec, P(None, None), P(None), P('ep', None, 'tp'), P('ep', 'tp'), P('ep', 'tp', None), P('ep', None), tok_spec)
    out_specs = (tok_spec, tok_spec, P('ep', None, 'tp'), P('ep', 'tp'), P('ep', 'tp', None), P('ep', None), P(None, None), P(None))

    return jax.shard_map(device_fn, mesh=mesh, in_specs=in_specs, out_specs=out_specs, check_vma=False)
```

```python
import functools
import jax
import jax.numpy as jnp
from jax import lax
from jax.experimental import pallas as pl
from jax.experimental.pallas import tpu as pltpu
from jax.sharding import PartitionSpec as P

LIMIT = 7.0
ALPHA = 1.702
BF = jnp.bfloat16
F32 = jnp.float32
TILE = 256
BACK = ((1,), (1,))
LHS = ((0,), (0,))


def dot(a, b, dims=((1,), (0,))):
    return lax.dot_general(a, b, (dims, ((), ())), preferred_element_type=F32)


def split3(v):
    top = v.astype(BF)
    rest = v - top.astype(F32)
    mid = rest.astype(BF)
    return top, mid, (rest - mid.astype(F32)).astype(BF)


def chunk_kernel(first, toks, ep_ref, xa_hbm, da_hbm, xb_hbm, db_hbm, w1_in, w2_ref, b1_ref, b2_ref, *refs):
    if first:
        split_ref, *refs = refs
    ya_hbm, dxa_hbm, yb_hbm, dxb_hbm, dg_ref, gb1_ref, gb2_ref, nt_ref, *refs = refs
    if first:
        w1_ref, *refs = refs
    else:
        w1_ref = w1_in
    xs_hbm, ds_hbm, dh_hbm, wa_hbm, *refs = refs
    xin, din, ost, wst, rst, bst, xbuf, dbuf, dhst, wast, sel, zbuf, acc, off, sems, io_sems = refs
    e = pl.program_id(0)
    n_e = pl.num_programs(0)
    half, dim = w2_ref.shape[1:]
    par = lax.rem(e, 2)
    cuts = [slice(j, j + TILE) for j in range(0, dim, TILE)]
    loads = [[pltpu.make_async_copy(x_h, xin.at[i], io_sems.at[i, 0]), pltpu.make_async_copy(d_h, din.at[i], io_sems.at[i, 1])]
             for i, (x_h, d_h) in enumerate(((xa_hbm, da_hbm), (xb_hbm, db_hbm)))]
    stores = [[pltpu.make_async_copy(ost.at[i, k], o_h, io_sems.at[i, k]) for k, o_h in enumerate(pair)]
              for i, pair in enumerate(((ya_hbm, dxa_hbm), (yb_hbm, dxb_hbm)))]

    def saves(expert, t, p):
        at = pl.ds(t * TILE, TILE)
        pairs = ((xbuf, xs_hbm), (dbuf, ds_hbm), (dhst, dh_hbm), (wast, wa_hbm))
        return [pltpu.make_async_copy(src.at[p, at], dst.at[expert, t], sems.at[p, t, k])
                for k, (src, dst) in enumerate(pairs)]

    def drain(expert, p):
        for t in range(2):
            @pl.when(nt_ref[expert] > t)
            def _():
                for copy in saves(expert, t, p):
                    copy.wait()

    @pl.when(e == 0)
    def _():
        for i in range(2):
            for copy in reversed(loads[i]):
                copy.start()
            off[i] = 0

    if first:
        w1_ref[0] = dot(w1_in[0], split_ref[...]).astype(BF)

    @pl.when(e == 0)
    def _():
        base = pl.multiple_of(ep_ref[0] * 8, 8)
        b_parts = jnp.concatenate(split3(b2_ref[...]), axis=0)
        for i in range(2):
            for copy in loads[i]:
                copy.wait()

        def prepare(i, _):
            aux = din[i, toks:, :].astype(F32)
            n = aux.shape[0] // 2
            wst[i] = aux[:n, :toks] + aux[:n, toks:] + aux[n:, :toks]
            rst[i] = aux[n:, toks:]
            local_w = wst[i, pl.ds(base, 8), :]
            local_r = rst[i, pl.ds(base, 8), :]
            w_parts = jnp.concatenate(split3(jnp.where(local_r >= 0.0, local_w, 0.0)), axis=0)
            d_all = din[i, :toks, :]
            got = dot(w_parts, d_all)
            gb2_ref[...] += got[:8] + got[8:16] + got[16:]
            got = dot(b_parts, d_all, BACK)
            bst[i] = got[:8] + got[8:16] + got[16:]
            return 0

        gb2_ref[...] = jnp.zeros_like(gb2_ref)
        lax.fori_loop(0, 2, prepare, 0)

    for p in range(2):
        @pl.when((e >= 2) & (par == p))
        def _():
            drain(e - 2, p)

    row = ep_ref[0] * n_e + e
    counts = [(jnp.max(rst[i, pl.ds(row, 1), :]) + 1.0).astype(jnp.int32) for i in range(2)]
    gb1_ref[...] = jnp.zeros_like(gb1_ref)
    b_row = b2_ref[pl.ds(e, 1), :]

    seg = TILE // 2
    parts = ((0, seg), (1, seg))
    for i in range(2):
        dg_ref[0, i:i + 1, :] = jnp.where(rst[i, pl.ds(row, 1), :] >= 0.0, bst[i, pl.ds(e, 1), :], 0.0)

    def tile(t, _):
        base = (t * seg).astype(F32)
        rows = pl.ds(pl.multiple_of(t * TILE, TILE), TILE)
        hots, w_rows, at = [], [], 0
        for i, m in parts:
            pos = lax.broadcasted_iota(jnp.int32, (m, toks), 0).astype(F32)
            hot = jnp.broadcast_to(rst[i, pl.ds(row, 1), :] - base, (m, toks)) == pos
            hot_b = jnp.where(hot, 1.0, 0.0).astype(BF)
            sel[i, pl.ds(pl.multiple_of(off[i], 128), m), :] = hot_b
            w_rows.append(jnp.sum(jnp.where(hot, jnp.broadcast_to(wst[i, pl.ds(row, 1), :], (m, toks)), 0.0), axis=1, keepdims=True))
            hots.append(hot)
            dst = pl.ds(pl.multiple_of(t * TILE + at, 128), m)
            for c in cuts:
                xbuf[par, dst, c] = dot(hot_b, xin[i, :, c]).astype(BF)
            for c in cuts:
                dbuf[par, dst, c] = dot(hot_b, din[i, :toks, c]).astype(BF)
            at += m
        w_row = jnp.concatenate(w_rows, axis=0)
        x_rows = xbuf[par, rows, :]
        gate = dot(x_rows, w1_ref[0, :, :half]) + b1_ref[0, :, :half]
        up = dot(x_rows, w1_ref[0, :, half:]) + b1_ref[0, :, half:]
        d_raw = dot(dbuf[par, rows, :], w2_ref[0], BACK)
        g = jnp.minimum(gate, LIMIT)
        u1 = jnp.clip(up, -LIMIT, LIMIT) + 1.0
        sg = jax.nn.sigmoid(ALPHA * g)
        gs = g * sg
        act = (gs * u1).astype(BF)
        act_w = act.astype(F32)
        wast[par, rows, :] = (w_row * act_w).astype(BF)
        dg_row = jnp.sum(act_w * d_raw, axis=1, keepdims=True)
        d_act = w_row * d_raw
        gate_on = jnp.where(gate < LIMIT, 1.0, jnp.where(gate == LIMIT, 0.5, 0.0))
        up_abs = jnp.abs(up)
        up_on = jnp.where(up_abs < LIMIT, 1.0, jnp.where(up_abs == LIMIT, 0.5, 0.0))
        d_gate = d_act * u1 * (sg * (1.0 + ALPHA * g * (1.0 - sg))) * gate_on
        d_up = d_act * gs * up_on
        gb1_ref[0, :, :half] += jnp.sum(d_gate, axis=0, keepdims=True)
        gb1_ref[0, :, half:] += jnp.sum(d_up, axis=0, keepdims=True)
        dhst[par, rows, :half] = d_gate.astype(BF)
        dhst[par, rows, half:] = d_up.astype(BF)
        d_hid = dhst[par, rows, :]

        def put(k, c, value):
            at = 0
            for i, m in parts:
                zbuf[k, i, pl.ds(pl.multiple_of(off[i], 128), m), c] = value[at:at + m]
                at += m

        for c in cuts:
            part = (dot(act, w2_ref[0, :, c]) + b_row[:, c]).astype(BF).astype(F32)
            put(0, c, (w_row * part).astype(BF))
        for c in cuts:
            put(1, c, dot(d_hid, w1_ref[0, c, :], BACK).astype(BF))
        for copy in saves(e, t, par):
            copy.start()
        at = 0
        for (i, m), hot in zip(parts, hots):
            dg = jnp.sum(jnp.where(hot, dg_row[at:at + m], 0.0), axis=0, keepdims=True)
            dg_ref[0, i:i + 1, :] += dg
            off[i] = off[i] + m
            at += m

        return 0

    n_pass = jnp.maximum((jnp.maximum(counts[0], counts[1]) + seg - 1) // seg, 1)
    nt_ref[e] = n_pass
    lax.fori_loop(0, n_pass, tile, 0)

    @pl.when(e == n_e - 1)
    def _():
        long = 4 * TILE

        def combine(j):
            i, k = j // 2, lax.rem(j, 2)
            total = pl.multiple_of(off[i], 128)
            acc[...] = dot(sel[i, :long, :], zbuf[k, i, :long, :], LHS)

            def step(q, _):
                at = pl.ds(pl.multiple_of(q * TILE, TILE), TILE)
                acc[...] += dot(sel[i, at, :], zbuf[k, i, at, :], LHS)
                return 0

            lax.fori_loop(4, (total + TILE - 1) // TILE, step, 0)
            ost[i, k] = acc[...].astype(BF)
            return 0

        for i in range(2):
            total = pl.multiple_of(off[i], 128)
            sel[i, pl.ds(total, TILE), :] = jnp.zeros((TILE, toks), BF)
            for k in range(2):
                zbuf[k, i, pl.ds(total, TILE), :] = jnp.zeros((TILE, dim), BF)

        def go(j, _):
            combine(j)
            for q in range(4):
                @pl.when(j == q)
                def _():
                    stores[q // 2][q % 2].start()
            return 0

        lax.fori_loop(0, 4, go, 0)
        for back in (1, 0):
            p = lax.rem(e - back, 2)
            drain(e - back, p)
        for i in range(2):
            for copy in stores[i]:
                copy.wait()


def run_chunk(ep, blocks, w1, w2, b1, b2, split=None):
    first = split is not None
    n_e, dim, wide = w1.shape
    half = w2.shape[1]
    toks, tall = blocks[0].shape[0], blocks[1].shape[0]
    whole = lambda e, ep: (0, 0)
    per_e = lambda e, ep: (e, 0, 0)
    room = n_e * TILE + TILE
    hbm = pl.BlockSpec(memory_space=pl.ANY)
    in_specs = [
        hbm, hbm, hbm, hbm,
        pl.BlockSpec((1, dim, wide), per_e),
        pl.BlockSpec((1, half, dim), per_e),
        pl.BlockSpec((1, 1, wide), per_e),
        pl.BlockSpec((n_e, dim), whole),
    ]
    out_specs = [
        hbm, hbm, hbm, hbm,
        pl.BlockSpec((1, 2, toks), per_e),
        pl.BlockSpec((1, 1, wide), per_e),
        pl.BlockSpec((n_e, dim), whole),
        pl.BlockSpec(memory_space=pltpu.SMEM),
    ]
    shape = jax.ShapeDtypeStruct
    out_shape = [
        *[shape((toks, dim), BF)] * 4, shape((n_e, 2, toks), F32),
        shape((n_e, 1, wide), F32), shape((n_e, dim), F32), shape((n_e,), jnp.int32),
    ]
    if first:
        in_specs.append(pl.BlockSpec((wide, wide), whole))
        out_specs.append(pl.BlockSpec((1, dim, wide), per_e))
        out_shape.append(shape((n_e, dim, wide), BF))
    out_specs += [hbm] * 4
    out_shape += [shape((n_e, 2, TILE, w), BF) for w in (dim, dim, wide, half)]
    got = pl.pallas_call(
        functools.partial(chunk_kernel, first, toks),
        grid_spec=pltpu.PrefetchScalarGridSpec(
            num_scalar_prefetch=1,
            grid=(n_e,),
            in_specs=in_specs,
            out_specs=out_specs,
            scratch_shapes=[
                pltpu.VMEM((2, toks, dim), BF),
                pltpu.VMEM((2, tall, dim), BF),
                pltpu.VMEM((2, 2, toks, dim), BF),
                pltpu.VMEM((2, (tall - toks) // 2, toks), F32),
                pltpu.VMEM((2, (tall - toks) // 2, toks), F32),
                pltpu.VMEM((2, n_e, toks), F32),
                pltpu.VMEM((2, 2 * TILE, dim), BF),
                pltpu.VMEM((2, 2 * TILE, dim), BF),
                pltpu.VMEM((2, 2 * TILE, wide), BF),
                pltpu.VMEM((2, 2 * TILE, half), BF),
                pltpu.VMEM((2, room, toks), BF),
                pltpu.VMEM((2, 2, room, dim), BF),
                pltpu.VMEM((toks, dim), F32),
                pltpu.SMEM((2,), jnp.int32),
                pltpu.SemaphoreType.DMA((2, 2, 4)),
                pltpu.SemaphoreType.DMA((2, 2)),
            ],
        ),
        out_shape=out_shape,
        compiler_params=pltpu.CompilerParams(dimension_semantics=('arbitrary',), vmem_limit_bytes=65000 * 1024),
        cost_estimate=pl.CostEstimate(flops=28_000_000_000, bytes_accessed=40_000_000, transcendentals=0),
        name='experts',
    )(ep, *blocks, w1, w2, b1, b2, *((split,) if first else ()))
    return got[:4], got[4:8], got[-4:], (got[8] if first else w1)


def wgrad_kernel(n_c, first_e, n_prev, nt_ref, *refs):
    hbm = [refs[k * n_c:(k + 1) * n_c] for k in range(4)]
    mix_ref = refs[4 * n_c]
    gw1_ref, gw2_ref, acc1, acc2, *bufs, sems = refs[4 * n_c + 1 + n_prev:]
    e = pl.program_id(0)
    n_e = pl.num_programs(0)
    par = lax.rem(e, 2)

    def fetches(step, c, t, p):
        return [pltpu.make_async_copy(hbm[k][c].at[first_e + step, t], bufs[k].at[p, 2 * c + t], sems.at[p, 2 * c + t, k])
                for k in range(4)]

    def each(step, act):
        for c in range(n_c):
            for t in range(2):
                pl.when(nt_ref[c, first_e + step] > t)(functools.partial(act, c, t))

    def start(step, p):
        def go(c, t):
            for copy in fetches(step, c, t, p):
                copy.start()

        each(step, go)

    @pl.when(e == 0)
    def _():
        start(e, par)

    @pl.when(e + 1 < n_e)
    def _():
        start(e + 1, 1 - par)

    acc1[...] = jnp.zeros_like(acc1)
    acc2[...] = jnp.zeros_like(acc2)

    def add(j, _):
        @pl.when(nt_ref[j // 2, first_e + e] > lax.rem(j, 2))
        def _():
            for k in range(4):
                pltpu.make_async_copy(hbm[k][0].at[0, 0], bufs[k].at[par, j], sems.at[par, j, k]).wait()
            x_rows, d_rows, d_hid, act_w = (buf[par, j] for buf in bufs)
            acc1[...] += dot(x_rows, d_hid, LHS)
            acc2[...] += dot(act_w, d_rows, LHS)

        return 0

    lax.fori_loop(0, 2 * n_c, add, 0)
    gw2_ref[0] = acc2[...].astype(BF)
    gw1_ref[0] = dot(acc1[...].astype(BF), mix_ref[...]).astype(BF)


def run_wgrad(nt, saved, unmix, first_e, n_e, all_e, prev=()):
    n_c = len(saved)
    xs, ds, dh, wa = (list(t) for t in zip(*saved))
    dim, wide, half = xs[0].shape[3], dh[0].shape[3], wa[0].shape[3]
    return pl.pallas_call(
        functools.partial(wgrad_kernel, n_c, first_e, len(prev)),
        grid_spec=pltpu.PrefetchScalarGridSpec(
            num_scalar_prefetch=1,
            grid=(n_e,),
            in_specs=[pl.BlockSpec(memory_space=pl.ANY)] * (4 * n_c) + [pl.BlockSpec((wide, wide), lambda e, nt: (0, 0))]
            + [pl.BlockSpec(memory_space=pl.ANY)] * len(prev),
            out_specs=[pl.BlockSpec((1, dim, wide), lambda e, nt: (first_e + e, 0, 0)), pl.BlockSpec((1, half, dim), lambda e, nt: (first_e + e, 0, 0))],
            scratch_shapes=[pltpu.VMEM((dim, wide), F32), pltpu.VMEM((half, dim), F32)]
            + [pltpu.VMEM((2, 2 * n_c, TILE, w), BF) for w in (dim, dim, wide, half)]
            + [pltpu.SemaphoreType.DMA((2, 2 * n_c, 4))],
        ),
        out_shape=[jax.ShapeDtypeStruct((all_e, dim, wide), BF), jax.ShapeDtypeStruct((all_e, half, dim), BF)],
        input_output_aliases={4 * n_c + 2 + k: k for k in range(len(prev))},
        compiler_params=pltpu.CompilerParams(dimension_semantics=('arbitrary',), vmem_limit_bytes=64000 * 1024),
        cost_estimate=pl.CostEstimate(flops=26_000_000_000, bytes_accessed=60_000_000, transcendentals=0),
        name='weight_grads',
    )(nt, *xs, *ds, *dh, *wa, unmix, *prev)


def pack_kernel(x_ref, d_ref, idx_ref, slot_ref, wr_ref, br_ref, tall_ref, w_ref):
    toks = x_ref.shape[0]
    top_k, n = idx_ref.shape[0], wr_ref.shape[0]
    logits = dot(wr_ref[...], x_ref[...], BACK) + br_ref[...]
    expert = lax.broadcasted_iota(jnp.int32, (n, toks), 0)
    hots = [jnp.broadcast_to(idx_ref[k:k + 1, :], (n, toks)) == expert for k in range(top_k)]
    picked = [jnp.sum(jnp.where(h, logits, 0.0), axis=0, keepdims=True) for h in hots]
    top = functools.reduce(jnp.maximum, picked)
    exps = [jnp.exp(v - top) for v in picked]
    norm = functools.reduce(jnp.add, exps)
    w_full = jnp.zeros((n, toks), F32)
    kept = jnp.zeros((n, toks), F32)
    for k in range(top_k):
        w_full += jnp.where(hots[k], exps[k] / norm, 0.0)
        kept += jnp.where(hots[k], jnp.where(slot_ref[k:k + 1, :] >= 0, 1.0, 0.0), 0.0)
    w_ref[...] = w_full
    ahead = lax.broadcasted_iota(jnp.int32, (toks, toks), 0) < lax.broadcasted_iota(jnp.int32, (toks, toks), 1)
    rank = dot(kept.astype(BF), jnp.where(ahead, 1.0, 0.0).astype(BF))
    rank = jnp.where(kept > 0.0, rank, -1.0)
    w_top = w_full.astype(BF)
    rest = w_full - w_top.astype(F32)
    w_mid = rest.astype(BF)
    w_low = (rest - w_mid.astype(F32)).astype(BF)
    tall_ref[:toks, :] = d_ref[...]
    tall_ref[toks:toks + n, :toks] = w_top
    tall_ref[toks:toks + n, toks:] = w_mid
    tall_ref[toks + n:, :toks] = w_low
    tall_ref[toks + n:, toks:] = rank.astype(BF)


def run_pack(x_loc, dy_loc, idx_t, slot_t, w_router, b_router):
    toks, dim = x_loc.shape
    n = w_router.shape[0]
    return pl.pallas_call(
        pack_kernel,
        out_shape=[jax.ShapeDtypeStruct((toks + 2 * n, dim), BF), jax.ShapeDtypeStruct((n, toks), F32)],
        compiler_params=pltpu.CompilerParams(vmem_limit_bytes=32000 * 1024),
        name='pack',
    )(x_loc, dy_loc, idx_t, slot_t, w_router, b_router)


def router_kernel(rel, me_ref, *refs):
    n = len(rel)
    d_ref, out_ref = refs[n:]
    total = jnp.zeros(out_ref.shape, F32)
    for k in range(n):
        d_one = d_ref[me_ref[0] ^ rel[k]].astype(BF)
        total += lax.dot_general(refs[k][...], d_one, (((0,), (1,)), ((), ())), preferred_element_type=F32)
    out_ref[...] = total


def run_router_grad(me, rel, x_blocks, d_rel):
    n = len(x_blocks)
    toks, dim = x_blocks[0].shape
    experts = d_rel.shape[1]
    cut = dim // 4
    return pl.pallas_call(
        functools.partial(router_kernel, rel),
        grid_spec=pltpu.PrefetchScalarGridSpec(
            num_scalar_prefetch=1,
            grid=(4,),
            in_specs=[pl.BlockSpec((toks, cut), lambda j, me: (0, j))] * n + [pl.BlockSpec(d_rel.shape, lambda j, me: (0, 0, 0))],
            out_specs=pl.BlockSpec((cut, experts), lambda j, me: (j, 0)),
        ),
        out_shape=jax.ShapeDtypeStruct((dim, experts), F32),
        compiler_params=pltpu.CompilerParams(vmem_limit_bytes=32000 * 1024),
        name='router_grad',
    )(me, *x_blocks, d_rel)


def solution(mesh):
    tp_count = mesh.shape['tp']
    ep_count = mesh.shape['ep']
    n_dev = tp_count * ep_count
    tok_spec = P(('ep', 'tp'), None)

    CORE, XF, YF = 2, 4, 1
    FAR = XF | YF
    CHIPS = (0, YF, FAR, XF)

    def flip(arr, bits):
        turned = (bits & 1) * ep_count + (bits >> 1)
        return lax.ppermute(arr, ('tp', 'ep'), [(s, s ^ turned) for s in range(n_dev)])

    def device_fn(x_loc, idx_loc, slot_loc, w_router, b_router, w_gate_up, b_gate_up, w_down, b_down, dy_loc):
        toks, _ = x_loc.shape
        n_experts = w_router.shape[1]
        n_e = w_gate_up.shape[0]
        wide = w_gate_up.shape[2]
        half = wide // 2
        tp_index = lax.axis_index('tp')
        ep_index = lax.axis_index('ep')
        me = ep_index * tp_count + tp_index

        tall, w_full = run_pack(x_loc, dy_loc, idx_loc.T, slot_loc.T, w_router.T, b_router[:, None])

        x_of = {XF: flip(x_loc, XF), YF: flip(x_loc, YF)}
        d_of = {XF: flip(tall, XF | CORE), YF: flip(tall, YF | CORE)}
        x_of[FAR] = flip(x_of[XF], YF)
        d_of[FAR] = flip(d_of[YF], XF)
        pairs = [(x_loc, tall, flip(x_loc, CORE), flip(tall, CORE))]
        for bits in CHIPS[1:]:
            pairs.append((x_of[bits], flip(d_of[bits], CORE), flip(x_of[bits], CORE), d_of[bits]))

        col = jnp.arange(wide)
        split_mat = (jnp.where(col < half, 2 * col, 2 * (col - half) + 1)[None, :] == col[:, None]).astype(BF)
        b1 = jnp.concatenate([b_gate_up[:, 0::2], b_gate_up[:, 1::2]], axis=1)[:, None, :]
        b2 = b_down * (tp_index == 0).astype(F32)
        ep = ep_index.astype(jnp.int32)[None]

        w1 = w_gate_up
        dgs, gb1s, gb2s, nts, saved, part = [], [], [], [], [], []

        def chunk(step, blocks, w1):
            o, small, keep, w1 = run_chunk(ep, blocks, w1, w_down, b1, b2, split_mat if step == 0 else None)
            for lst, v in zip((dgs, gb1s, gb2s, nts), small):
                lst.append(v)
            saved.append(keep)
            ya, dxa, yb, dxb = o
            if step == 0:
                part.append((ya, flip(yb, CORE), dxa, flip(dxb, CORE)))
            else:
                part.append((ya, flip(yb, CORE), dxb, flip(dxa, CORE)))
            return w1

        def both(step):
            ya, yb, dxa, dxb = part[step]
            add = lambda a, b: (a.astype(F32) + b.astype(F32)).astype(BF)
            return add(ya, yb), add(dxa, dxb)

        def hop(step, y, dx):
            bits = CHIPS[step]
            return flip(y, bits), flip(dx, bits | CORE)

        w1 = chunk(0, pairs[0], w_gate_up)
        w1 = chunk(1, pairs[1], w1)
        sum_1, blocks = lax.optimization_barrier((both(1), pairs[2]))
        got_1 = hop(1, *sum_1)
        w1 = chunk(2, blocks, w1)
        sum_2, blocks = lax.optimization_barrier((both(2), pairs[3]))
        got_2 = hop(2, *sum_2)
        chunk(3, blocks, w1)

        rel = [CHIPS[k // 2] ^ (CORE * (k % 2)) for k in range(n_dev)]
        dg_rel = jnp.stack([dg[:, k, :] for dg in dgs for k in range(2)])
        slot_of = jnp.array([rel.index(m) for m in range(n_dev)], jnp.int32)
        dg_abs = dg_rel[slot_of[jnp.arange(n_dev) ^ me]]
        dg_back = lax.all_to_all(dg_abs, ('ep', 'tp'), 0, 0, tiled=True)
        nt_all = jnp.stack(nts)
        unmix = split_mat.T
        part_e = n_e // 4
        grads = run_wgrad(nt_all, saved, unmix, 0, part_e, n_e)
        last, dg_back, nt_b, grads = lax.optimization_barrier((part[3], dg_back, nt_all, grads))
        part[3] = last
        d_gate = jnp.sum(dg_back.reshape(ep_count, tp_count, n_e, toks), axis=1).reshape(n_experts, toks)
        d_logits = w_full * (d_gate - jnp.sum(w_full * d_gate, axis=0, keepdims=True))
        sum_3, d_logits, nt_b, grads = lax.optimization_barrier((both(3), d_logits, nt_b, grads))
        d_all = lax.all_to_all(jnp.broadcast_to(d_logits[None], (n_dev, *d_logits.shape)), ('ep', 'tp'), 0, 0, tiled=True)
        got_3 = hop(3, *sum_3)
        gw1, gw2 = run_wgrad(nt_b, saved, unmix, part_e, n_e - part_e, n_e, grads)
        gb1 = functools.reduce(jnp.add, gb1s)[:, 0, :]
        gb1 = jnp.stack([gb1[:, :half], gb1[:, half:]], axis=2).reshape(n_e, wide)
        gb2 = functools.reduce(jnp.add, gb2s)

        wide_sum = lambda *terms: functools.reduce(jnp.add, [t.astype(F32) for t in terms])
        via_router = jnp.einsum('et,de->td', d_logits.astype(BF), w_router, preferred_element_type=F32)
        d_all, gw1, own = lax.optimization_barrier((d_all, gw1, part[0]))
        gwr = run_router_grad(me.astype(jnp.int32)[None], rel, [p[k] for p in pairs for k in (0, 2)], d_all)
        gwr, got_3 = lax.optimization_barrier((gwr, got_3))
        moe = wide_sum(own[0], own[1], got_1[0], got_2[0], got_3[0])
        d_x = wide_sum(own[2], own[3], got_1[1], got_2[1], got_3[1], via_router)
        gbr = jnp.sum(d_all, axis=(0, 2))
        return (moe.astype(BF), d_x.astype(BF), gw1, gb1, gw2, gb2, gwr, gbr)

    in_specs = (tok_spec, tok_spec, tok_spec, P(None, None), P(None), P('ep', None, 'tp'), P('ep', 'tp'), P('ep', 'tp', None), P('ep', None), tok_spec)
    out_specs = (tok_spec, tok_spec, P('ep', None, 'tp'), P('ep', 'tp'), P('ep', 'tp', None), P('ep', None), P(None, None), P(None))

    return jax.shard_map(device_fn, mesh=mesh, in_specs=in_specs, out_specs=out_specs, check_vma=False)
```

```python
import functools
import jax
import jax.numpy as jnp
from jax import lax
from jax.experimental import pallas as pl
from jax.experimental.pallas import tpu as pltpu
from jax.sharding import PartitionSpec as P

LIMIT = 7.0
ALPHA = 1.702
BF = jnp.bfloat16
F32 = jnp.float32
TILE = 256
BACK = ((1,), (1,))
LHS = ((0,), (0,))


def dot(a, b, dims=((1,), (0,))):
    return lax.dot_general(a, b, (dims, ((), ())), preferred_element_type=F32)


def split3(v):
    top = v.astype(BF)
    rest = v - top.astype(F32)
    mid = rest.astype(BF)
    return top, mid, (rest - mid.astype(F32)).astype(BF)


def chunk_kernel(first, toks, ep_ref, xa_hbm, da_hbm, xb_hbm, db_hbm, w1_in, w2_ref, b1_ref, b2_ref, *refs):
    if first:
        split_ref, *refs = refs
    ya_hbm, dxa_hbm, yb_hbm, dxb_hbm, dg_ref, gb1_ref, gb2_ref, nt_ref, *refs = refs
    if first:
        w1_ref, *refs = refs
    else:
        w1_ref = w1_in
    xs_hbm, ds_hbm, dh_hbm, wa_hbm, *refs = refs
    xin, din, ost, wst, rst, bst, xbuf, dbuf, dhst, wast, sel, zbuf, acc, off, sems, io_sems = refs
    e = pl.program_id(0)
    n_e = pl.num_programs(0)
    half, dim = w2_ref.shape[1:]
    par = lax.rem(e, 2)
    cuts = [slice(j, j + TILE) for j in range(0, dim, TILE)]
    loads = [[pltpu.make_async_copy(x_h, xin.at[i], io_sems.at[i, 0]), pltpu.make_async_copy(d_h, din.at[i], io_sems.at[i, 1])]
             for i, (x_h, d_h) in enumerate(((xa_hbm, da_hbm), (xb_hbm, db_hbm)))]
    stores = [[pltpu.make_async_copy(ost.at[i, k], o_h, io_sems.at[i, k]) for k, o_h in enumerate(pair)]
              for i, pair in enumerate(((ya_hbm, dxa_hbm), (yb_hbm, dxb_hbm)))]

    def saves(expert, t, p):
        at = pl.ds(t * TILE, TILE)
        pairs = ((xbuf, xs_hbm), (dbuf, ds_hbm), (dhst, dh_hbm), (wast, wa_hbm))
        return [pltpu.make_async_copy(src.at[p, at], dst.at[expert, t], sems.at[p, t, k])
                for k, (src, dst) in enumerate(pairs)]

    def drain(expert, p):
        for t in range(2):
            @pl.when(nt_ref[expert] > t)
            def _():
                for copy in saves(expert, t, p):
                    copy.wait()

    @pl.when(e == 0)
    def _():
        for i in range(2):
            for copy in reversed(loads[i]):
                copy.start()
            off[i] = 0
        sel[...] = jnp.zeros_like(sel)
        zbuf[...] = jnp.zeros_like(zbuf)

    if first:
        w1_ref[0] = dot(w1_in[0], split_ref[...]).astype(BF)

    @pl.when(e == 0)
    def _():
        base = pl.multiple_of(ep_ref[0] * 8, 8)
        b_parts = jnp.concatenate(split3(b2_ref[...]), axis=0)
        for i in range(2):
            for copy in loads[i]:
                copy.wait()

        def prepare(i, _):
            aux = din[i, toks:, :].astype(F32)
            n = aux.shape[0] // 2
            wst[i] = aux[:n, :toks] + aux[:n, toks:] + aux[n:, :toks]
            rst[i] = aux[n:, toks:]
            local_w = wst[i, pl.ds(base, 8), :]
            local_r = rst[i, pl.ds(base, 8), :]
            w_parts = jnp.concatenate(split3(jnp.where(local_r >= 0.0, local_w, 0.0)), axis=0)
            d_all = din[i, :toks, :]
            got = dot(w_parts, d_all)
            gb2_ref[...] += got[:8] + got[8:16] + got[16:]
            got = dot(b_parts, d_all, BACK)
            bst[i] = got[:8] + got[8:16] + got[16:]
            return 0

        gb2_ref[...] = jnp.zeros_like(gb2_ref)
        lax.fori_loop(0, 2, prepare, 0)

    for p in range(2):
        @pl.when((e >= 2) & (par == p))
        def _():
            drain(e - 2, p)

    row = ep_ref[0] * n_e + e
    counts = [(jnp.max(rst[i, pl.ds(row, 1), :]) + 1.0).astype(jnp.int32) for i in range(2)]
    gb1_ref[...] = jnp.zeros_like(gb1_ref)
    b_row = b2_ref[pl.ds(e, 1), :]

    seg = TILE // 2
    parts = ((0, seg), (1, seg))
    for i in range(2):
        dg_ref[0, i:i + 1, :] = jnp.where(rst[i, pl.ds(row, 1), :] >= 0.0, bst[i, pl.ds(e, 1), :], 0.0)

    def tile(t, _):
        base = (t * seg).astype(F32)
        rows = pl.ds(pl.multiple_of(t * TILE, TILE), TILE)
        hots, w_rows, at = [], [], 0
        for i, m in parts:
            pos = lax.broadcasted_iota(jnp.int32, (m, toks), 0).astype(F32)
            hot = jnp.broadcast_to(rst[i, pl.ds(row, 1), :] - base, (m, toks)) == pos
            hot_b = jnp.where(hot, 1.0, 0.0).astype(BF)
            sel[i, pl.ds(pl.multiple_of(off[i], 16), m), :] = hot_b
            w_rows.append(jnp.sum(jnp.where(hot, jnp.broadcast_to(wst[i, pl.ds(row, 1), :], (m, toks)), 0.0), axis=1, keepdims=True))
            hots.append(hot)
            dst = pl.ds(pl.multiple_of(t * TILE + at, 128), m)
            for c in cuts:
                xbuf[par, dst, c] = dot(hot_b, xin[i, :, c]).astype(BF)
            for c in cuts:
                dbuf[par, dst, c] = dot(hot_b, din[i, :toks, c]).astype(BF)
            at += m
        w_row = jnp.concatenate(w_rows, axis=0)
        x_rows = xbuf[par, rows, :]
        gate = dot(x_rows, w1_ref[0, :, :half]) + b1_ref[0, :, :half]
        up = dot(x_rows, w1_ref[0, :, half:]) + b1_ref[0, :, half:]
        d_raw = dot(dbuf[par, rows, :], w2_ref[0], BACK)
        g = jnp.minimum(gate, LIMIT)
        u1 = jnp.clip(up, -LIMIT, LIMIT) + 1.0
        sg = jax.nn.sigmoid(ALPHA * g)
        gs = g * sg
        act = (gs * u1).astype(BF)
        act_w = act.astype(F32)
        wast[par, rows, :] = (w_row * act_w).astype(BF)
        dg_row = jnp.sum(act_w * d_raw, axis=1, keepdims=True)
        d_act = w_row * d_raw
        gate_on = jnp.where(gate < LIMIT, 1.0, jnp.where(gate == LIMIT, 0.5, 0.0))
        up_abs = jnp.abs(up)
        up_on = jnp.where(up_abs < LIMIT, 1.0, jnp.where(up_abs == LIMIT, 0.5, 0.0))
        d_gate = d_act * u1 * (sg * (1.0 + ALPHA * g * (1.0 - sg))) * gate_on
        d_up = d_act * gs * up_on
        gb1_ref[0, :, :half] += jnp.sum(d_gate, axis=0, keepdims=True)
        gb1_ref[0, :, half:] += jnp.sum(d_up, axis=0, keepdims=True)
        dhst[par, rows, :half] = d_gate.astype(BF)
        dhst[par, rows, half:] = d_up.astype(BF)
        d_hid = dhst[par, rows, :]

        def put(k, c, value):
            at = 0
            for i, m in parts:
                zbuf[k, i, pl.ds(pl.multiple_of(off[i], 16), m), c] = value[at:at + m]
                at += m

        for c in cuts:
            part = (dot(act, w2_ref[0, :, c]) + b_row[:, c]).astype(BF).astype(F32)
            put(0, c, (w_row * part).astype(BF))
        for c in cuts:
            put(1, c, dot(d_hid, w1_ref[0, c, :], BACK).astype(BF))
        for copy in saves(e, t, par):
            copy.start()
        at = 0
        for (i, m), hot in zip(parts, hots):
            dg = jnp.sum(jnp.where(hot, dg_row[at:at + m], 0.0), axis=0, keepdims=True)
            dg_ref[0, i:i + 1, :] += dg
            used = jnp.clip(counts[i] - t * seg, 0, seg)
            off[i] = off[i] + (used + 15) // 16 * 16
            at += m

        return 0

    n_pass = jnp.maximum((jnp.maximum(counts[0], counts[1]) + seg - 1) // seg, 1)
    nt_ref[e] = n_pass
    lax.fori_loop(0, n_pass, tile, 0)

    @pl.when(e == n_e - 1)
    def _():
        long = 4 * TILE

        def combine(j):
            i, k = j // 2, lax.rem(j, 2)
            total = off[i]
            acc[...] = dot(sel[i, :long, :], zbuf[k, i, :long, :], LHS)

            def step(q, _):
                at = pl.ds(pl.multiple_of(q * TILE, TILE), TILE)
                acc[...] += dot(sel[i, at, :], zbuf[k, i, at, :], LHS)
                return 0

            lax.fori_loop(4, (total + TILE - 1) // TILE, step, 0)
            ost[i, k] = acc[...].astype(BF)
            return 0

        def go(j, _):
            combine(j)
            for q in range(4):
                @pl.when(j == q)
                def _():
                    stores[q // 2][q % 2].start()
            return 0

        lax.fori_loop(0, 4, go, 0)
        for back in (1, 0):
            p = lax.rem(e - back, 2)
            drain(e - back, p)
        for i in range(2):
            for copy in stores[i]:
                copy.wait()


def run_chunk(ep, blocks, w1, w2, b1, b2, split=None):
    first = split is not None
    n_e, dim, wide = w1.shape
    half = w2.shape[1]
    toks, tall = blocks[0].shape[0], blocks[1].shape[0]
    whole = lambda e, ep: (0, 0)
    per_e = lambda e, ep: (e, 0, 0)
    room = n_e * TILE + TILE
    hbm = pl.BlockSpec(memory_space=pl.ANY)
    in_specs = [
        hbm, hbm, hbm, hbm,
        pl.BlockSpec((1, dim, wide), per_e),
        pl.BlockSpec((1, half, dim), per_e),
        pl.BlockSpec((1, 1, wide), per_e),
        pl.BlockSpec((n_e, dim), whole),
    ]
    out_specs = [
        hbm, hbm, hbm, hbm,
        pl.BlockSpec((1, 2, toks), per_e),
        pl.BlockSpec((1, 1, wide), per_e),
        pl.BlockSpec((n_e, dim), whole),
        pl.BlockSpec(memory_space=pltpu.SMEM),
    ]
    shape = jax.ShapeDtypeStruct
    out_shape = [
        *[shape((toks, dim), BF)] * 4, shape((n_e, 2, toks), F32),
        shape((n_e, 1, wide), F32), shape((n_e, dim), F32), shape((n_e,), jnp.int32),
    ]
    if first:
        in_specs.append(pl.BlockSpec((wide, wide), whole))
        out_specs.append(pl.BlockSpec((1, dim, wide), per_e))
        out_shape.append(shape((n_e, dim, wide), BF))
    out_specs += [hbm] * 4
    out_shape += [shape((n_e, 2, TILE, w), BF) for w in (dim, dim, wide, half)]
    got = pl.pallas_call(
        functools.partial(chunk_kernel, first, toks),
        grid_spec=pltpu.PrefetchScalarGridSpec(
            num_scalar_prefetch=1,
            grid=(n_e,),
            in_specs=in_specs,
            out_specs=out_specs,
            scratch_shapes=[
                pltpu.VMEM((2, toks, dim), BF),
                pltpu.VMEM((2, tall, dim), BF),
                pltpu.VMEM((2, 2, toks, dim), BF),
                pltpu.VMEM((2, (tall - toks) // 2, toks), F32),
                pltpu.VMEM((2, (tall - toks) // 2, toks), F32),
                pltpu.VMEM((2, n_e, toks), F32),
                pltpu.VMEM((2, 2 * TILE, dim), BF),
                pltpu.VMEM((2, 2 * TILE, dim), BF),
                pltpu.VMEM((2, 2 * TILE, wide), BF),
                pltpu.VMEM((2, 2 * TILE, half), BF),
                pltpu.VMEM((2, room, toks), BF),
                pltpu.VMEM((2, 2, room, dim), BF),
                pltpu.VMEM((toks, dim), F32),
                pltpu.SMEM((2,), jnp.int32),
                pltpu.SemaphoreType.DMA((2, 2, 4)),
                pltpu.SemaphoreType.DMA((2, 2)),
            ],
        ),
        out_shape=out_shape,
        compiler_params=pltpu.CompilerParams(dimension_semantics=('arbitrary',), vmem_limit_bytes=65000 * 1024),
        cost_estimate=pl.CostEstimate(flops=28_000_000_000, bytes_accessed=40_000_000, transcendentals=0),
        name='experts',
    )(ep, *blocks, w1, w2, b1, b2, *((split,) if first else ()))
    return got[:4], got[4:8], got[-4:], (got[8] if first else w1)


def wgrad_kernel(n_c, first_e, n_prev, nt_ref, *refs):
    hbm = [refs[k * n_c:(k + 1) * n_c] for k in range(4)]
    mix_ref = refs[4 * n_c]
    gw1_ref, gw2_ref, acc1, acc2, *bufs, sems = refs[4 * n_c + 1 + n_prev:]
    e = pl.program_id(0)
    n_e = pl.num_programs(0)
    par = lax.rem(e, 2)

    def fetches(step, c, t, p):
        return [pltpu.make_async_copy(hbm[k][c].at[first_e + step, t], bufs[k].at[p, 2 * c + t], sems.at[p, 2 * c + t, k])
                for k in range(4)]

    def each(step, act):
        for c in range(n_c):
            for t in range(2):
                pl.when(nt_ref[c, first_e + step] > t)(functools.partial(act, c, t))

    def start(step, p):
        def go(c, t):
            for copy in fetches(step, c, t, p):
                copy.start()

        each(step, go)

    @pl.when(e == 0)
    def _():
        start(e, par)

    @pl.when(e + 1 < n_e)
    def _():
        start(e + 1, 1 - par)

    acc1[...] = jnp.zeros_like(acc1)
    acc2[...] = jnp.zeros_like(acc2)

    def add(j, _):
        @pl.when(nt_ref[j // 2, first_e + e] > lax.rem(j, 2))
        def _():
            for k in range(4):
                pltpu.make_async_copy(hbm[k][0].at[0, 0], bufs[k].at[par, j], sems.at[par, j, k]).wait()
            x_rows, d_rows, d_hid, act_w = (buf[par, j] for buf in bufs)
            acc1[...] += dot(x_rows, d_hid, LHS)
            acc2[...] += dot(act_w, d_rows, LHS)

        return 0

    lax.fori_loop(0, 2 * n_c, add, 0)
    gw2_ref[0] = acc2[...].astype(BF)
    gw1_ref[0] = dot(acc1[...].astype(BF), mix_ref[...]).astype(BF)


def run_wgrad(nt, saved, unmix, first_e, n_e, all_e, prev=()):
    n_c = len(saved)
    xs, ds, dh, wa = (list(t) for t in zip(*saved))
    dim, wide, half = xs[0].shape[3], dh[0].shape[3], wa[0].shape[3]
    return pl.pallas_call(
        functools.partial(wgrad_kernel, n_c, first_e, len(prev)),
        grid_spec=pltpu.PrefetchScalarGridSpec(
            num_scalar_prefetch=1,
            grid=(n_e,),
            in_specs=[pl.BlockSpec(memory_space=pl.ANY)] * (4 * n_c) + [pl.BlockSpec((wide, wide), lambda e, nt: (0, 0))]
            + [pl.BlockSpec(memory_space=pl.ANY)] * len(prev),
            out_specs=[pl.BlockSpec((1, dim, wide), lambda e, nt: (first_e + e, 0, 0)), pl.BlockSpec((1, half, dim), lambda e, nt: (first_e + e, 0, 0))],
            scratch_shapes=[pltpu.VMEM((dim, wide), F32), pltpu.VMEM((half, dim), F32)]
            + [pltpu.VMEM((2, 2 * n_c, TILE, w), BF) for w in (dim, dim, wide, half)]
            + [pltpu.SemaphoreType.DMA((2, 2 * n_c, 4))],
        ),
        out_shape=[jax.ShapeDtypeStruct((all_e, dim, wide), BF), jax.ShapeDtypeStruct((all_e, half, dim), BF)],
        input_output_aliases={4 * n_c + 2 + k: k for k in range(len(prev))},
        compiler_params=pltpu.CompilerParams(dimension_semantics=('arbitrary',), vmem_limit_bytes=64000 * 1024),
        cost_estimate=pl.CostEstimate(flops=26_000_000_000, bytes_accessed=60_000_000, transcendentals=0),
        name='weight_grads',
    )(nt, *xs, *ds, *dh, *wa, unmix, *prev)


def pack_kernel(x_ref, d_ref, idx_ref, slot_ref, wr_ref, br_ref, tall_ref, w_ref):
    toks = x_ref.shape[0]
    top_k, n = idx_ref.shape[0], wr_ref.shape[0]
    logits = dot(wr_ref[...], x_ref[...], BACK) + br_ref[...]
    expert = lax.broadcasted_iota(jnp.int32, (n, toks), 0)
    hots = [jnp.broadcast_to(idx_ref[k:k + 1, :], (n, toks)) == expert for k in range(top_k)]
    picked = [jnp.sum(jnp.where(h, logits, 0.0), axis=0, keepdims=True) for h in hots]
    top = functools.reduce(jnp.maximum, picked)
    exps = [jnp.exp(v - top) for v in picked]
    norm = functools.reduce(jnp.add, exps)
    w_full = jnp.zeros((n, toks), F32)
    kept = jnp.zeros((n, toks), F32)
    for k in range(top_k):
        w_full += jnp.where(hots[k], exps[k] / norm, 0.0)
        kept += jnp.where(hots[k], jnp.where(slot_ref[k:k + 1, :] >= 0, 1.0, 0.0), 0.0)
    w_ref[...] = w_full
    ahead = lax.broadcasted_iota(jnp.int32, (toks, toks), 0) < lax.broadcasted_iota(jnp.int32, (toks, toks), 1)
    rank = dot(kept.astype(BF), jnp.where(ahead, 1.0, 0.0).astype(BF))
    rank = jnp.where(kept > 0.0, rank, -1.0)
    w_top = w_full.astype(BF)
    rest = w_full - w_top.astype(F32)
    w_mid = rest.astype(BF)
    w_low = (rest - w_mid.astype(F32)).astype(BF)
    tall_ref[:toks, :] = d_ref[...]
    tall_ref[toks:toks + n, :toks] = w_top
    tall_ref[toks:toks + n, toks:] = w_mid
    tall_ref[toks + n:, :toks] = w_low
    tall_ref[toks + n:, toks:] = rank.astype(BF)


def run_pack(x_loc, dy_loc, idx_t, slot_t, w_router, b_router):
    toks, dim = x_loc.shape
    n = w_router.shape[0]
    return pl.pallas_call(
        pack_kernel,
        out_shape=[jax.ShapeDtypeStruct((toks + 2 * n, dim), BF), jax.ShapeDtypeStruct((n, toks), F32)],
        compiler_params=pltpu.CompilerParams(vmem_limit_bytes=32000 * 1024),
        name='pack',
    )(x_loc, dy_loc, idx_t, slot_t, w_router, b_router)


def router_kernel(rel, me_ref, *refs):
    n = len(rel)
    d_ref, out_ref = refs[n:]
    total = jnp.zeros(out_ref.shape, F32)
    for k in range(n):
        d_one = d_ref[me_ref[0] ^ rel[k]].astype(BF)
        total += lax.dot_general(refs[k][...], d_one, (((0,), (1,)), ((), ())), preferred_element_type=F32)
    out_ref[...] = total


def run_router_grad(me, rel, x_blocks, d_rel):
    n = len(x_blocks)
    toks, dim = x_blocks[0].shape
    experts = d_rel.shape[1]
    cut = dim // 4
    return pl.pallas_call(
        functools.partial(router_kernel, rel),
        grid_spec=pltpu.PrefetchScalarGridSpec(
            num_scalar_prefetch=1,
            grid=(4,),
            in_specs=[pl.BlockSpec((toks, cut), lambda j, me: (0, j))] * n + [pl.BlockSpec(d_rel.shape, lambda j, me: (0, 0, 0))],
            out_specs=pl.BlockSpec((cut, experts), lambda j, me: (j, 0)),
        ),
        out_shape=jax.ShapeDtypeStruct((dim, experts), F32),
        compiler_params=pltpu.CompilerParams(vmem_limit_bytes=32000 * 1024),
        name='router_grad',
    )(me, *x_blocks, d_rel)


def solution(mesh):
    tp_count = mesh.shape['tp']
    ep_count = mesh.shape['ep']
    n_dev = tp_count * ep_count
    tok_spec = P(('ep', 'tp'), None)

    CORE, XF, YF = 2, 4, 1
    FAR = XF | YF
    CHIPS = (0, YF, FAR, XF)

    def flip(arr, bits):
        turned = (bits & 1) * ep_count + (bits >> 1)
        return lax.ppermute(arr, ('tp', 'ep'), [(s, s ^ turned) for s in range(n_dev)])

    def device_fn(x_loc, idx_loc, slot_loc, w_router, b_router, w_gate_up, b_gate_up, w_down, b_down, dy_loc):
        toks, _ = x_loc.shape
        n_experts = w_router.shape[1]
        n_e = w_gate_up.shape[0]
        wide = w_gate_up.shape[2]
        half = wide // 2
        tp_index = lax.axis_index('tp')
        ep_index = lax.axis_index('ep')
        me = ep_index * tp_count + tp_index

        tall, w_full = run_pack(x_loc, dy_loc, idx_loc.T, slot_loc.T, w_router.T, b_router[:, None])

        x_of = {XF: flip(x_loc, XF), YF: flip(x_loc, YF)}
        d_of = {XF: flip(tall, XF | CORE), YF: flip(tall, YF | CORE)}
        x_of[FAR] = flip(x_of[XF], YF)
        d_of[FAR] = flip(d_of[YF], XF)
        pairs = [(x_loc, tall, flip(x_loc, CORE), flip(tall, CORE))]
        for bits in CHIPS[1:]:
            pairs.append((x_of[bits], flip(d_of[bits], CORE), flip(x_of[bits], CORE), d_of[bits]))

        col = jnp.arange(wide)
        split_mat = (jnp.where(col < half, 2 * col, 2 * (col - half) + 1)[None, :] == col[:, None]).astype(BF)
        b1 = jnp.concatenate([b_gate_up[:, 0::2], b_gate_up[:, 1::2]], axis=1)[:, None, :]
        b2 = b_down * (tp_index == 0).astype(F32)
        ep = ep_index.astype(jnp.int32)[None]

        w1 = w_gate_up
        dgs, gb1s, gb2s, nts, saved, part = [], [], [], [], [], []

        def chunk(step, blocks, w1):
            o, small, keep, w1 = run_chunk(ep, blocks, w1, w_down, b1, b2, split_mat if step == 0 else None)
            for lst, v in zip((dgs, gb1s, gb2s, nts), small):
                lst.append(v)
            saved.append(keep)
            ya, dxa, yb, dxb = o
            if step == 0:
                part.append((ya, flip(yb, CORE), dxa, flip(dxb, CORE)))
            else:
                part.append((ya, flip(yb, CORE), dxb, flip(dxa, CORE)))
            return w1

        def both(step):
            ya, yb, dxa, dxb = part[step]
            add = lambda a, b: (a.astype(F32) + b.astype(F32)).astype(BF)
            return add(ya, yb), add(dxa, dxb)

        def hop(step, y, dx):
            bits = CHIPS[step]
            return flip(y, bits), flip(dx, bits | CORE)

        w1 = chunk(0, pairs[0], w_gate_up)
        w1 = chunk(1, pairs[1], w1)
        sum_1, blocks = lax.optimization_barrier((both(1), pairs[2]))
        got_1 = hop(1, *sum_1)
        w1 = chunk(2, blocks, w1)
        sum_2, blocks = lax.optimization_barrier((both(2), pairs[3]))
        got_2 = hop(2, *sum_2)
        chunk(3, blocks, w1)

        rel = [CHIPS[k // 2] ^ (CORE * (k % 2)) for k in range(n_dev)]
        dg_rel = jnp.stack([dg[:, k, :] for dg in dgs for k in range(2)])
        slot_of = jnp.array([rel.index(m) for m in range(n_dev)], jnp.int32)
        dg_abs = dg_rel[slot_of[jnp.arange(n_dev) ^ me]]
        dg_back = lax.all_to_all(dg_abs, ('ep', 'tp'), 0, 0, tiled=True)
        sum_3, nt_all = lax.optimization_barrier((both(3), jnp.stack(nts)))
        got_3 = hop(3, *sum_3)
        unmix = split_mat.T
        part_e = n_e // 2
        grads = run_wgrad(nt_all, saved, unmix, 0, part_e, n_e)
        dg_back, nt_b, grads = lax.optimization_barrier((dg_back, nt_all, grads))
        d_gate = jnp.sum(dg_back.reshape(ep_count, tp_count, n_e, toks), axis=1).reshape(n_experts, toks)
        d_logits = w_full * (d_gate - jnp.sum(w_full * d_gate, axis=0, keepdims=True))
        d_all = lax.all_to_all(jnp.broadcast_to(d_logits[None], (n_dev, *d_logits.shape)), ('ep', 'tp'), 0, 0, tiled=True)
        gw1, gw2 = run_wgrad(nt_b, saved, unmix, part_e, n_e - part_e, n_e, grads)
        gb1 = functools.reduce(jnp.add, gb1s)[:, 0, :]
        gb1 = jnp.stack([gb1[:, :half], gb1[:, half:]], axis=2).reshape(n_e, wide)
        gb2 = functools.reduce(jnp.add, gb2s)

        wide_sum = lambda *terms: functools.reduce(jnp.add, [t.astype(F32) for t in terms])
        via_router = jnp.einsum('et,de->td', d_logits.astype(BF), w_router, preferred_element_type=F32)
        d_all, gw1, own = lax.optimization_barrier((d_all, gw1, part[0]))
        gwr = run_router_grad(me.astype(jnp.int32)[None], rel, [p[k] for p in pairs for k in (0, 2)], d_all)
        gwr, got_3 = lax.optimization_barrier((gwr, got_3))
        moe = wide_sum(own[0], own[1], got_1[0], got_2[0], got_3[0])
        d_x = wide_sum(own[2], own[3], got_1[1], got_2[1], got_3[1], via_router)
        gbr = jnp.sum(d_all, axis=(0, 2))
        return (moe.astype(BF), d_x.astype(BF), gw1, gb1, gw2, gb2, gwr, gbr)

    in_specs = (tok_spec, tok_spec, tok_spec, P(None, None), P(None), P('ep', None, 'tp'), P('ep', 'tp'), P('ep', 'tp', None), P('ep', None), tok_spec)
    out_specs = (tok_spec, tok_spec, P('ep', None, 'tp'), P('ep', 'tp'), P('ep', 'tp', None), P('ep', None), P(None, None), P(None))

    return jax.shard_map(device_fn, mesh=mesh, in_specs=in_specs, out_specs=out_specs, check_vma=False)
```

```python
import functools
import jax
import jax.numpy as jnp
from jax import lax
from jax.experimental import pallas as pl
from jax.experimental.pallas import tpu as pltpu
from jax.sharding import PartitionSpec as P

LIMIT = 7.0
ALPHA = 1.702
BF = jnp.bfloat16
F32 = jnp.float32
TILE = 256
BACK = ((1,), (1,))
LHS = ((0,), (0,))


def dot(a, b, dims=((1,), (0,))):
    return lax.dot_general(a, b, (dims, ((), ())), preferred_element_type=F32)


def split3(v):
    top = v.astype(BF)
    rest = v - top.astype(F32)
    mid = rest.astype(BF)
    return top, mid, (rest - mid.astype(F32)).astype(BF)


def chunk_kernel(first, toks, ep_ref, xa_hbm, da_hbm, xb_hbm, db_hbm, w1_in, w2_ref, b1_ref, b2_ref, *refs):
    if first:
        split_ref, *refs = refs
    ya_hbm, dxa_hbm, yb_hbm, dxb_hbm, dg_ref, gb1_ref, gb2_ref, nt_ref, *refs = refs
    if first:
        w1_ref, *refs = refs
    else:
        w1_ref = w1_in
    xs_hbm, ds_hbm, dh_hbm, wa_hbm, *refs = refs
    xin, din, ost, wst, rst, bst, xbuf, dbuf, dhst, wast, sel, zbuf, acc, off, sems, io_sems = refs
    e = pl.program_id(0)
    n_e = pl.num_programs(0)
    half, dim = w2_ref.shape[1:]
    par = lax.rem(e, 2)
    cuts = [slice(j, j + TILE) for j in range(0, dim, TILE)]
    loads = [[pltpu.make_async_copy(x_h, xin.at[i], io_sems.at[i, 0]), pltpu.make_async_copy(d_h, din.at[i], io_sems.at[i, 1])]
             for i, (x_h, d_h) in enumerate(((xa_hbm, da_hbm), (xb_hbm, db_hbm)))]
    stores = [[pltpu.make_async_copy(ost.at[i, k], o_h, io_sems.at[i, k]) for k, o_h in enumerate(pair)]
              for i, pair in enumerate(((ya_hbm, dxa_hbm), (yb_hbm, dxb_hbm)))]

    def saves(expert, t, p):
        at = pl.ds(t * TILE, TILE)
        pairs = ((xbuf, xs_hbm), (dbuf, ds_hbm), (dhst, dh_hbm), (wast, wa_hbm))
        return [pltpu.make_async_copy(src.at[p, at], dst.at[expert, t], sems.at[p, t, k])
                for k, (src, dst) in enumerate(pairs)]

    def drain(expert, p):
        for t in range(2):
            @pl.when(nt_ref[expert] > t)
            def _():
                for copy in saves(expert, t, p):
                    copy.wait()

    @pl.when(e == 0)
    def _():
        for i in range(2):
            for copy in reversed(loads[i]):
                copy.start()
            off[i] = 0
        sel[...] = jnp.zeros_like(sel)
        zbuf[...] = jnp.zeros_like(zbuf)

    if first:
        w1_ref[0] = dot(w1_in[0], split_ref[...]).astype(BF)

    @pl.when(e == 0)
    def _():
        base = pl.multiple_of(ep_ref[0] * 8, 8)
        b_parts = jnp.concatenate(split3(b2_ref[...]), axis=0)
        for i in range(2):
            for copy in loads[i]:
                copy.wait()

        def prepare(i, _):
            aux = din[i, toks:, :].astype(F32)
            n = aux.shape[0] // 2
            wst[i] = aux[:n, :toks] + aux[:n, toks:] + aux[n:, :toks]
            rst[i] = aux[n:, toks:]
            local_w = wst[i, pl.ds(base, 8), :]
            local_r = rst[i, pl.ds(base, 8), :]
            w_parts = jnp.concatenate(split3(jnp.where(local_r >= 0.0, local_w, 0.0)), axis=0)
            d_all = din[i, :toks, :]
            got = dot(w_parts, d_all)
            gb2_ref[...] += got[:8] + got[8:16] + got[16:]
            got = dot(b_parts, d_all, BACK)
            bst[i] = got[:8] + got[8:16] + got[16:]
            return 0

        gb2_ref[...] = jnp.zeros_like(gb2_ref)
        lax.fori_loop(0, 2, prepare, 0)

    for p in range(2):
        @pl.when((e >= 2) & (par == p))
        def _():
            drain(e - 2, p)

    row = ep_ref[0] * n_e + e
    counts = [(jnp.max(rst[i, pl.ds(row, 1), :]) + 1.0).astype(jnp.int32) for i in range(2)]
    gb1_ref[...] = jnp.zeros_like(gb1_ref)
    b_row = b2_ref[pl.ds(e, 1), :]

    seg = TILE // 2
    parts = ((0, seg), (1, seg))
    for i in range(2):
        dg_ref[0, i:i + 1, :] = jnp.where(rst[i, pl.ds(row, 1), :] >= 0.0, bst[i, pl.ds(e, 1), :], 0.0)

    def tile(t, _):
        base = (t * seg).astype(F32)
        rows = pl.ds(pl.multiple_of(t * TILE, TILE), TILE)
        hots, w_rows, at = [], [], 0
        for i, m in parts:
            pos = lax.broadcasted_iota(jnp.int32, (m, toks), 0).astype(F32)
            hot = jnp.broadcast_to(rst[i, pl.ds(row, 1), :] - base, (m, toks)) == pos
            hot_b = jnp.where(hot, 1.0, 0.0).astype(BF)
            sel[i, pl.ds(pl.multiple_of(off[i], 16), m), :] = hot_b
            w_rows.append(jnp.sum(jnp.where(hot, jnp.broadcast_to(wst[i, pl.ds(row, 1), :], (m, toks)), 0.0), axis=1, keepdims=True))
            hots.append(hot)
            dst = pl.ds(pl.multiple_of(t * TILE + at, 128), m)
            for c in cuts:
                xbuf[par, dst, c] = dot(hot_b, xin[i, :, c]).astype(BF)
            for c in cuts:
                dbuf[par, dst, c] = dot(hot_b, din[i, :toks, c]).astype(BF)
            at += m
        w_row = jnp.concatenate(w_rows, axis=0)
        x_rows = xbuf[par, rows, :]
        gate = dot(x_rows, w1_ref[0, :, :half]) + b1_ref[0, :, :half]
        up = dot(x_rows, w1_ref[0, :, half:]) + b1_ref[0, :, half:]
        d_raw = dot(dbuf[par, rows, :], w2_ref[0], BACK)
        g = jnp.minimum(gate, LIMIT)
        u1 = jnp.clip(up, -LIMIT, LIMIT) + 1.0
        sg = jax.nn.sigmoid(ALPHA * g)
        gs = g * sg
        act = (gs * u1).astype(BF)
        act_w = act.astype(F32)
        wast[par, rows, :] = (w_row * act_w).astype(BF)
        dg_row = jnp.sum(act_w * d_raw, axis=1, keepdims=True)
        d_act = w_row * d_raw
        gate_on = jnp.where(gate < LIMIT, 1.0, jnp.where(gate == LIMIT, 0.5, 0.0))
        up_abs = jnp.abs(up)
        up_on = jnp.where(up_abs < LIMIT, 1.0, jnp.where(up_abs == LIMIT, 0.5, 0.0))
        d_gate = d_act * u1 * (sg * (1.0 + ALPHA * g * (1.0 - sg))) * gate_on
        d_up = d_act * gs * up_on
        gb1_ref[0, :, :half] += jnp.sum(d_gate, axis=0, keepdims=True)
        gb1_ref[0, :, half:] += jnp.sum(d_up, axis=0, keepdims=True)
        dhst[par, rows, :half] = d_gate.astype(BF)
        dhst[par, rows, half:] = d_up.astype(BF)
        d_hid = dhst[par, rows, :]

        def put(k, c, value):
            at = 0
            for i, m in parts:
                zbuf[k, i, pl.ds(pl.multiple_of(off[i], 16), m), c] = value[at:at + m]
                at += m

        for c in cuts:
            part = (dot(act, w2_ref[0, :, c]) + b_row[:, c]).astype(BF).astype(F32)
            put(0, c, (w_row * part).astype(BF))
        for c in cuts:
            put(1, c, dot(d_hid, w1_ref[0, c, :], BACK).astype(BF))
        for copy in saves(e, t, par):
            copy.start()
        at = 0
        for (i, m), hot in zip(parts, hots):
            dg = jnp.sum(jnp.where(hot, dg_row[at:at + m], 0.0), axis=0, keepdims=True)
            dg_ref[0, i:i + 1, :] += dg
            used = jnp.clip(counts[i] - t * seg, 0, seg)
            off[i] = off[i] + (used + 15) // 16 * 16
            at += m

        return 0

    n_pass = jnp.maximum((jnp.maximum(counts[0], counts[1]) + seg - 1) // seg, 1)
    nt_ref[e] = n_pass
    lax.fori_loop(0, n_pass, tile, 0)

    @pl.when(e == n_e - 1)
    def _():
        long = 4 * TILE

        def combine(j):
            i, k = j // 2, lax.rem(j, 2)
            total = off[i]
            acc[...] = dot(sel[i, :long, :], zbuf[k, i, :long, :], LHS)

            def step(q, _):
                at = pl.ds(pl.multiple_of(q * TILE, TILE), TILE)
                acc[...] += dot(sel[i, at, :], zbuf[k, i, at, :], LHS)
                return 0

            lax.fori_loop(4, (total + TILE - 1) // TILE, step, 0)
            ost[i, k] = acc[...].astype(BF)
            return 0

        def go(j, _):
            combine(j)
            for q in range(4):
                @pl.when(j == q)
                def _():
                    stores[q // 2][q % 2].start()
            return 0

        lax.fori_loop(0, 4, go, 0)
        for back in (1, 0):
            p = lax.rem(e - back, 2)
            drain(e - back, p)
        for i in range(2):
            for copy in stores[i]:
                copy.wait()


def run_chunk(ep, blocks, w1, w2, b1, b2, split=None):
    first = split is not None
    n_e, dim, wide = w1.shape
    half = w2.shape[1]
    toks, tall = blocks[0].shape[0], blocks[1].shape[0]
    whole = lambda e, ep: (0, 0)
    per_e = lambda e, ep: (e, 0, 0)
    room = n_e * TILE + TILE
    hbm = pl.BlockSpec(memory_space=pl.ANY)
    in_specs = [
        hbm, hbm, hbm, hbm,
        pl.BlockSpec((1, dim, wide), per_e),
        pl.BlockSpec((1, half, dim), per_e),
        pl.BlockSpec((1, 1, wide), per_e),
        pl.BlockSpec((n_e, dim), whole),
    ]
    out_specs = [
        hbm, hbm, hbm, hbm,
        pl.BlockSpec((1, 2, toks), per_e),
        pl.BlockSpec((1, 1, wide), per_e),
        pl.BlockSpec((n_e, dim), whole),
        pl.BlockSpec(memory_space=pltpu.SMEM),
    ]
    shape = jax.ShapeDtypeStruct
    out_shape = [
        *[shape((toks, dim), BF)] * 4, shape((n_e, 2, toks), F32),
        shape((n_e, 1, wide), F32), shape((n_e, dim), F32), shape((n_e,), jnp.int32),
    ]
    if first:
        in_specs.append(pl.BlockSpec((wide, wide), whole))
        out_specs.append(pl.BlockSpec((1, dim, wide), per_e))
        out_shape.append(shape((n_e, dim, wide), BF))
    out_specs += [hbm] * 4
    out_shape += [shape((n_e, 2, TILE, w), BF) for w in (dim, dim, wide, half)]
    got = pl.pallas_call(
        functools.partial(chunk_kernel, first, toks),
        grid_spec=pltpu.PrefetchScalarGridSpec(
            num_scalar_prefetch=1,
            grid=(n_e,),
            in_specs=in_specs,
            out_specs=out_specs,
            scratch_shapes=[
                pltpu.VMEM((2, toks, dim), BF),
                pltpu.VMEM((2, tall, dim), BF),
                pltpu.VMEM((2, 2, toks, dim), BF),
                pltpu.VMEM((2, (tall - toks) // 2, toks), F32),
                pltpu.VMEM((2, (tall - toks) // 2, toks), F32),
                pltpu.VMEM((2, n_e, toks), F32),
                pltpu.VMEM((2, 2 * TILE, dim), BF),
                pltpu.VMEM((2, 2 * TILE, dim), BF),
                pltpu.VMEM((2, 2 * TILE, wide), BF),
                pltpu.VMEM((2, 2 * TILE, half), BF),
                pltpu.VMEM((2, room, toks), BF),
                pltpu.VMEM((2, 2, room, dim), BF),
                pltpu.VMEM((toks, dim), F32),
                pltpu.SMEM((2,), jnp.int32),
                pltpu.SemaphoreType.DMA((2, 2, 4)),
                pltpu.SemaphoreType.DMA((2, 2)),
            ],
        ),
        out_shape=out_shape,
        compiler_params=pltpu.CompilerParams(dimension_semantics=('arbitrary',), vmem_limit_bytes=65000 * 1024),
        cost_estimate=pl.CostEstimate(flops=28_000_000_000, bytes_accessed=40_000_000, transcendentals=0),
        name='experts',
    )(ep, *blocks, w1, w2, b1, b2, *((split,) if first else ()))
    return got[:4], got[4:8], got[-4:], (got[8] if first else w1)


def wgrad_kernel(n_c, *refs):
    nts, refs = refs[:n_c], refs[n_c:]
    hbm = [refs[k * n_c:(k + 1) * n_c] for k in range(4)]
    mix_ref, gw1_ref, gw2_ref, nt_ref, acc1, acc2, *bufs, sems = refs[4 * n_c:]
    e = pl.program_id(0)
    n_e = pl.num_programs(0)
    par = lax.rem(e, 2)

    def fetches(step, c, t, p):
        return [pltpu.make_async_copy(hbm[k][c].at[step, t], bufs[k].at[p, 2 * c + t], sems.at[p, 2 * c + t, k])
                for k in range(4)]

    def each(step, act):
        for c in range(n_c):
            for t in range(2):
                pl.when(nt_ref[c, step] > t)(functools.partial(act, c, t))

    def start(step, p):
        def go(c, t):
            for copy in fetches(step, c, t, p):
                copy.start()

        each(step, go)

    @pl.when(e == 0)
    def _():
        for c in range(n_c):
            for k in range(nts[c].shape[0]):
                nt_ref[c, k] = nts[c][k]
        start(e, par)

    @pl.when(e + 1 < n_e)
    def _():
        start(e + 1, 1 - par)

    acc1[...] = jnp.zeros_like(acc1)
    acc2[...] = jnp.zeros_like(acc2)

    def add(j, _):
        @pl.when(nt_ref[j // 2, e] > lax.rem(j, 2))
        def _():
            for k in range(4):
                pltpu.make_async_copy(hbm[k][0].at[0, 0], bufs[k].at[par, j], sems.at[par, j, k]).wait()
            x_rows, d_rows, d_hid, act_w = (buf[par, j] for buf in bufs)
            acc1[...] += dot(x_rows, d_hid, LHS)
            acc2[...] += dot(act_w, d_rows, LHS)

        return 0

    lax.fori_loop(0, 2 * n_c, add, 0)
    gw2_ref[0] = acc2[...].astype(BF)
    gw1_ref[0] = dot(acc1[...].astype(BF), mix_ref[...]).astype(BF)


def run_wgrad(nts, saved, unmix):
    n_c = len(saved)
    xs, ds, dh, wa = (list(t) for t in zip(*saved))
    n_e, dim, wide, half = xs[0].shape[0], xs[0].shape[3], dh[0].shape[3], wa[0].shape[3]
    per_e = lambda e, *nts: (e, 0, 0)
    return pl.pallas_call(
        functools.partial(wgrad_kernel, n_c),
        grid_spec=pltpu.PrefetchScalarGridSpec(
            num_scalar_prefetch=n_c,
            grid=(n_e,),
            in_specs=[pl.BlockSpec(memory_space=pl.ANY)] * (4 * n_c) + [pl.BlockSpec((wide, wide), lambda e, *nts: (0, 0))],
            out_specs=[pl.BlockSpec((1, dim, wide), per_e), pl.BlockSpec((1, half, dim), per_e)],
            scratch_shapes=[pltpu.SMEM((n_c, n_e), jnp.int32), pltpu.VMEM((dim, wide), F32), pltpu.VMEM((half, dim), F32)]
            + [pltpu.VMEM((2, 2 * n_c, TILE, w), BF) for w in (dim, dim, wide, half)]
            + [pltpu.SemaphoreType.DMA((2, 2 * n_c, 4))],
        ),
        out_shape=[jax.ShapeDtypeStruct((n_e, dim, wide), BF), jax.ShapeDtypeStruct((n_e, half, dim), BF)],
        compiler_params=pltpu.CompilerParams(dimension_semantics=('arbitrary',), vmem_limit_bytes=64000 * 1024),
        cost_estimate=pl.CostEstimate(flops=26_000_000_000, bytes_accessed=60_000_000, transcendentals=0),
        name='weight_grads',
    )(*nts, *xs, *ds, *dh, *wa, unmix)


def pack_kernel(x_ref, d_ref, idx_ref, slot_ref, wr_ref, br_ref, tall_ref, w_ref):
    toks = x_ref.shape[0]
    top_k, n = idx_ref.shape[0], wr_ref.shape[0]
    logits = dot(wr_ref[...], x_ref[...], BACK) + br_ref[...]
    expert = lax.broadcasted_iota(jnp.int32, (n, toks), 0)
    hots = [jnp.broadcast_to(idx_ref[k:k + 1, :], (n, toks)) == expert for k in range(top_k)]
    picked = [jnp.sum(jnp.where(h, logits, 0.0), axis=0, keepdims=True) for h in hots]
    top = functools.reduce(jnp.maximum, picked)
    exps = [jnp.exp(v - top) for v in picked]
    norm = functools.reduce(jnp.add, exps)
    w_full = jnp.zeros((n, toks), F32)
    kept = jnp.zeros((n, toks), F32)
    for k in range(top_k):
        w_full += jnp.where(hots[k], exps[k] / norm, 0.0)
        kept += jnp.where(hots[k], jnp.where(slot_ref[k:k + 1, :] >= 0, 1.0, 0.0), 0.0)
    w_ref[...] = w_full
    ahead = lax.broadcasted_iota(jnp.int32, (toks, toks), 0) < lax.broadcasted_iota(jnp.int32, (toks, toks), 1)
    rank = dot(kept.astype(BF), jnp.where(ahead, 1.0, 0.0).astype(BF))
    rank = jnp.where(kept > 0.0, rank, -1.0)
    w_top = w_full.astype(BF)
    rest = w_full - w_top.astype(F32)
    w_mid = rest.astype(BF)
    w_low = (rest - w_mid.astype(F32)).astype(BF)
    tall_ref[:toks, :] = d_ref[...]
    tall_ref[toks:toks + n, :toks] = w_top
    tall_ref[toks:toks + n, toks:] = w_mid
    tall_ref[toks + n:, :toks] = w_low
    tall_ref[toks + n:, toks:] = rank.astype(BF)


def run_pack(x_loc, dy_loc, idx_t, slot_t, w_router, b_router):
    toks, dim = x_loc.shape
    n = w_router.shape[0]
    return pl.pallas_call(
        pack_kernel,
        out_shape=[jax.ShapeDtypeStruct((toks + 2 * n, dim), BF), jax.ShapeDtypeStruct((n, toks), F32)],
        compiler_params=pltpu.CompilerParams(vmem_limit_bytes=32000 * 1024),
        name='pack',
    )(x_loc, dy_loc, idx_t, slot_t, w_router, b_router)


def router_kernel(rel, me_ref, *refs):
    n = len(rel)
    d_ref, out_ref = refs[n:]
    total = jnp.zeros(out_ref.shape, F32)
    for k in range(n):
        d_one = d_ref[me_ref[0] ^ rel[k]].astype(BF)
        total += lax.dot_general(refs[k][...], d_one, (((0,), (1,)), ((), ())), preferred_element_type=F32)
    out_ref[...] = total


def run_router_grad(me, rel, x_blocks, d_rel):
    n = len(x_blocks)
    toks, dim = x_blocks[0].shape
    experts = d_rel.shape[1]
    cut = dim // 4
    return pl.pallas_call(
        functools.partial(router_kernel, rel),
        grid_spec=pltpu.PrefetchScalarGridSpec(
            num_scalar_prefetch=1,
            grid=(4,),
            in_specs=[pl.BlockSpec((toks, cut), lambda j, me: (0, j))] * n + [pl.BlockSpec(d_rel.shape, lambda j, me: (0, 0, 0))],
            out_specs=pl.BlockSpec((cut, experts), lambda j, me: (j, 0)),
        ),
        out_shape=jax.ShapeDtypeStruct((dim, experts), F32),
        compiler_params=pltpu.CompilerParams(vmem_limit_bytes=32000 * 1024),
        name='router_grad',
    )(me, *x_blocks, d_rel)


def solution(mesh):
    tp_count = mesh.shape['tp']
    ep_count = mesh.shape['ep']
    n_dev = tp_count * ep_count
    tok_spec = P(('ep', 'tp'), None)

    CORE, XF, YF = 2, 4, 1
    FAR = XF | YF
    CHIPS = (0, YF, FAR, XF)

    def flip(arr, bits):
        turned = (bits & 1) * ep_count + (bits >> 1)
        return lax.ppermute(arr, ('tp', 'ep'), [(s, s ^ turned) for s in range(n_dev)])

    def device_fn(x_loc, idx_loc, slot_loc, w_router, b_router, w_gate_up, b_gate_up, w_down, b_down, dy_loc):
        toks, _ = x_loc.shape
        n_experts = w_router.shape[1]
        n_e = w_gate_up.shape[0]
        wide = w_gate_up.shape[2]
        half = wide // 2
        tp_index = lax.axis_index('tp')
        ep_index = lax.axis_index('ep')
        me = ep_index * tp_count + tp_index

        tall, w_full = run_pack(x_loc, dy_loc, idx_loc.T, slot_loc.T, w_router.T, b_router[:, None])

        x_of = {XF: flip(x_loc, XF), YF: flip(x_loc, YF)}
        d_of = {XF: flip(tall, XF | CORE), YF: flip(tall, YF | CORE)}
        x_of[FAR] = flip(x_of[XF], YF)
        d_of[FAR] = flip(d_of[YF], XF)
        pairs = [(x_loc, tall, flip(x_loc, CORE), flip(tall, CORE))]
        for bits in CHIPS[1:]:
            pairs.append((x_of[bits], flip(d_of[bits], CORE), flip(x_of[bits], CORE), d_of[bits]))

        col = jnp.arange(wide)
        split_mat = (jnp.where(col < half, 2 * col, 2 * (col - half) + 1)[None, :] == col[:, None]).astype(BF)
        b1 = jnp.concatenate([b_gate_up[:, 0::2], b_gate_up[:, 1::2]], axis=1)[:, None, :]
        b2 = b_down * (tp_index == 0).astype(F32)
        ep = ep_index.astype(jnp.int32)[None]

        w1 = w_gate_up
        dgs, gb1s, gb2s, nts, saved, part = [], [], [], [], [], []

        def chunk(step, blocks, w1):
            o, small, keep, w1 = run_chunk(ep, blocks, w1, w_down, b1, b2, split_mat if step == 0 else None)
            for lst, v in zip((dgs, gb1s, gb2s, nts), small):
                lst.append(v)
            saved.append(keep)
            ya, dxa, yb, dxb = o
            if step == 0:
                part.append((ya, flip(yb, CORE), dxa, flip(dxb, CORE)))
            else:
                part.append((ya, flip(yb, CORE), dxb, flip(dxa, CORE)))
            return w1

        def both(step):
            ya, yb, dxa, dxb = part[step]
            add = lambda a, b: (a.astype(F32) + b.astype(F32)).astype(BF)
            return add(ya, yb), add(dxa, dxb)

        def hop(step, y, dx):
            bits = CHIPS[step]
            return flip(y, bits), flip(dx, bits | CORE)

        w1 = chunk(0, pairs[0], w_gate_up)
        w1 = chunk(1, pairs[1], w1)
        sum_1, blocks = lax.optimization_barrier((both(1), pairs[2]))
        got_1 = hop(1, *sum_1)
        w1 = chunk(2, blocks, w1)
        sum_2, blocks = lax.optimization_barrier((both(2), pairs[3]))
        got_2 = hop(2, *sum_2)
        chunk(3, blocks, w1)

        rel = [CHIPS[k // 2] ^ (CORE * (k % 2)) for k in range(n_dev)]
        dg_rel = jnp.stack([dg[:, k, :] for dg in dgs for k in range(2)])
        slot_of = jnp.array([rel.index(m) for m in range(n_dev)], jnp.int32)
        dg_abs = dg_rel[slot_of[jnp.arange(n_dev) ^ me]]
        dg_back = lax.all_to_all(dg_abs, ('ep', 'tp'), 0, 0, tiled=True)
        d_gate = jnp.sum(dg_back.reshape(ep_count, tp_count, n_e, toks), axis=1).reshape(n_experts, toks)
        d_logits = w_full * (d_gate - jnp.sum(w_full * d_gate, axis=0, keepdims=True))
        sum_3, d_logits, last = lax.optimization_barrier((both(3), d_logits, saved[3]))
        d_all = lax.all_to_all(jnp.broadcast_to(d_logits[None], (n_dev, *d_logits.shape)), ('ep', 'tp'), 0, 0, tiled=True)
        got_3 = hop(3, *sum_3)
        gw1, gw2 = run_wgrad(nts, [*saved[:3], last], split_mat.T)
        gb1 = functools.reduce(jnp.add, gb1s)[:, 0, :]
        gb1 = jnp.stack([gb1[:, :half], gb1[:, half:]], axis=2).reshape(n_e, wide)
        gb2 = functools.reduce(jnp.add, gb2s)

        wide_sum = lambda *terms: functools.reduce(jnp.add, [t.astype(F32) for t in terms])
        via_router = jnp.einsum('et,de->td', d_logits.astype(BF), w_router, preferred_element_type=F32)
        d_all, gw1, own = lax.optimization_barrier((d_all, gw1, part[0]))
        gwr = run_router_grad(me.astype(jnp.int32)[None], rel, [p[k] for p in pairs for k in (0, 2)], d_all)
        gwr, got_3 = lax.optimization_barrier((gwr, got_3))
        moe = wide_sum(own[0], own[1], got_1[0], got_2[0], got_3[0])
        d_x = wide_sum(own[2], own[3], got_1[1], got_2[1], got_3[1], via_router)
        gbr = jnp.sum(d_all, axis=(0, 2))
        return (moe.astype(BF), d_x.astype(BF), gw1, gb1, gw2, gb2, gwr, gbr)

    in_specs = (tok_spec, tok_spec, tok_spec, P(None, None), P(None), P('ep', None, 'tp'), P('ep', 'tp'), P('ep', 'tp', None), P('ep', None), tok_spec)
    out_specs = (tok_spec, tok_spec, P('ep', None, 'tp'), P('ep', 'tp'), P('ep', 'tp', None), P('ep', None), P(None, None), P(None))

    return jax.shard_map(device_fn, mesh=mesh, in_specs=in_specs, out_specs=out_specs, check_vma=False)
```

```python
import functools
import jax
import jax.numpy as jnp
from jax import lax
from jax.experimental import pallas as pl
from jax.experimental.pallas import tpu as pltpu
from jax.sharding import PartitionSpec as P

LIMIT = 7.0
ALPHA = 1.702
BF = jnp.bfloat16
F32 = jnp.float32
TILE = 256
BACK = ((1,), (1,))
LHS = ((0,), (0,))


def dot(a, b, dims=((1,), (0,))):
    return lax.dot_general(a, b, (dims, ((), ())), preferred_element_type=F32)


def split3(v):
    top = v.astype(BF)
    rest = v - top.astype(F32)
    mid = rest.astype(BF)
    return top, mid, (rest - mid.astype(F32)).astype(BF)


def chunk_kernel(first, toks, ep_ref, xa_hbm, da_hbm, xb_hbm, db_hbm, w1_in, w2_ref, b1_ref, b2_ref, *refs):
    if first:
        split_ref, *refs = refs
    ya_hbm, dxa_hbm, yb_hbm, dxb_hbm, dg_ref, gb1_ref, gb2_ref, nt_ref, *refs = refs
    if first:
        w1_ref, *refs = refs
    else:
        w1_ref = w1_in
    xs_hbm, ds_hbm, dh_hbm, wa_hbm, *refs = refs
    xin, din, ost, wst, rst, bst, xbuf, dbuf, dhst, wast, sel, zbuf, acc, off, sems, io_sems = refs
    e = pl.program_id(0)
    n_e = pl.num_programs(0)
    half, dim = w2_ref.shape[1:]
    par = lax.rem(e, 2)
    cuts = [slice(j, j + TILE) for j in range(0, dim, TILE)]
    loads = [[pltpu.make_async_copy(x_h, xin.at[i], io_sems.at[i, 0]), pltpu.make_async_copy(d_h, din.at[i], io_sems.at[i, 1])]
             for i, (x_h, d_h) in enumerate(((xa_hbm, da_hbm), (xb_hbm, db_hbm)))]
    stores = [[pltpu.make_async_copy(ost.at[i, k], o_h, io_sems.at[i, k]) for k, o_h in enumerate(pair)]
              for i, pair in enumerate(((ya_hbm, dxa_hbm), (yb_hbm, dxb_hbm)))]

    def saves(expert, t, p):
        at = pl.ds(t * TILE, TILE)
        pairs = ((xbuf, xs_hbm), (dbuf, ds_hbm), (dhst, dh_hbm), (wast, wa_hbm))
        return [pltpu.make_async_copy(src.at[p, at], dst.at[expert, t], sems.at[p, t, k])
                for k, (src, dst) in enumerate(pairs)]

    def drain(expert, p):
        for t in range(2):
            @pl.when(nt_ref[expert] > t)
            def _():
                for copy in saves(expert, t, p):
                    copy.wait()

    @pl.when(e == 0)
    def _():
        for i in range(2):
            for copy in reversed(loads[i]):
                copy.start()
            off[i] = 0
        sel[...] = jnp.zeros_like(sel)
        zbuf[...] = jnp.zeros_like(zbuf)

    if first:
        w1_ref[0] = dot(w1_in[0], split_ref[...]).astype(BF)

    @pl.when(e == 0)
    def _():
        base = pl.multiple_of(ep_ref[0] * 8, 8)
        b_parts = jnp.concatenate(split3(b2_ref[...]), axis=0)
        for i in range(2):
            for copy in loads[i]:
                copy.wait()

        def prepare(i, _):
            aux = din[i, toks:, :].astype(F32)
            n = aux.shape[0] // 2
            wst[i] = aux[:n, :toks] + aux[:n, toks:] + aux[n:, :toks]
            rst[i] = aux[n:, toks:]
            local_w = wst[i, pl.ds(base, 8), :]
            local_r = rst[i, pl.ds(base, 8), :]
            w_parts = jnp.concatenate(split3(jnp.where(local_r >= 0.0, local_w, 0.0)), axis=0)
            d_all = din[i, :toks, :]
            got = dot(w_parts, d_all)
            gb2_ref[...] += got[:8] + got[8:16] + got[16:]
            got = dot(b_parts, d_all, BACK)
            bst[i] = got[:8] + got[8:16] + got[16:]
            return 0

        gb2_ref[...] = jnp.zeros_like(gb2_ref)
        lax.fori_loop(0, 2, prepare, 0)

    for p in range(2):
        @pl.when((e >= 2) & (par == p))
        def _():
            drain(e - 2, p)

    row = ep_ref[0] * n_e + e
    counts = [(jnp.max(rst[i, pl.ds(row, 1), :]) + 1.0).astype(jnp.int32) for i in range(2)]
    gb1_ref[...] = jnp.zeros_like(gb1_ref)
    b_row = b2_ref[pl.ds(e, 1), :]

    seg = TILE // 2
    parts = ((0, seg), (1, seg))
    for i in range(2):
        dg_ref[0, i:i + 1, :] = jnp.where(rst[i, pl.ds(row, 1), :] >= 0.0, bst[i, pl.ds(e, 1), :], 0.0)

    def tile(t, _):
        base = (t * seg).astype(F32)
        rows = pl.ds(pl.multiple_of(t * TILE, TILE), TILE)
        hots, w_rows, at = [], [], 0
        for i, m in parts:
            pos = lax.broadcasted_iota(jnp.int32, (m, toks), 0).astype(F32)
            hot = jnp.broadcast_to(rst[i, pl.ds(row, 1), :] - base, (m, toks)) == pos
            hot_b = jnp.where(hot, 1.0, 0.0).astype(BF)
            sel[i, pl.ds(pl.multiple_of(off[i], 16), m), :] = hot_b
            w_rows.append(jnp.sum(jnp.where(hot, jnp.broadcast_to(wst[i, pl.ds(row, 1), :], (m, toks)), 0.0), axis=1, keepdims=True))
            hots.append(hot)
            dst = pl.ds(pl.multiple_of(t * TILE + at, 128), m)
            for c in cuts:
                xbuf[par, dst, c] = dot(hot_b, xin[i, :, c]).astype(BF)
            for c in cuts:
                dbuf[par, dst, c] = dot(hot_b, din[i, :toks, c]).astype(BF)
            at += m
        w_row = jnp.concatenate(w_rows, axis=0)
        x_rows = xbuf[par, rows, :]
        gate = dot(x_rows, w1_ref[0, :, :half]) + b1_ref[0, :, :half]
        up = dot(x_rows, w1_ref[0, :, half:]) + b1_ref[0, :, half:]
        d_raw = dot(dbuf[par, rows, :], w2_ref[0], BACK)
        g = jnp.minimum(gate, LIMIT)
        u1 = jnp.clip(up, -LIMIT, LIMIT) + 1.0
        sg = jax.nn.sigmoid(ALPHA * g)
        gs = g * sg
        act = (gs * u1).astype(BF)
        act_w = act.astype(F32)
        wast[par, rows, :] = (w_row * act_w).astype(BF)
        dg_row = jnp.sum(act_w * d_raw, axis=1, keepdims=True)
        d_act = w_row * d_raw
        gate_on = jnp.where(gate < LIMIT, 1.0, jnp.where(gate == LIMIT, 0.5, 0.0))
        up_abs = jnp.abs(up)
        up_on = jnp.where(up_abs < LIMIT, 1.0, jnp.where(up_abs == LIMIT, 0.5, 0.0))
        d_gate = d_act * u1 * (sg + ALPHA * gs * (1.0 - sg)) * gate_on
        d_up = d_act * gs * up_on
        gb1_ref[0, :, :half] += jnp.sum(d_gate, axis=0, keepdims=True)
        gb1_ref[0, :, half:] += jnp.sum(d_up, axis=0, keepdims=True)
        dhst[par, rows, :half] = d_gate.astype(BF)
        dhst[par, rows, half:] = d_up.astype(BF)
        d_hid = dhst[par, rows, :]

        def put(k, c, value):
            at = 0
            for i, m in parts:
                zbuf[k, i, pl.ds(pl.multiple_of(off[i], 16), m), c] = value[at:at + m]
                at += m

        for c in cuts:
            part = (dot(act, w2_ref[0, :, c]) + b_row[:, c]).astype(BF).astype(F32)
            put(0, c, (w_row * part).astype(BF))
        for c in cuts:
            put(1, c, dot(d_hid, w1_ref[0, c, :], BACK).astype(BF))
        for copy in saves(e, t, par):
            copy.start()
        at = 0
        for (i, m), hot in zip(parts, hots):
            dg = jnp.sum(jnp.where(hot, dg_row[at:at + m], 0.0), axis=0, keepdims=True)
            dg_ref[0, i:i + 1, :] += dg
            used = jnp.clip(counts[i] - t * seg, 0, seg)
            off[i] = off[i] + (used + 15) // 16 * 16
            at += m

        return 0

    n_pass = jnp.maximum((jnp.maximum(counts[0], counts[1]) + seg - 1) // seg, 1)
    nt_ref[e] = n_pass
    lax.fori_loop(0, n_pass, tile, 0)

    @pl.when(e == n_e - 1)
    def _():
        long = 4 * TILE

        def combine(j):
            i, k = j // 2, lax.rem(j, 2)
            total = off[i]
            acc[...] = dot(sel[i, :long, :], zbuf[k, i, :long, :], LHS)

            def step(q, _):
                at = pl.ds(pl.multiple_of(q * TILE, TILE), TILE)
                acc[...] += dot(sel[i, at, :], zbuf[k, i, at, :], LHS)
                return 0

            lax.fori_loop(4, (total + TILE - 1) // TILE, step, 0)
            ost[i, k] = acc[...].astype(BF)
            return 0

        def go(j, _):
            combine(j)
            for q in range(4):
                @pl.when(j == q)
                def _():
                    stores[q // 2][q % 2].start()
            return 0

        lax.fori_loop(0, 4, go, 0)
        for back in (1, 0):
            p = lax.rem(e - back, 2)
            drain(e - back, p)
        for i in range(2):
            for copy in stores[i]:
                copy.wait()


def run_chunk(ep, blocks, w1, w2, b1, b2, split=None):
    first = split is not None
    n_e, dim, wide = w1.shape
    half = w2.shape[1]
    toks, tall = blocks[0].shape[0], blocks[1].shape[0]
    whole = lambda e, ep: (0, 0)
    per_e = lambda e, ep: (e, 0, 0)
    room = n_e * TILE + TILE
    hbm = pl.BlockSpec(memory_space=pl.ANY)
    in_specs = [
        hbm, hbm, hbm, hbm,
        pl.BlockSpec((1, dim, wide), per_e),
        pl.BlockSpec((1, half, dim), per_e),
        pl.BlockSpec((1, 1, wide), per_e),
        pl.BlockSpec((n_e, dim), whole),
    ]
    out_specs = [
        hbm, hbm, hbm, hbm,
        pl.BlockSpec((1, 2, toks), per_e),
        pl.BlockSpec((1, 1, wide), per_e),
        pl.BlockSpec((n_e, dim), whole),
        pl.BlockSpec(memory_space=pltpu.SMEM),
    ]
    shape = jax.ShapeDtypeStruct
    out_shape = [
        *[shape((toks, dim), BF)] * 4, shape((n_e, 2, toks), F32),
        shape((n_e, 1, wide), F32), shape((n_e, dim), F32), shape((n_e,), jnp.int32),
    ]
    if first:
        in_specs.append(pl.BlockSpec((wide, wide), whole))
        out_specs.append(pl.BlockSpec((1, dim, wide), per_e))
        out_shape.append(shape((n_e, dim, wide), BF))
    out_specs += [hbm] * 4
    out_shape += [shape((n_e, 2, TILE, w), BF) for w in (dim, dim, wide, half)]
    got = pl.pallas_call(
        functools.partial(chunk_kernel, first, toks),
        grid_spec=pltpu.PrefetchScalarGridSpec(
            num_scalar_prefetch=1,
            grid=(n_e,),
            in_specs=in_specs,
            out_specs=out_specs,
            scratch_shapes=[
                pltpu.VMEM((2, toks, dim), BF),
                pltpu.VMEM((2, tall, dim), BF),
                pltpu.VMEM((2, 2, toks, dim), BF),
                pltpu.VMEM((2, (tall - toks) // 2, toks), F32),
                pltpu.VMEM((2, (tall - toks) // 2, toks), F32),
                pltpu.VMEM((2, n_e, toks), F32),
                pltpu.VMEM((2, 2 * TILE, dim), BF),
                pltpu.VMEM((2, 2 * TILE, dim), BF),
                pltpu.VMEM((2, 2 * TILE, wide), BF),
                pltpu.VMEM((2, 2 * TILE, half), BF),
                pltpu.VMEM((2, room, toks), BF),
                pltpu.VMEM((2, 2, room, dim), BF),
                pltpu.VMEM((toks, dim), F32),
                pltpu.SMEM((2,), jnp.int32),
                pltpu.SemaphoreType.DMA((2, 2, 4)),
                pltpu.SemaphoreType.DMA((2, 2)),
            ],
        ),
        out_shape=out_shape,
        compiler_params=pltpu.CompilerParams(dimension_semantics=('arbitrary',), vmem_limit_bytes=65000 * 1024),
        cost_estimate=pl.CostEstimate(flops=28_000_000_000, bytes_accessed=40_000_000, transcendentals=0),
        name='experts',
    )(ep, *blocks, w1, w2, b1, b2, *((split,) if first else ()))
    return got[:4], got[4:8], got[-4:], (got[8] if first else w1)


def wgrad_kernel(n_c, *refs):
    nts, refs = refs[:n_c], refs[n_c:]
    hbm = [refs[k * n_c:(k + 1) * n_c] for k in range(4)]
    mix_ref, gw1_ref, gw2_ref, nt_ref, acc1, acc2, *bufs, sems = refs[4 * n_c:]
    e = pl.program_id(0)
    n_e = pl.num_programs(0)
    par = lax.rem(e, 2)

    def fetches(step, c, t, p):
        return [pltpu.make_async_copy(hbm[k][c].at[step, t], bufs[k].at[p, 2 * c + t], sems.at[p, 2 * c + t, k])
                for k in range(4)]

    def each(step, act):
        for c in range(n_c):
            for t in range(2):
                pl.when(nt_ref[c, step] > t)(functools.partial(act, c, t))

    def start(step, p):
        def go(c, t):
            for copy in fetches(step, c, t, p):
                copy.start()

        each(step, go)

    @pl.when(e == 0)
    def _():
        for c in range(n_c):
            for k in range(nts[c].shape[0]):
                nt_ref[c, k] = nts[c][k]
        start(e, par)

    @pl.when(e + 1 < n_e)
    def _():
        start(e + 1, 1 - par)

    acc1[...] = jnp.zeros_like(acc1)
    acc2[...] = jnp.zeros_like(acc2)

    def add(j, _):
        @pl.when(nt_ref[j // 2, e] > lax.rem(j, 2))
        def _():
            for k in range(4):
                pltpu.make_async_copy(hbm[k][0].at[0, 0], bufs[k].at[par, j], sems.at[par, j, k]).wait()
            x_rows, d_rows, d_hid, act_w = (buf[par, j] for buf in bufs)
            acc1[...] += dot(x_rows, d_hid, LHS)
            acc2[...] += dot(act_w, d_rows, LHS)

        return 0

    lax.fori_loop(0, 2 * n_c, add, 0)
    gw2_ref[0] = acc2[...].astype(BF)
    gw1_ref[0] = dot(acc1[...].astype(BF), mix_ref[...]).astype(BF)


def run_wgrad(nts, saved, unmix):
    n_c = len(saved)
    xs, ds, dh, wa = (list(t) for t in zip(*saved))
    n_e, dim, wide, half = xs[0].shape[0], xs[0].shape[3], dh[0].shape[3], wa[0].shape[3]
    per_e = lambda e, *nts: (e, 0, 0)
    return pl.pallas_call(
        functools.partial(wgrad_kernel, n_c),
        grid_spec=pltpu.PrefetchScalarGridSpec(
            num_scalar_prefetch=n_c,
            grid=(n_e,),
            in_specs=[pl.BlockSpec(memory_space=pl.ANY)] * (4 * n_c) + [pl.BlockSpec((wide, wide), lambda e, *nts: (0, 0))],
            out_specs=[pl.BlockSpec((1, dim, wide), per_e), pl.BlockSpec((1, half, dim), per_e)],
            scratch_shapes=[pltpu.SMEM((n_c, n_e), jnp.int32), pltpu.VMEM((dim, wide), F32), pltpu.VMEM((half, dim), F32)]
            + [pltpu.VMEM((2, 2 * n_c, TILE, w), BF) for w in (dim, dim, wide, half)]
            + [pltpu.SemaphoreType.DMA((2, 2 * n_c, 4))],
        ),
        out_shape=[jax.ShapeDtypeStruct((n_e, dim, wide), BF), jax.ShapeDtypeStruct((n_e, half, dim), BF)],
        compiler_params=pltpu.CompilerParams(dimension_semantics=('arbitrary',), vmem_limit_bytes=64000 * 1024),
        cost_estimate=pl.CostEstimate(flops=26_000_000_000, bytes_accessed=60_000_000, transcendentals=0),
        name='weight_grads',
    )(*nts, *xs, *ds, *dh, *wa, unmix)


def pack_kernel(x_ref, d_ref, idx_ref, slot_ref, wr_ref, br_ref, tall_ref, w_ref):
    toks = x_ref.shape[0]
    top_k, n = idx_ref.shape[0], wr_ref.shape[0]
    logits = dot(wr_ref[...], x_ref[...], BACK) + br_ref[...]
    expert = lax.broadcasted_iota(jnp.int32, (n, toks), 0)
    hots = [jnp.broadcast_to(idx_ref[k:k + 1, :], (n, toks)) == expert for k in range(top_k)]
    picked = [jnp.sum(jnp.where(h, logits, 0.0), axis=0, keepdims=True) for h in hots]
    top = functools.reduce(jnp.maximum, picked)
    exps = [jnp.exp(v - top) for v in picked]
    norm = functools.reduce(jnp.add, exps)
    w_full = jnp.zeros((n, toks), F32)
    kept = jnp.zeros((n, toks), F32)
    for k in range(top_k):
        w_full += jnp.where(hots[k], exps[k] / norm, 0.0)
        kept += jnp.where(hots[k], jnp.where(slot_ref[k:k + 1, :] >= 0, 1.0, 0.0), 0.0)
    w_ref[...] = w_full
    ahead = lax.broadcasted_iota(jnp.int32, (toks, toks), 0) < lax.broadcasted_iota(jnp.int32, (toks, toks), 1)
    rank = dot(kept.astype(BF), jnp.where(ahead, 1.0, 0.0).astype(BF))
    rank = jnp.where(kept > 0.0, rank, -1.0)
    w_top = w_full.astype(BF)
    rest = w_full - w_top.astype(F32)
    w_mid = rest.astype(BF)
    w_low = (rest - w_mid.astype(F32)).astype(BF)
    tall_ref[:toks, :] = d_ref[...]
    tall_ref[toks:toks + n, :toks] = w_top
    tall_ref[toks:toks + n, toks:] = w_mid
    tall_ref[toks + n:, :toks] = w_low
    tall_ref[toks + n:, toks:] = rank.astype(BF)


def run_pack(x_loc, dy_loc, idx_t, slot_t, w_router, b_router):
    toks, dim = x_loc.shape
    n = w_router.shape[0]
    return pl.pallas_call(
        pack_kernel,
        out_shape=[jax.ShapeDtypeStruct((toks + 2 * n, dim), BF), jax.ShapeDtypeStruct((n, toks), F32)],
        compiler_params=pltpu.CompilerParams(vmem_limit_bytes=32000 * 1024),
        name='pack',
    )(x_loc, dy_loc, idx_t, slot_t, w_router, b_router)


def router_kernel(rel, me_ref, *refs):
    n = len(rel)
    d_ref, out_ref = refs[n:]
    total = jnp.zeros(out_ref.shape, F32)
    for k in range(n):
        d_one = d_ref[me_ref[0] ^ rel[k]].astype(BF)
        total += lax.dot_general(refs[k][...], d_one, (((0,), (1,)), ((), ())), preferred_element_type=F32)
    out_ref[...] = total


def run_router_grad(me, rel, x_blocks, d_rel):
    n = len(x_blocks)
    toks, dim = x_blocks[0].shape
    experts = d_rel.shape[1]
    cut = dim // 4
    return pl.pallas_call(
        functools.partial(router_kernel, rel),
        grid_spec=pltpu.PrefetchScalarGridSpec(
            num_scalar_prefetch=1,
            grid=(4,),
            in_specs=[pl.BlockSpec((toks, cut), lambda j, me: (0, j))] * n + [pl.BlockSpec(d_rel.shape, lambda j, me: (0, 0, 0))],
            out_specs=pl.BlockSpec((cut, experts), lambda j, me: (j, 0)),
        ),
        out_shape=jax.ShapeDtypeStruct((dim, experts), F32),
        compiler_params=pltpu.CompilerParams(vmem_limit_bytes=32000 * 1024),
        name='router_grad',
    )(me, *x_blocks, d_rel)


def solution(mesh):
    tp_count = mesh.shape['tp']
    ep_count = mesh.shape['ep']
    n_dev = tp_count * ep_count
    tok_spec = P(('ep', 'tp'), None)

    CORE, XF, YF = 2, 4, 1
    FAR = XF | YF
    CHIPS = (0, YF, FAR, XF)

    def flip(arr, bits):
        turned = (bits & 1) * ep_count + (bits >> 1)
        return lax.ppermute(arr, ('tp', 'ep'), [(s, s ^ turned) for s in range(n_dev)])

    def device_fn(x_loc, idx_loc, slot_loc, w_router, b_router, w_gate_up, b_gate_up, w_down, b_down, dy_loc):
        toks, _ = x_loc.shape
        n_experts = w_router.shape[1]
        n_e = w_gate_up.shape[0]
        wide = w_gate_up.shape[2]
        half = wide // 2
        tp_index = lax.axis_index('tp')
        ep_index = lax.axis_index('ep')
        me = ep_index * tp_count + tp_index

        tall, w_full = run_pack(x_loc, dy_loc, idx_loc.T, slot_loc.T, w_router.T, b_router[:, None])

        x_of = {XF: flip(x_loc, XF), YF: flip(x_loc, YF)}
        d_of = {XF: flip(tall, XF | CORE), YF: flip(tall, YF | CORE)}
        x_of[FAR] = flip(x_of[XF], YF)
        d_of[FAR] = flip(d_of[YF], XF)
        pairs = [(x_loc, tall, flip(x_loc, CORE), flip(tall, CORE))]
        for bits in CHIPS[1:]:
            pairs.append((x_of[bits], flip(d_of[bits], CORE), flip(x_of[bits], CORE), d_of[bits]))

        col = jnp.arange(wide)
        split_mat = (jnp.where(col < half, 2 * col, 2 * (col - half) + 1)[None, :] == col[:, None]).astype(BF)
        b1 = jnp.concatenate([b_gate_up[:, 0::2], b_gate_up[:, 1::2]], axis=1)[:, None, :]
        b2 = b_down * (tp_index == 0).astype(F32)
        ep = ep_index.astype(jnp.int32)[None]

        w1 = w_gate_up
        dgs, gb1s, gb2s, nts, saved, part = [], [], [], [], [], []

        def chunk(step, blocks, w1):
            o, small, keep, w1 = run_chunk(ep, blocks, w1, w_down, b1, b2, split_mat if step == 0 else None)
            for lst, v in zip((dgs, gb1s, gb2s, nts), small):
                lst.append(v)
            saved.append(keep)
            ya, dxa, yb, dxb = o
            if step == 0:
                part.append((ya, flip(yb, CORE), dxa, flip(dxb, CORE)))
            else:
                part.append((ya, flip(yb, CORE), dxb, flip(dxa, CORE)))
            return w1

        def both(step):
            ya, yb, dxa, dxb = part[step]
            add = lambda a, b: (a.astype(F32) + b.astype(F32)).astype(BF)
            return add(ya, yb), add(dxa, dxb)

        def hop(step, y, dx):
            bits = CHIPS[step]
            return flip(y, bits), flip(dx, bits | CORE)

        w1 = chunk(0, pairs[0], w_gate_up)
        w1 = chunk(1, pairs[1], w1)
        sum_1, blocks = lax.optimization_barrier((both(1), pairs[2]))
        got_1 = hop(1, *sum_1)
        w1 = chunk(2, blocks, w1)
        sum_2, blocks = lax.optimization_barrier((both(2), pairs[3]))
        got_2 = hop(2, *sum_2)
        chunk(3, blocks, w1)

        rel = [CHIPS[k // 2] ^ (CORE * (k % 2)) for k in range(n_dev)]
        dg_rel = jnp.stack([dg[:, k, :] for dg in dgs for k in range(2)])
        slot_of = jnp.array([rel.index(m) for m in range(n_dev)], jnp.int32)
        dg_abs = dg_rel[slot_of[jnp.arange(n_dev) ^ me]]
        dg_back = lax.all_to_all(dg_abs, ('ep', 'tp'), 0, 0, tiled=True)
        sum_3, dg_back = lax.optimization_barrier((both(3), dg_back))
        d_gate = jnp.sum(dg_back.reshape(ep_count, tp_count, n_e, toks), axis=1).reshape(n_experts, toks)
        d_logits = w_full * (d_gate - jnp.sum(w_full * d_gate, axis=0, keepdims=True))
        sum_3, d_logits, last = lax.optimization_barrier((sum_3, d_logits, saved[3]))
        d_all = lax.all_to_all(jnp.broadcast_to(d_logits[None], (n_dev, *d_logits.shape)), ('ep', 'tp'), 0, 0, tiled=True)
        got_3 = hop(3, *sum_3)
        gw1, gw2 = run_wgrad(nts, [*saved[:3], last], split_mat.T)
        gw1, gb1s, gb2s, d_late, own, got_1, got_2 = lax.optimization_barrier((gw1, gb1s, gb2s, d_logits, part[0], got_1, got_2))
        gb1 = functools.reduce(jnp.add, gb1s)[:, 0, :]
        gb1 = jnp.stack([gb1[:, :half], gb1[:, half:]], axis=2).reshape(n_e, wide)
        gb2 = functools.reduce(jnp.add, gb2s)

        wide_sum = lambda *terms: functools.reduce(jnp.add, [t.astype(F32) for t in terms])
        via_router = jnp.einsum('et,de->td', d_late.astype(BF), w_router, preferred_element_type=F32)
        dx_most = wide_sum(own[2], own[3], got_1[1], got_2[1], via_router)
        gwr = run_router_grad(me.astype(jnp.int32)[None], rel, [p[k] for p in pairs for k in (0, 2)], d_all)
        gwr, dx_most, got_3 = lax.optimization_barrier((gwr, dx_most, got_3))
        moe = wide_sum(own[0], own[1], got_1[0], got_2[0], got_3[0])
        d_x = dx_most + got_3[1].astype(F32)
        gbr = jnp.sum(d_all, axis=(0, 2))
        return (moe.astype(BF), d_x.astype(BF), gw1, gb1, gw2, gb2, gwr, gbr)

    in_specs = (tok_spec, tok_spec, tok_spec, P(None, None), P(None), P('ep', None, 'tp'), P('ep', 'tp'), P('ep', 'tp', None), P('ep', None), tok_spec)
    out_specs = (tok_spec, tok_spec, P('ep', None, 'tp'), P('ep', 'tp'), P('ep', 'tp', None), P('ep', None), P(None, None), P(None))

    return jax.shard_map(device_fn, mesh=mesh, in_specs=in_specs, out_specs=out_specs, check_vma=False)
```
